256 devices in a mesh: sector: 8 (over z), op: 32 (over y, x, core).
Axes of the slice: x: 4, y: 4, z: 8, core: 2. Of those that a mesh axis runs over, the one named last changes fastest.
Arguments:
- wavefunction: float32 [8, 512, 512], P('sector', 'op'), may hold values from -6 to 6
- diagonal: float32 [8, 512, 512], P('sector', 'op'), may hold values from 2 to 10
- left_blocks: bfloat16 [256, 512, 512], P('op'), may hold values from -1 to 1
- right_blocks: bfloat16 [256, 512, 512], P('op'), may hold values from -1 to 1
- coupling: int32 [8, 256], replicated, may hold values from 0 to 7
- sector_sizes: int32 [8], replicated, may hold values from 256 to 512
Outputs:
- vector: float32 [8, 512, 512], P('sector', 'op')
- energies: float32 [2], replicated
The draws below stay inside these ranges and needn't reach their ends.
All inputs are finite; a program needn't handle non-finite values.
Results may differ from the reference program's by a relative error of at most 0.0052.
Values may be sent and summed in bfloat16 or wider, within the bound.
No kernel may reach another device: no remote copies, remote signals or barrier semaphores. Data moves between devices by JAX's collectives and lax.ppermute only.
A program may use at most 64 MiB of HBM per device.

```python
import math
import jax
import jax.numpy as jnp
import numpy as np
from jax import lax

BLOCK = 512
STEPS = 2
NSEC = 8
PAIRS = 256


def operator_draw(key):
    first, second = jax.random.split(key)
    spread = 1.0 / jnp.sqrt(jnp.float32(BLOCK))
    noise = jnp.clip(jax.random.normal(first, (PAIRS, BLOCK, BLOCK), jnp.float32), -4.0, 4.0)
    level = jax.random.uniform(second, (PAIRS, BLOCK), jnp.float32, 0.2, 0.3)
    ident = jnp.eye(BLOCK, dtype=jnp.float32)
    whole = noise * spread + ident[None, :, :] * level[:, :, None]
    return jnp.clip(whole, -1.0, 1.0).astype(jnp.bfloat16)


def draw_left_blocks(key, part):
    return operator_draw(jax.random.fold_in(key, 11))


def draw_right_blocks(key, part):
    return operator_draw(jax.random.fold_in(key, 23))


def set_ends(drawn, key, smallest, top_value):
    place = [jax.random.randint(jax.random.fold_in(key, axis), (), 0, length) for axis, length in enumerate(drawn.shape)]
    widest = drawn.shape.index(max(drawn.shape))
    neighbour = place[:widest] + [(place[widest] + 1) % drawn.shape[widest]] + place[widest + 1:]
    return drawn.at[tuple(place)].set(smallest).at[tuple(neighbour)].set(top_value)


def shard_levels(stream_key, extent, pieces, low, high):
    level, own = 1.0, jax.random.fold_in(stream_key, 6)
    for axis_at, shards_of in pieces:
        steps = jnp.exp(jax.random.uniform(jax.random.fold_in(own, axis_at), (shards_of,), jnp.float32, low / len(pieces), high / len(pieces)))
        level = level * jnp.repeat(steps, extent[axis_at] // shards_of).reshape([-1 if axis == axis_at else 1 for axis in range(len(extent))])
    return level


def rank_table(number_of, skew):
    portions = [(1 << 20) // math.isqrt(grade ** skew) + 1 for grade in range(1, number_of + 1)]
    scale = 1 + sum(portions) // (1 << 30)
    return np.cumsum(np.array([max(1, weight // scale) for weight in portions]))


def ranked(own_key, shape, number_of, skew):
    grid = rank_table(number_of, skew)
    lot = jax.random.randint(jax.random.fold_in(own_key, 1), shape, 0, int(grid[number_of - 1]))
    rank = jnp.searchsorted(jnp.asarray(grid, jnp.int32), lot, side="right")
    return jax.random.permutation(jax.random.fold_in(own_key, 2), number_of)[rank].astype(jnp.int32)


def scatter_about(stream_key, extent, scale, limit, cuts=(), kind=jnp.bfloat16):
    array = scale * jax.random.normal(stream_key, extent, jnp.float32)
    if cuts:
        array = array * shard_levels(stream_key, extent, cuts, -0.22, 0.18)
    return jnp.clip(array, -limit, limit).astype(kind)


def setup_inputs(seed: int = 0) -> dict:
    streams_of = jax.random.split(jax.random.key(seed), 7)
    wavefunction = scatter_about(streams_of[0], (NSEC, BLOCK, BLOCK), 1.0, 6.0, ((0, 8), (1, 32)), jnp.float32)
    diagonal = jnp.clip(2.0 + 8.0 * jax.random.uniform(streams_of[1], (NSEC, BLOCK, BLOCK), jnp.float32) ** shard_levels(streams_of[1], (NSEC, BLOCK, BLOCK), ((0, 8), (1, 32)), -0.2, 0.2), 2.0, 10.0)
    left_blocks = draw_left_blocks(jax.random.fold_in(streams_of[6], 71), 0)
    right_blocks = draw_right_blocks(jax.random.fold_in(streams_of[6], 71), 0)
    coupling = set_ends(ranked(streams_of[4], (NSEC, PAIRS), NSEC, 2), jax.random.fold_in(streams_of[4], 3), 0, NSEC - 1).astype(jnp.int32)
    sector_sizes = set_ends(jax.random.randint(streams_of[5], (NSEC,), BLOCK // 2, BLOCK + 1), jax.random.fold_in(streams_of[5], 1), BLOCK // 2, BLOCK).astype(jnp.int32)
    return {"wavefunction": wavefunction, "diagonal": diagonal, "left_blocks": left_blocks, "right_blocks": right_blocks, "coupling": coupling, "sector_sizes": sector_sizes}


def reference(wavefunction, diagonal, left_blocks, right_blocks, coupling, sector_sizes):
    positions = jnp.arange(BLOCK, dtype=jnp.int32)
    live = positions[None, :] < sector_sizes[:, None]
    mask = (live[:, :, None] & live[:, None, :]).astype(jnp.float32)
    current = wavefunction * mask
    left_wide = left_blocks.astype(jnp.float32)
    right_wide = right_blocks.astype(jnp.float32)
    collected = []
    for iteration in range(STEPS):
        current_low = current.astype(jnp.bfloat16)

        def sector_sigma(target):
            picked = jnp.take(current_low, coupling[target], axis=0).astype(jnp.float32)
            half = jnp.einsum('pij,pjk->pik', left_wide, picked).astype(jnp.bfloat16)
            return jnp.einsum('pik,plk->il', half.astype(jnp.float32), right_wide)
        sigma = lax.map(sector_sigma, jnp.arange(NSEC, dtype=jnp.int32)) * mask
        numerator = jnp.sum(current * sigma)
        denominator = jnp.sum(current * current)
        theta = numerator / (denominator + 1e-06)
        collected.append(theta)
        gap = diagonal - theta
        update = current - (sigma - theta * current) * gap / (gap * gap + 1.0)
        current = update * lax.rsqrt(jnp.mean(update * update) + 1e-06)
    return (current, jnp.stack(collected).astype(jnp.float32))
```

```python
import functools
import jax
import jax.numpy as jnp
from jax import lax
from jax.experimental import pallas as pl
from jax.experimental.pallas import tpu as pltpu
from jax.sharding import Mesh
from jax.sharding import PartitionSpec as P

OP = ("op_0", "op_1", "op_2")
CHIP = ("op_0", "op_1")
CORE = "op_2"
COLUMN = ("sector", "op_2")
BF = jnp.bfloat16
F32 = jnp.float32
VMEM = pl.BlockSpec(memory_space=pltpu.VMEM)
SMEM = pl.BlockSpec(memory_space=pltpu.SMEM)
ANY = pl.BlockSpec(memory_space=pl.ANY)


def swap_all(x, axes):
    return lax.all_to_all(x, axes, split_axis=0, concat_axis=0, tiled=True)


def other_core(x):
    return lax.ppermute(x, CORE, [(0, 1), (1, 0)])


def three_way(first, second):
    row = lax.broadcasted_iota(jnp.int32, (16, 128), 0)
    value = jnp.where(row < 3, first, second)
    high = value.astype(BF).astype(F32)
    middle = (value - high).astype(BF).astype(F32)
    low = value - high - middle
    part = jnp.where(row < 3, row, row - 3)
    return jnp.where(part == 0, high, jnp.where(part == 1, middle, low)).astype(BF)


def two_sums(tile):
    first = tile[0:1] + tile[1:2] + tile[2:3]
    second = tile[3:4] + tile[4:5] + tile[5:6]
    return first[:, :1], second[:, :1]


def place():
    z = lax.axis_index("sector")
    chip = lax.axis_index("op_0") * lax.axis_size("op_1") + lax.axis_index("op_1")
    return z, chip, lax.axis_index(CORE)


def live(shape, where_ref):
    first_row, size = where_ref[0], where_ref[1]
    row = lax.broadcasted_iota(jnp.int32, shape, 0) + first_row
    column = lax.broadcasted_iota(jnp.int32, shape, 1)
    return (row < size) & (column < size)


def opening_kernel(where_ref, wave_ref, diag_ref, send_ref, current_ref, square_ref):
    wave = wave_ref[...]
    current = jnp.where(live(wave.shape, where_ref), wave, 0.0)
    current_ref[...] = current
    square_ref[...] = jnp.full((8, 128), jnp.sum(current * current), F32)
    diag = diag_ref[...]
    high = diag.astype(BF)
    low = (diag - high.astype(F32)).astype(BF)
    current_low = current.astype(BF)
    width = wave.shape[1] // 2
    for peer in range(send_ref.shape[0]):
        cut = slice((peer % 2) * width, (peer % 2 + 1) * width)
        send_ref[peer, 0] = current_low[:, cut]
        send_ref[peer, 1] = high[:, cut]
        send_ref[peer, 2] = low[:, cut]


def product_kernel(
    where_ref, coupling_ref, rows_ref, left_a, right_a, left_b, right_b, total_ref, low_ref
):
    pair = pl.program_id(0)
    block = left_a.shape[1]
    halves = []
    for base, left in ((where_ref[3], left_a), (where_ref[4], left_b)):
        source = coupling_ref[where_ref[2], base + pair]
        rows = rows_ref[:, source].reshape(block, -1)
        halves.append(jnp.dot(left[0], rows, preferred_element_type=F32).astype(BF))
    half = jnp.concatenate(halves, axis=1)
    right = jnp.concatenate([right_a[0], right_b[0]], axis=1)
    term = lax.dot_general(half, right, (((1,), (1,)), ((), ())), preferred_element_type=F32)

    @pl.when(pair == 0)
    def _():
        total_ref[...] = term

    @pl.when(pair > 0)
    def _():
        total_ref[...] += term

    @pl.when(pair == pl.num_programs(0) - 1)
    def _():
        low_ref[...] = total_ref[...].astype(BF)


def products(where, coupling, rows, left, right, left_other, right_other):
    pairs, block, _ = left.shape
    width = rows.shape[-1]
    whole = rows.shape
    return pl.pallas_call(
        product_kernel,
        grid_spec=pltpu.PrefetchScalarGridSpec(
            num_scalar_prefetch=2,
            grid=(pairs,),
            in_specs=[
                pl.BlockSpec(whole, lambda p, w, c: (0,) * len(whole), pipeline_mode=pl.Buffered(1)),
                pl.BlockSpec((1, block, block), lambda p, w, c: (p, 0, 0)),
                pl.BlockSpec((1, block, width), lambda p, w, c: (p, 0, w[5])),
                pl.BlockSpec((1, block, block), lambda p, w, c: (p, 0, 0)),
                pl.BlockSpec((1, block, width), lambda p, w, c: (p, 0, w[5])),
            ],
            out_specs=[
                pl.BlockSpec((block, block), lambda p, w, c: (0, 0)),
                pl.BlockSpec((block, block), lambda p, w, c: (0, 0)),
            ],
        ),
        out_shape=[
            jax.ShapeDtypeStruct((block, block), F32),
            jax.ShapeDtypeStruct((block, block), BF),
        ],
        compiler_params=pltpu.CompilerParams(vmem_limit_bytes=40 << 20),
        name="products",
    )(where, coupling, rows, left, right, left_other, right_other)


def parting_kernel(where_ref, total_ref, other_ref, rows_ref, square_ref, send_ref):
    core = where_ref[5]
    block = total_ref.shape[0]
    width = rows_ref.shape[-1]
    cut = pl.ds(pl.multiple_of(core * width, width), width)
    mine = total_ref[:, cut] + other_ref[:, cut].astype(F32)
    vector = rows_ref[:, 0].reshape(block, width).astype(F32)
    extra = three_way(jnp.sum(vector * mine), square_ref[0, 0])
    for chip in range(send_ref.shape[0]):
        rows = pl.ds(pl.multiple_of(chip * 32 + core * 16, 16), 16)
        tile = (total_ref[rows, :] + other_ref[rows, :].astype(F32)).astype(BF)
        for j in range(block // 128):
            send_ref[chip, j * 16 : (j + 1) * 16, :] = tile[:, j * 128 : (j + 1) * 128]
        send_ref[chip, block // 8 : block // 8 + 16, :] = extra


def parting(where, total, other, rows, square):
    block = total.shape[0]
    chips, sectors, share, width = rows.shape
    return pl.pallas_call(
        parting_kernel,
        grid_spec=pltpu.PrefetchScalarGridSpec(
            num_scalar_prefetch=1,
            grid=(1,),
            in_specs=[
                pl.BlockSpec((block, block), lambda i, w: (0, 0)),
                pl.BlockSpec((block, block), lambda i, w: (0, 0)),
                pl.BlockSpec((chips, 1, share, width), lambda i, w: (0, w[2], 0, 0)),
                pl.BlockSpec((8, 128), lambda i, w: (0, 0)),
            ],
            out_specs=pl.BlockSpec((chips, block // 8 + 16, 128), lambda i, w: (0, 0, 0)),
        ),
        out_shape=jax.ShapeDtypeStruct((chips, block // 8 + 16, 128), BF),
        name="parting",
    )(where, total, other, rows, square)


def joining_kernel(where_ref, arrived_ref, sigma_ref, send_ref):
    total = arrived_ref[0].astype(F32)
    for chip in range(1, arrived_ref.shape[0]):
        total = total + arrived_ref[chip].astype(F32)
    parts = (total.shape[0] - 16) // 16
    sigma = jnp.concatenate([total[j * 16 : (j + 1) * 16] for j in range(parts)], axis=1)
    sigma = jnp.where(live(sigma.shape, where_ref), sigma, 0.0)
    sigma_ref[...] = sigma
    first, second = two_sums(total[parts * 16 :])
    extra = three_way(first, second)
    low = sigma.astype(BF)
    each = parts // 2
    for peer in range(send_ref.shape[0]):
        for j in range(each):
            at = ((peer % 2) * each + j) * 128
            send_ref[peer, j * 16 : (j + 1) * 16, :] = low[:, at : at + 128]
        send_ref[peer, each * 16 : each * 16 + 16, :] = extra


def scalars_of(arrived_ref):
    at = arrived_ref.shape[1] - 16
    total = arrived_ref[0, at:].astype(F32)
    for peer in range(1, arrived_ref.shape[0]):
        total = total + arrived_ref[peer, at:].astype(F32)
    return two_sums(total)


def sigma_of(arrived_ref, peer):
    parts = (arrived_ref.shape[1] - 16) // 16
    return jnp.concatenate(
        [arrived_ref[peer, j * 16 : (j + 1) * 16, :] for j in range(parts)], axis=1
    ).astype(F32)


def corrected(current, sigma, diag, theta):
    gap = diag - theta
    return current - (sigma - theta * current) * gap / (gap * gap + 1.0)


def middle_kernel(
    arrived_ref, begun_ref, sigma_ref, current_ref, diag_ref,
    send_ref, all_ref, own_ref, square_ref, theta_ref, low_ref, sems,
):
    first, second = scalars_of(arrived_ref)
    theta = first / (second + 1e-6)
    theta_ref[...] = jnp.broadcast_to(theta, (8, 128))
    for peer in range(arrived_ref.shape[0]):
        current = begun_ref[peer, 0].astype(F32)
        diag = begun_ref[peer, 1].astype(F32) + begun_ref[peer, 2].astype(F32)
        update = corrected(current, sigma_of(arrived_ref, peer), diag, theta)
        all_ref[peer] = update
        low_ref[peer] = update.astype(BF)
    own = corrected(current_ref[...], sigma_ref[...], diag_ref[...], theta)
    own_ref[...] = own
    square_ref[...] = jnp.full((8, 128), jnp.sum(own * own), F32)
    copies = [
        pltpu.make_async_copy(low_ref, send_ref.at[chip], sems.at[chip])
        for chip in range(send_ref.shape[0])
    ]
    for copy in copies:
        copy.start()
    for copy in copies:
        copy.wait()


def closing_kernel(
    entries, arrived_ref, begun_ref, all_ref, sigma_ref, own_ref, diag_ref, before_ref,
    final_ref, send_ref, theta_ref,
):
    first, second = scalars_of(arrived_ref)
    scale = lax.rsqrt(second / entries + 1e-6)
    squared = scale * scale
    theta = squared * first / (squared * second + 1e-6)
    lane = lax.broadcasted_iota(jnp.int32, (8, 128), 1)
    theta_ref[...] = jnp.where(lane == 0, before_ref[...], theta)
    total = jnp.zeros(all_ref.shape[1:], F32)
    for peer in range(arrived_ref.shape[0]):
        diag = begun_ref[peer, 1].astype(F32) + begun_ref[peer, 2].astype(F32)
        update = corrected(scale * all_ref[peer], scale * sigma_of(arrived_ref, peer), diag, theta)
        total = total + update * update
    final_ref[...] = corrected(scale * own_ref[...], scale * sigma_ref[...], diag_ref[...], theta)
    send_ref[...] = jnp.full(send_ref.shape, jnp.sum(total), F32)


def scaling_kernel(entries, arrived_ref, final_ref, vector_ref):
    total = arrived_ref[0]
    for peer in range(1, arrived_ref.shape[0]):
        total = total + arrived_ref[peer]
    vector_ref[...] = final_ref[...] * lax.rsqrt(total[0:1, 0:1] / entries + 1e-6)


def call(kernel, shapes, specs, name, scratch=(), out_specs=None):
    return pl.pallas_call(
        kernel,
        in_specs=specs,
        out_specs=out_specs if out_specs is not None else [VMEM] * len(shapes),
        out_shape=[jax.ShapeDtypeStruct(s, t) for s, t in shapes],
        scratch_shapes=scratch,
        name=name,
    )


def shards(wavefunction, diagonal, left_blocks, right_blocks, coupling, sector_sizes):
    _, share, block = wavefunction.shape
    pairs = left_blocks.shape[0]
    sectors = lax.axis_size("sector")
    chips = lax.axis_size("op_0") * lax.axis_size("op_1")
    width = block // 2
    entries = float(sectors * block * block)
    z, chip, core = place()
    mine = chip * 2 + core
    theirs = chip * 2 + 1 - core
    where = jnp.stack(
        [mine * share, sector_sizes[z], z, mine * pairs, theirs * pairs, core]
    ).astype(jnp.int32)
    wave, diag = wavefunction[0], diagonal[0]
    left_other = other_core(left_blocks)
    right_other = other_core(right_blocks)

    begin, current, square = call(
        opening_kernel,
        [((sectors * 2, 3, share, width), BF), ((share, block), F32), ((8, 128), F32)],
        [SMEM, VMEM, VMEM],
        "opening",
    )(where, wave, diag)
    begun = swap_all(begin, COLUMN)
    outgoing = jnp.broadcast_to(begun[None, :, 0], (chips, sectors * 2, share, width))

    def sigma_step(outgoing, square):
        rows = swap_all(outgoing, CHIP).reshape(chips, sectors, 2 * share, width)
        total, low = products(
            where, coupling, rows, left_blocks, right_blocks, left_other, right_other
        )
        send = parting(where, total, other_core(low), rows, square)
        sigma, send = call(
            joining_kernel,
            [((share, block), F32), ((sectors * 2, width // 8 + 16, 128), BF)],
            [SMEM, VMEM],
            "joining",
        )(where, swap_all(send, CHIP))
        return sigma, swap_all(send, COLUMN)

    sigma, arrived = sigma_step(outgoing, square)
    outgoing, everyone, own, square, theta = call(
        middle_kernel,
        [
            ((chips, sectors * 2, share, width), BF),
            ((sectors * 2, share, width), F32),
            ((share, block), F32),
            ((8, 128), F32),
            ((8, 128), F32),
        ],
        [VMEM] * 5,
        "middle",
        [pltpu.VMEM((sectors * 2, share, width), BF), pltpu.SemaphoreType.DMA((chips,))],
        [ANY, VMEM, VMEM, VMEM, VMEM],
    )(arrived, begun, sigma, current, diag)

    sigma, arrived = sigma_step(outgoing, square)
    final, send, thetas = call(
        functools.partial(closing_kernel, entries),
        [((share, block), F32), ((chips * 2, 8, 128), F32), ((8, 128), F32)],
        [VMEM] * 7,
        "closing",
    )(arrived, begun, everyone, sigma, own, diag, theta)
    (vector,) = call(
        functools.partial(scaling_kernel, entries),
        [((share, block), F32)],
        [VMEM] * 2,
        "scaling",
    )(swap_all(send, OP), final)
    return vector[None], thetas[0, :2]


def solution(mesh):
    split = Mesh(
        mesh.devices.reshape(mesh.shape["sector"], 4, 4, 2), ("sector", "op_0", "op_1", "op_2")
    )
    in_specs = (
        P("sector", OP, None),
        P("sector", OP, None),
        P(OP, None, None),
        P(OP, None, None),
        P(),
        P(),
    )
    out_specs = (P("sector", OP, None), P())
    return jax.shard_map(
        shards, mesh=split, in_specs=in_specs, out_specs=out_specs, check_vma=False
    )
```

```python
import functools
import jax
import jax.numpy as jnp
from jax import lax
from jax.experimental import pallas as pl
from jax.experimental.pallas import tpu as pltpu
from jax.sharding import Mesh
from jax.sharding import PartitionSpec as P

OP = ("op_0", "op_1", "op_2")
CHIP = ("op_0", "op_1")
CORE = "op_2"
COLUMN = ("sector", "op_2")
BF = jnp.bfloat16
F32 = jnp.float32
VMEM = pl.BlockSpec(memory_space=pltpu.VMEM)
SMEM = pl.BlockSpec(memory_space=pltpu.SMEM)
ANY = pl.BlockSpec(memory_space=pl.ANY)
SHARE = 16
LANES = 128


def swap_all(x, axes):
    return lax.all_to_all(x, axes, split_axis=0, concat_axis=0, tiled=True)


def other_core(x):
    return lax.ppermute(x, CORE, [(0, 1), (1, 0)])


def three_way(first, second):
    row = lax.broadcasted_iota(jnp.int32, (16, 128), 0)
    value = jnp.where(row < 3, first, second)
    high = value.astype(BF).astype(F32)
    middle = (value - high).astype(BF).astype(F32)
    low = value - high - middle
    part = jnp.where(row < 3, row, row - 3)
    return jnp.where(part == 0, high, jnp.where(part == 1, middle, low)).astype(BF)


def two_sums(tile):
    first = tile[0:1] + tile[1:2] + tile[2:3]
    second = tile[3:4] + tile[4:5] + tile[5:6]
    return first[:, :1], second[:, :1]


def place():
    z = lax.axis_index("sector")
    chip = lax.axis_index("op_0") * lax.axis_size("op_1") + lax.axis_index("op_1")
    return z, chip, lax.axis_index(CORE)


def live(shape, first_row, size):
    row = lax.broadcasted_iota(jnp.int32, shape, 0) + first_row
    column = lax.broadcasted_iota(jnp.int32, shape, 1)
    return (row < size) & (column < size)


def stacked(ref, lead, tile):
    rows, block = tile.shape
    for j in range(block // LANES):
        ref[lead, j * rows : (j + 1) * rows, :] = tile[:, j * LANES : (j + 1) * LANES]


def unstacked(value, rows):
    parts = value.shape[0] // rows
    return jnp.concatenate([value[j * rows : (j + 1) * rows] for j in range(parts)], axis=1)


def opening_kernel(sizes_ref, wave_ref, diag_ref, send_ref, current_ref, square_ref):
    z, chip, core = place()
    wave = wave_ref[0]
    inside = live(wave.shape, (chip * 2 + core) * SHARE, sizes_ref[z])
    current = jnp.where(inside, wave, 0.0)
    current_ref[...] = current
    square_ref[...] = jnp.full((8, LANES), jnp.sum(current * current), F32)
    diag = diag_ref[0]
    high = diag.astype(BF)
    low = (diag - high.astype(F32)).astype(BF)
    current_low = current.astype(BF)
    for peer in range(send_ref.shape[0]):
        send_ref[peer, 0] = current_low
        send_ref[peer, 1] = high
        send_ref[peer, 2] = low


def halves_of(z, width):
    half = z % 2
    near = pl.ds(pl.multiple_of(half * width, width), width)
    far = pl.ds(pl.multiple_of((1 - half) * width, width), width)
    return near, far


def slabs(rows_at, send_ref):
    z, _, _ = place()
    chips, count, _, width = send_ref.shape
    near, far = halves_of(z, width)
    for k in range(count):
        if k < count - 2:
            slab = rows_at(k, near)
        else:
            slab = rows_at((z // 2) * 2 + k - (count - 2), far)
        for chip in range(chips):
            send_ref[chip, k] = slab


def spreading_kernel(begun_ref, send_ref):
    slabs(lambda k, cut: begun_ref[k, 0, :, cut], send_ref)


def product_kernel(
    coupling_ref, mine_ref, theirs_ref, left_a, right_a, left_b, right_b, square_ref,
    send_ref, total, rows, sems,
):
    pair = pl.program_id(0)
    z, chip, core = place()
    target = (z // 2) * 2 + core
    block, width = total.shape[0], rows.shape[-1]

    @pl.when(pair == 0)
    def _():
        copies = []
        for k in range(rows.shape[0]):
            for j, (ref, at) in enumerate(((mine_ref, core), (theirs_ref, 1 - core))):
                copies.append(
                    pltpu.make_async_copy(ref.at[:, k], rows.at[k, :, at], sems.at[2 * k + j])
                )
        for copy in copies:
            copy.start()
        for copy in copies:
            copy.wait()

    halves = []
    for owner, left in ((core, left_a), (1 - core, left_b)):
        source = coupling_ref[target, (chip * 2 + owner) * pl.num_programs(0) + pair]
        vector = rows[source].reshape(block, width)
        halves.append(jnp.dot(left[0], vector, preferred_element_type=F32).astype(BF))
    half = jnp.concatenate(halves, axis=1)
    right = jnp.concatenate([right_a[0], right_b[0]], axis=1)
    term = lax.dot_general(half, right, (((1,), (1,)), ((), ())), preferred_element_type=F32)

    @pl.when(pair == 0)
    def _():
        total[...] = term

    @pl.when(pair > 0)
    def _():
        total[...] += term

    @pl.when(pair == pl.num_programs(0) - 1)
    def _():
        near, far = halves_of(z, width)
        here = rows[target].reshape(block, width).astype(F32)
        there = rows[rows.shape[0] - 2 + core].reshape(block, width).astype(F32)
        product = jnp.sum(here * total[:, near] + there * total[:, far])
        extra = three_way(product, square_ref[0, 0])
        for peer in range(send_ref.shape[0]):
            stacked(send_ref, peer, total[peer * 32 : (peer + 1) * 32, :].astype(BF))
            send_ref[peer, block // 4 :, :] = extra


def products(coupling, mine, theirs, left, right, left_other, right_other, square):
    pairs, block, _ = left.shape
    chips, count, share, width = mine.shape
    operator = pl.BlockSpec((1, block, block), lambda p, c: (p, 0, 0))
    columns = pl.BlockSpec((1, block, width), lambda p, c: (p, 0, lax.axis_index("sector") % 2))
    return pl.pallas_call(
        product_kernel,
        grid_spec=pltpu.PrefetchScalarGridSpec(
            num_scalar_prefetch=1,
            grid=(pairs,),
            in_specs=[
                ANY, ANY, operator, columns, operator, columns,
                pl.BlockSpec((8, LANES), lambda p, c: (0, 0)),
            ],
            out_specs=pl.BlockSpec((chips, block // 4 + 16, LANES), lambda p, c: (0, 0, 0)),
            scratch_shapes=[
                pltpu.VMEM((block, block), F32),
                pltpu.VMEM((count, chips, 2, share, width), BF),
                pltpu.SemaphoreType.DMA((2 * count,)),
            ],
        ),
        out_shape=jax.ShapeDtypeStruct((chips, block // 4 + 16, LANES), BF),
        compiler_params=pltpu.CompilerParams(vmem_limit_bytes=60 << 20),
        name="products",
    )(coupling, mine, theirs, left, right, left_other, right_other, square)


def joining_kernel(sizes_ref, arrived_ref, send_ref):
    z, chip, core = place()
    total = arrived_ref[0].astype(F32)
    for peer in range(1, arrived_ref.shape[0]):
        total = total + arrived_ref[peer].astype(F32)
    end = total.shape[0] - 16
    sigma = unstacked(total[:end], 32)
    inside = live(sigma.shape, chip * 32, sizes_ref[(z // 2) * 2 + core])
    low = jnp.where(inside, sigma, 0.0).astype(BF)
    extra = three_way(*two_sums(total[end:]))
    for peer in range(send_ref.shape[0]):
        at = (peer % 2) * SHARE
        stacked(send_ref, peer, low[at : at + SHARE])
        send_ref[peer, end // 2 :, :] = extra


def scalars_of(arrived_ref):
    at = arrived_ref.shape[1] - 16
    total = arrived_ref[0, at:].astype(F32)
    for peer in range(1, arrived_ref.shape[0]):
        total = total + arrived_ref[peer, at:].astype(F32)
    return two_sums(total)


def sigma_of(arrived_ref, target):
    end = arrived_ref.shape[1] - 16
    at = (target // 2) * 4 + target % 2
    both = arrived_ref[at, :end].astype(F32) + arrived_ref[at + 2, :end].astype(F32)
    return unstacked(both, SHARE)


def corrected(current, sigma, diag, theta):
    gap = diag - theta
    return current - (sigma - theta * current) * gap / (gap * gap + 1.0)


def middle_kernel(
    arrived_ref, begun_ref, current_ref, diag_ref,
    send_ref, all_ref, own_ref, square_ref, theta_ref, low_ref,
):
    z, _, _ = place()
    first, second = scalars_of(arrived_ref)
    theta = first / (second + 1e-6)
    theta_ref[...] = jnp.broadcast_to(theta, (8, LANES))
    for k in range(all_ref.shape[0]):
        diag = begun_ref[k, 1].astype(F32) + begun_ref[k, 2].astype(F32)
        update = corrected(begun_ref[k, 0].astype(F32), sigma_of(arrived_ref, k), diag, theta)
        all_ref[k] = update
        low_ref[k] = update.astype(BF)
    own = corrected(current_ref[...], sigma_of(arrived_ref, z), diag_ref[0], theta)
    own_ref[...] = own
    square_ref[...] = jnp.full((8, LANES), jnp.sum(own * own), F32)
    slabs(lambda k, cut: low_ref[k, :, cut], send_ref)


def closing_kernel(
    entries, arrived_ref, begun_ref, all_ref, own_ref, diag_ref, before_ref,
    final_ref, send_ref, theta_ref,
):
    z, _, _ = place()
    first, second = scalars_of(arrived_ref)
    scale = lax.rsqrt(second / entries + 1e-6)
    squared = scale * scale
    theta = squared * first / (squared * second + 1e-6)
    lane = lax.broadcasted_iota(jnp.int32, (8, LANES), 1)
    theta_ref[...] = jnp.where(lane == 0, before_ref[...], theta)
    total = jnp.zeros(all_ref.shape[1:], F32)
    for k in range(all_ref.shape[0]):
        diag = begun_ref[k, 1].astype(F32) + begun_ref[k, 2].astype(F32)
        update = corrected(scale * all_ref[k], scale * sigma_of(arrived_ref, k), diag, theta)
        total = total + update * update
    sigma = sigma_of(arrived_ref, z)
    final_ref[...] = corrected(scale * own_ref[...], scale * sigma, diag_ref[0], theta)
    send_ref[...] = jnp.full(send_ref.shape, jnp.sum(total), F32)


def scaling_kernel(entries, arrived_ref, final_ref, vector_ref):
    total = arrived_ref[0]
    for peer in range(1, arrived_ref.shape[0]):
        total = total + arrived_ref[peer]
    vector_ref[0] = final_ref[...] * lax.rsqrt(total[0:1, 0:1] / entries + 1e-6)


def call(kernel, shapes, specs, name, scratch=()):
    return pl.pallas_call(
        kernel,
        in_specs=specs,
        out_specs=[VMEM] * len(shapes),
        out_shape=[jax.ShapeDtypeStruct(s, t) for s, t in shapes],
        scratch_shapes=scratch,
        compiler_params=pltpu.CompilerParams(vmem_limit_bytes=16 << 20),
        name=name,
    )


def shards(wavefunction, diagonal, left_blocks, right_blocks, coupling, sector_sizes):
    _, share, block = wavefunction.shape
    sectors = lax.axis_size("sector")
    chips = lax.axis_size("op_0") * lax.axis_size("op_1")
    width = block // 2
    entries = float(sectors * block * block)
    left_other = other_core(left_blocks)
    right_other = other_core(right_blocks)
    spread = ((chips, sectors + 2, share, width), BF)
    scalar = ((8, LANES), F32)

    begin, current, square = call(
        opening_kernel,
        [((sectors, 3, share, block), BF), ((share, block), F32), scalar],
        [SMEM, VMEM, VMEM],
        "opening",
    )(sector_sizes, wavefunction, diagonal)
    begun = swap_all(begin, "sector")
    (outgoing,) = call(spreading_kernel, [spread], [VMEM], "spreading")(begun)

    def sigma_step(outgoing, square):
        mine = swap_all(outgoing, CHIP)
        send = products(
            coupling, mine, other_core(mine),
            left_blocks, right_blocks, left_other, right_other, square,
        )
        (send,) = call(
            joining_kernel,
            [((sectors * 2, block // 8 + 16, LANES), BF)],
            [SMEM, VMEM],
            "joining",
        )(sector_sizes, swap_all(send, CHIP))
        return swap_all(send, COLUMN)

    arrived = sigma_step(outgoing, square)
    outgoing, everyone, own, square, theta = call(
        middle_kernel,
        [spread, ((sectors, share, block), F32), ((share, block), F32), scalar, scalar],
        [VMEM] * 4,
        "middle",
        [pltpu.VMEM((sectors, share, block), BF)],
    )(arrived, begun, current, diagonal)

    arrived = sigma_step(outgoing, square)
    final, send, thetas = call(
        functools.partial(closing_kernel, entries),
        [((share, block), F32), ((chips * 2, 8, LANES), F32), scalar],
        [VMEM] * 6,
        "closing",
    )(arrived, begun, everyone, own, diagonal, theta)
    (vector,) = call(
        functools.partial(scaling_kernel, entries),
        [((1, share, block), F32)],
        [VMEM] * 2,
        "scaling",
    )(swap_all(send, OP), final)
    return vector, thetas[0, :2]


def solution(mesh):
    split = Mesh(
        mesh.devices.reshape(mesh.shape["sector"], 4, 4, 2), ("sector", "op_0", "op_1", "op_2")
    )
    in_specs = (
        P("sector", OP, None),
        P("sector", OP, None),
        P(OP, None, None),
        P(OP, None, None),
        P(),
        P(),
    )
    out_specs = (P("sector", OP, None), P())
    return jax.shard_map(
        shards, mesh=split, in_specs=in_specs, out_specs=out_specs, check_vma=False
    )
```

```python
import functools
import jax
import jax.numpy as jnp
from jax import lax
from jax.experimental import pallas as pl
from jax.experimental.pallas import tpu as pltpu
from jax.sharding import Mesh
from jax.sharding import PartitionSpec as P

OP = ("op_0", "op_1", "op_2")
CHIP = ("op_0", "op_1")
CORE = "op_2"
COLUMN = ("sector", "op_2")
BF = jnp.bfloat16
F32 = jnp.float32
VMEM = pl.BlockSpec(memory_space=pltpu.VMEM)
SMEM = pl.BlockSpec(memory_space=pltpu.SMEM)
HBM = pl.BlockSpec(memory_space=pltpu.HBM)
SHARE = 16
LANES = 128


def swap_all(x, axes):
    return lax.all_to_all(x, axes, split_axis=0, concat_axis=0, tiled=True)


def other_core(x):
    return lax.ppermute(x, CORE, [(0, 1), (1, 0)])


def three_way(first, second):
    row = lax.broadcasted_iota(jnp.int32, (16, 128), 0)
    value = jnp.where(row < 3, first, second)
    high = value.astype(BF).astype(F32)
    middle = (value - high).astype(BF).astype(F32)
    low = value - high - middle
    part = jnp.where(row < 3, row, row - 3)
    return jnp.where(part == 0, high, jnp.where(part == 1, middle, low)).astype(BF)


def two_sums(tile):
    first = tile[0:1] + tile[1:2] + tile[2:3]
    second = tile[3:4] + tile[4:5] + tile[5:6]
    return first[:, :1], second[:, :1]


def place():
    z = lax.axis_index("sector")
    chip = lax.axis_index("op_0") * lax.axis_size("op_1") + lax.axis_index("op_1")
    return z, chip, lax.axis_index(CORE)


def live(shape, first_row, size):
    row = lax.broadcasted_iota(jnp.int32, shape, 0) + first_row
    column = lax.broadcasted_iota(jnp.int32, shape, 1)
    return (row < size) & (column < size)


def stacked(ref, lead, tile):
    rows, block = tile.shape
    for j in range(block // LANES):
        ref[lead, j * rows : (j + 1) * rows, :] = tile[:, j * LANES : (j + 1) * LANES]


def unstacked(value, rows):
    parts = value.shape[0] // rows
    return jnp.concatenate([value[j * rows : (j + 1) * rows] for j in range(parts)], axis=1)


def opening_kernel(sizes_ref, wave_ref, diag_ref, send_ref, current_ref, square_ref):
    z, chip, core = place()
    wave = wave_ref[0]
    inside = live(wave.shape, (chip * 2 + core) * SHARE, sizes_ref[z])
    current = jnp.where(inside, wave, 0.0)
    current_ref[...] = current
    square_ref[...] = jnp.full((8, LANES), jnp.sum(current * current), F32)
    diag = diag_ref[0]
    high = diag.astype(BF)
    low = (diag - high.astype(F32)).astype(BF)
    current_low = current.astype(BF)
    for peer in range(send_ref.shape[0]):
        send_ref[peer, 0] = current_low
        send_ref[peer, 1] = high
        send_ref[peer, 2] = low


def halves_of(z, width):
    half = z % 2
    near = pl.ds(pl.multiple_of(half * width, width), width)
    far = pl.ds(pl.multiple_of((1 - half) * width, width), width)
    return near, far


def slabs(rows_at, send_ref):
    z, _, _ = place()
    chips, count, _, width = send_ref.shape
    near, far = halves_of(z, width)
    for k in range(count):
        if k < count - 2:
            slab = rows_at(k, near)
        else:
            slab = rows_at((z // 2) * 2 + k - (count - 2), far)
        for chip in range(chips):
            send_ref[chip, k] = slab


def spreading_kernel(begun_ref, send_ref):
    slabs(lambda k, cut: begun_ref[k, 0, :, cut], send_ref)


def product_kernel(
    coupling_ref, mine_ref, theirs_ref, left_a, right_a, left_b, right_b, square_ref,
    send_ref, total, rows, lefts, rights, halves, sems,
):
    z, chip, core = place()
    target = (z // 2) * 2 + core
    block, width = total.shape[0], rows.shape[-1]
    pairs = left_a.shape[0]
    cut, _ = halves_of(z, width)

    def operators(pair):
        return [
            pltpu.make_async_copy(left_a.at[pair], lefts.at[pair, 0], sems.at[pair, 0]),
            pltpu.make_async_copy(left_b.at[pair], lefts.at[pair, 1], sems.at[pair, 1]),
            pltpu.make_async_copy(
                right_a.at[pair, :, cut], rights.at[pair, :, :width], sems.at[pair, 2]
            ),
            pltpu.make_async_copy(
                right_b.at[pair, :, cut], rights.at[pair, :, width:], sems.at[pair, 3]
            ),
        ]

    for pair in range(pairs):
        for copy in operators(pair):
            copy.start()
    for k in range(rows.shape[0]):
        for at in range(mine_ref.shape[0]):
            rows[k, 2 * at + core] = mine_ref[at, k]
            rows[k, 2 * at + 1 - core] = theirs_ref[at, k]
    total[...] = jnp.zeros_like(total)

    def first(pair):
        for copy in operators(pair):
            copy.wait()
        for j, owner in enumerate((core, 1 - core)):
            source = coupling_ref[target, (chip * 2 + owner) * pairs + pair]
            vector = rows[source].reshape(block, width)
            half = jnp.dot(lefts[pair, j], vector, preferred_element_type=F32)
            halves[pair % 2, :, j * width : (j + 1) * width] = half.astype(BF)

    def second(pair):
        total[...] += lax.dot_general(
            halves[pair % 2], rights[pair], (((1,), (1,)), ((), ())), preferred_element_type=F32
        )

    def both(pair, _):
        second(pair - 1)
        first(pair)
        return 0

    first(0)
    lax.fori_loop(1, pairs, both, 0)
    second(pairs - 1)

    near, far = halves_of(z, width)
    here = rows[target].reshape(block, width).astype(F32)
    there = rows[rows.shape[0] - 2 + core].reshape(block, width).astype(F32)
    product = jnp.sum(here * total[:, near] + there * total[:, far])
    extra = three_way(product, square_ref[0, 0])
    for peer in range(send_ref.shape[0]):
        stacked(send_ref, peer, total[peer * 32 : (peer + 1) * 32, :].astype(BF))
        send_ref[peer, block // 4 :, :] = extra


def products(coupling, mine, theirs, left, right, left_other, right_other, square):
    pairs, block, _ = left.shape
    chips, count, share, width = mine.shape
    return pl.pallas_call(
        product_kernel,
        in_specs=[SMEM, VMEM, VMEM, HBM, HBM, HBM, HBM, VMEM],
        out_specs=VMEM,
        scratch_shapes=[
            pltpu.VMEM((block, block), F32),
            pltpu.VMEM((count, 2 * chips, share, width), BF),
            pltpu.VMEM((pairs, 2, block, block), BF),
            pltpu.VMEM((pairs, block, 2 * width), BF),
            pltpu.VMEM((2, block, 2 * width), BF),
            pltpu.SemaphoreType.DMA((pairs, 4)),
        ],
        out_shape=jax.ShapeDtypeStruct((chips, block // 4 + 16, LANES), BF),
        compiler_params=pltpu.CompilerParams(vmem_limit_bytes=28 << 20),
        name="products",
    )(coupling, mine, theirs, left, right, left_other, right_other, square)


def joining_kernel(sizes_ref, arrived_ref, send_ref):
    z, chip, core = place()
    total = arrived_ref[0].astype(F32)
    for peer in range(1, arrived_ref.shape[0]):
        total = total + arrived_ref[peer].astype(F32)
    end = total.shape[0] - 16
    sigma = unstacked(total[:end], 32)
    inside = live(sigma.shape, chip * 32, sizes_ref[(z // 2) * 2 + core])
    low = jnp.where(inside, sigma, 0.0).astype(BF)
    extra = three_way(*two_sums(total[end:]))
    for peer in range(send_ref.shape[0]):
        at = (peer % 2) * SHARE
        stacked(send_ref, peer, low[at : at + SHARE])
        send_ref[peer, end // 2 :, :] = extra


def scalars_of(arrived_ref):
    at = arrived_ref.shape[1] - 16
    total = arrived_ref[0, at:].astype(F32)
    for peer in range(1, arrived_ref.shape[0]):
        total = total + arrived_ref[peer, at:].astype(F32)
    return two_sums(total)


def sigma_of(arrived_ref, target):
    end = arrived_ref.shape[1] - 16
    at = (target // 2) * 4 + target % 2
    both = arrived_ref[at, :end].astype(F32) + arrived_ref[at + 2, :end].astype(F32)
    return unstacked(both, SHARE)


def corrected(current, sigma, diag, theta):
    gap = diag - theta
    return current - (sigma - theta * current) * gap / (gap * gap + 1.0)


def middle_kernel(
    arrived_ref, begun_ref, current_ref, diag_ref,
    send_ref, all_ref, own_ref, square_ref, theta_ref, low_ref,
):
    z, _, _ = place()
    first, second = scalars_of(arrived_ref)
    theta = first / (second + 1e-6)
    theta_ref[...] = jnp.broadcast_to(theta, (8, LANES))
    for k in range(all_ref.shape[0]):
        diag = begun_ref[k, 1].astype(F32) + begun_ref[k, 2].astype(F32)
        update = corrected(begun_ref[k, 0].astype(F32), sigma_of(arrived_ref, k), diag, theta)
        all_ref[k] = update
        low_ref[k] = update.astype(BF)
    own = corrected(current_ref[...], sigma_of(arrived_ref, z), diag_ref[0], theta)
    own_ref[...] = own
    square_ref[...] = jnp.full((8, LANES), jnp.sum(own * own), F32)
    slabs(lambda k, cut: low_ref[k, :, cut], send_ref)


def closing_kernel(
    entries, arrived_ref, begun_ref, all_ref, own_ref, diag_ref, before_ref,
    final_ref, send_ref, theta_ref,
):
    z, _, _ = place()
    first, second = scalars_of(arrived_ref)
    scale = lax.rsqrt(second / entries + 1e-6)
    squared = scale * scale
    theta = squared * first / (squared * second + 1e-6)
    lane = lax.broadcasted_iota(jnp.int32, (8, LANES), 1)
    theta_ref[...] = jnp.where(lane == 0, before_ref[...], theta)
    total = jnp.zeros(all_ref.shape[1:], F32)
    for k in range(all_ref.shape[0]):
        diag = begun_ref[k, 1].astype(F32) + begun_ref[k, 2].astype(F32)
        update = corrected(scale * all_ref[k], scale * sigma_of(arrived_ref, k), diag, theta)
        total = total + update * update
    sigma = sigma_of(arrived_ref, z)
    final_ref[...] = corrected(scale * own_ref[...], scale * sigma, diag_ref[0], theta)
    send_ref[...] = jnp.full(send_ref.shape, jnp.sum(total), F32)


def scaling_kernel(entries, arrived_ref, final_ref, vector_ref):
    total = arrived_ref[0]
    for peer in range(1, arrived_ref.shape[0]):
        total = total + arrived_ref[peer]
    vector_ref[0] = final_ref[...] * lax.rsqrt(total[0:1, 0:1] / entries + 1e-6)


def call(kernel, shapes, specs, name, scratch=(), limit=16):
    return pl.pallas_call(
        kernel,
        in_specs=specs,
        out_specs=[VMEM] * len(shapes),
        out_shape=[jax.ShapeDtypeStruct(s, t) for s, t in shapes],
        scratch_shapes=scratch,
        compiler_params=pltpu.CompilerParams(vmem_limit_bytes=limit << 20),
        name=name,
    )


def shards(wavefunction, diagonal, left_blocks, right_blocks, coupling, sector_sizes):
    _, share, block = wavefunction.shape
    sectors = lax.axis_size("sector")
    chips = lax.axis_size("op_0") * lax.axis_size("op_1")
    width = block // 2
    left_blocks = pltpu.with_memory_space_constraint(left_blocks, pltpu.HBM)
    right_blocks = pltpu.with_memory_space_constraint(right_blocks, pltpu.HBM)
    entries = float(sectors * block * block)
    left_other = other_core(left_blocks)
    right_other = other_core(right_blocks)
    spread = ((chips, sectors + 2, share, width), BF)
    scalar = ((8, LANES), F32)

    begin, current, square = call(
        opening_kernel,
        [((sectors, 3, share, block), BF), ((share, block), F32), scalar],
        [SMEM, VMEM, VMEM],
        "opening",
        limit=60,
    )(sector_sizes, wavefunction, diagonal)
    begun = swap_all(begin, "sector")
    (outgoing,) = call(spreading_kernel, [spread], [VMEM], "spreading")(begun)

    def sigma_step(outgoing, square):
        mine = swap_all(outgoing, CHIP)
        send = products(
            coupling, mine, other_core(mine),
            left_blocks, right_blocks, left_other, right_other, square,
        )
        (send,) = call(
            joining_kernel,
            [((sectors * 2, block // 8 + 16, LANES), BF)],
            [SMEM, VMEM],
            "joining",
        )(sector_sizes, swap_all(send, CHIP))
        return swap_all(send, COLUMN)

    arrived = sigma_step(outgoing, square)
    outgoing, everyone, own, square, theta = call(
        middle_kernel,
        [spread, ((sectors, share, block), F32), ((share, block), F32), scalar, scalar],
        [VMEM] * 4,
        "middle",
        [pltpu.VMEM((sectors, share, block), BF)],
    )(arrived, begun, current, diagonal)

    arrived = sigma_step(outgoing, square)
    final, send, thetas = call(
        functools.partial(closing_kernel, entries),
        [((share, block), F32), ((chips * 2, 8, LANES), F32), scalar],
        [VMEM] * 6,
        "closing",
    )(arrived, begun, everyone, own, diagonal, theta)
    (vector,) = call(
        functools.partial(scaling_kernel, entries),
        [((1, share, block), F32)],
        [VMEM] * 2,
        "scaling",
    )(swap_all(send, OP), final)
    return vector, thetas[0, :2]


def solution(mesh):
    split = Mesh(
        mesh.devices.reshape(mesh.shape["sector"], 4, 4, 2), ("sector", "op_0", "op_1", "op_2")
    )
    in_specs = (
        P("sector", OP, None),
        P("sector", OP, None),
        P(OP, None, None),
        P(OP, None, None),
        P(),
        P(),
    )
    out_specs = (P("sector", OP, None), P())
    return jax.shard_map(
        shards, mesh=split, in_specs=in_specs, out_specs=out_specs, check_vma=False
    )
```

```python
import functools
import jax
import jax.numpy as jnp
from jax import lax
from jax.experimental import pallas as pl
from jax.experimental.pallas import tpu as pltpu
from jax.sharding import Mesh
from jax.sharding import PartitionSpec as P

OP = ("op_0", "op_1", "op_2")
CHIP = ("op_0", "op_1")
CORE = "op_2"
COLUMN = ("sector", "op_2")
BF = jnp.bfloat16
F32 = jnp.float32
VMEM = pl.BlockSpec(memory_space=pltpu.VMEM)
SMEM = pl.BlockSpec(memory_space=pltpu.SMEM)
HBM = pl.BlockSpec(memory_space=pltpu.HBM)
SHARE = 16
LANES = 128
AHEAD = 3


def swap_all(x, axes):
    return lax.all_to_all(x, axes, split_axis=0, concat_axis=0, tiled=True)


def other_core(x):
    return lax.ppermute(x, CORE, [(0, 1), (1, 0)])


def three_way(first, second):
    row = lax.broadcasted_iota(jnp.int32, (16, 128), 0)
    value = jnp.where(row < 3, first, second)
    high = value.astype(BF).astype(F32)
    middle = (value - high).astype(BF).astype(F32)
    low = value - high - middle
    part = jnp.where(row < 3, row, row - 3)
    return jnp.where(part == 0, high, jnp.where(part == 1, middle, low)).astype(BF)


def two_sums(tile):
    first = tile[0:1] + tile[1:2] + tile[2:3]
    second = tile[3:4] + tile[4:5] + tile[5:6]
    return first[:, :1], second[:, :1]


def place():
    z = lax.axis_index("sector")
    chip = lax.axis_index("op_0") * lax.axis_size("op_1") + lax.axis_index("op_1")
    return z, chip, lax.axis_index(CORE)


def live(shape, first_row, size):
    row = lax.broadcasted_iota(jnp.int32, shape, 0) + first_row
    column = lax.broadcasted_iota(jnp.int32, shape, 1)
    return (row < size) & (column < size)


def stacked(ref, lead, tile):
    rows, block = tile.shape
    for j in range(block // LANES):
        ref[lead, j * rows : (j + 1) * rows, :] = tile[:, j * LANES : (j + 1) * LANES]


def unstacked(value, rows):
    parts = value.shape[0] // rows
    return jnp.concatenate([value[j * rows : (j + 1) * rows] for j in range(parts)], axis=1)


def opening_kernel(sizes_ref, wave_ref, diag_ref, send_ref, current_ref, square_ref):
    z, chip, core = place()
    wave = wave_ref[0]
    inside = live(wave.shape, (chip * 2 + core) * SHARE, sizes_ref[z])
    current = jnp.where(inside, wave, 0.0)
    current_ref[...] = current
    square_ref[...] = jnp.full((8, LANES), jnp.sum(current * current), F32)
    diag = diag_ref[0]
    high = diag.astype(BF)
    low = (diag - high.astype(F32)).astype(BF)
    current_low = current.astype(BF)
    for peer in range(send_ref.shape[0]):
        send_ref[peer, 0] = current_low
        send_ref[peer, 1] = high
        send_ref[peer, 2] = low


def halves_of(z, width):
    half = z % 2
    near = pl.ds(pl.multiple_of(half * width, width), width)
    far = pl.ds(pl.multiple_of((1 - half) * width, width), width)
    return near, far


def slabs(rows_at, send_ref):
    z, _, _ = place()
    chips, count, _, width = send_ref.shape
    near, far = halves_of(z, width)
    for k in range(count):
        if k < count - 2:
            slab = rows_at(k, near)
        else:
            slab = rows_at((z // 2) * 2 + k - (count - 2), far)
        for chip in range(chips):
            send_ref[chip, k] = slab


def spreading_kernel(begun_ref, send_ref):
    slabs(lambda k, cut: begun_ref[k, 0, :, cut], send_ref)


def product_kernel(
    coupling_ref, mine_ref, theirs_ref, left_a, left_b, right_a, right_b, square_ref,
    send_ref, total, rows, lefts, rights, halves, sems,
):
    z, chip, core = place()
    target = (z // 2) * 2 + core
    block, width = total.shape[0], rows.shape[-1]
    pairs = left_a.shape[0]
    near, far = halves_of(z, width)

    def fetches(pair):
        return [
            pltpu.make_async_copy(
                right.at[pair, :, near], rights.at[pair, :, side], sems.at[pair, j]
            )
            for j, (right, side) in enumerate(
                ((right_a, slice(0, width)), (right_b, slice(width, 2 * width)))
            )
        ] + [pltpu.make_async_copy(left_b.at[pair], lefts.at[pair], sems.at[pair, 2])]

    def fetch(pair):
        for copy in fetches(pair):
            copy.start()

    def fetched(pair):
        for copy in fetches(pair):
            copy.wait()

    for pair in range(AHEAD):
        fetch(pair)
    for k in range(rows.shape[0]):
        for at in range(mine_ref.shape[0]):
            rows[k, 2 * at + core] = mine_ref[at, k]
            rows[k, 2 * at + 1 - core] = theirs_ref[at, k]
    total[...] = jnp.zeros_like(total)

    def first(pair):
        for j, (owner, left) in enumerate(((core, left_a), (1 - core, lefts))):
            source = coupling_ref[target, (chip * 2 + owner) * pairs + pair]
            vector = rows[source].reshape(block, width)
            half = jnp.dot(left[pair], vector, preferred_element_type=F32)
            halves[pair % 2, :, j * width : (j + 1) * width] = half.astype(BF)

    def second(pair):
        total[...] += lax.dot_general(
            halves[pair % 2], rights[pair], (((1,), (1,)), ((), ())), preferred_element_type=F32
        )

    def both(pair, _):
        fetched(pair)

        @pl.when(pair + AHEAD < pairs)
        def _():
            fetch(pair + AHEAD)

        second(pair - 1)
        first(pair)
        return 0

    fetched(0)
    fetch(AHEAD)
    first(0)
    lax.fori_loop(1, pairs, both, 0)
    second(pairs - 1)

    here = rows[target].reshape(block, width).astype(F32)
    there = rows[rows.shape[0] - 2 + core].reshape(block, width).astype(F32)
    product = jnp.sum(here * total[:, near] + there * total[:, far])
    extra = three_way(product, square_ref[0, 0])
    for peer in range(send_ref.shape[0]):
        stacked(send_ref, peer, total[peer * 32 : (peer + 1) * 32, :].astype(BF))
        send_ref[peer, block // 4 :, :] = extra


def products(coupling, mine, theirs, left, right, left_other, right_other, square):
    pairs, block, _ = left.shape
    chips, count, share, width = mine.shape
    return pl.pallas_call(
        product_kernel,
        in_specs=[SMEM, VMEM, VMEM, VMEM, HBM, HBM, HBM, VMEM],
        out_specs=VMEM,
        scratch_shapes=[
            pltpu.VMEM((block, block), F32),
            pltpu.VMEM((count, 2 * chips, share, width), BF),
            pltpu.VMEM((pairs, block, block), BF),
            pltpu.VMEM((pairs, block, 2 * width), BF),
            pltpu.VMEM((2, block, 2 * width), BF),
            pltpu.SemaphoreType.DMA((pairs, 3)),
        ],
        out_shape=jax.ShapeDtypeStruct((chips, block // 4 + 16, LANES), BF),
        compiler_params=pltpu.CompilerParams(vmem_limit_bytes=28 << 20),
        name="products",
    )(coupling, mine, theirs, left, left_other, right, right_other, square)


def joining_kernel(sizes_ref, arrived_ref, send_ref):
    z, chip, core = place()
    total = arrived_ref[0].astype(F32)
    for peer in range(1, arrived_ref.shape[0]):
        total = total + arrived_ref[peer].astype(F32)
    end = total.shape[0] - 16
    sigma = unstacked(total[:end], 32)
    inside = live(sigma.shape, chip * 32, sizes_ref[(z // 2) * 2 + core])
    low = jnp.where(inside, sigma, 0.0).astype(BF)
    extra = three_way(*two_sums(total[end:]))
    for peer in range(send_ref.shape[0]):
        at = (peer % 2) * SHARE
        stacked(send_ref, peer, low[at : at + SHARE])
        send_ref[peer, end // 2 :, :] = extra


def scalars_of(arrived_ref):
    at = arrived_ref.shape[1] - 16
    total = arrived_ref[0, at:].astype(F32)
    for peer in range(1, arrived_ref.shape[0]):
        total = total + arrived_ref[peer, at:].astype(F32)
    return two_sums(total)


def sigma_of(arrived_ref, target):
    end = arrived_ref.shape[1] - 16
    at = (target // 2) * 4 + target % 2
    both = arrived_ref[at, :end].astype(F32) + arrived_ref[at + 2, :end].astype(F32)
    return unstacked(both, SHARE)


def corrected(current, sigma, diag, theta):
    gap = diag - theta
    return current - (sigma - theta * current) * gap / (gap * gap + 1.0)


def middle_kernel(
    arrived_ref, begun_ref, current_ref, diag_ref,
    send_ref, all_ref, own_ref, square_ref, theta_ref, low_ref,
):
    z, _, _ = place()
    first, second = scalars_of(arrived_ref)
    theta = first / (second + 1e-6)
    theta_ref[...] = jnp.broadcast_to(theta, (8, LANES))
    for k in range(all_ref.shape[0]):
        diag = begun_ref[k, 1].astype(F32) + begun_ref[k, 2].astype(F32)
        update = corrected(begun_ref[k, 0].astype(F32), sigma_of(arrived_ref, k), diag, theta)
        all_ref[k] = update
        low_ref[k] = update.astype(BF)
    own = corrected(current_ref[...], sigma_of(arrived_ref, z), diag_ref[0], theta)
    own_ref[...] = own
    square_ref[...] = jnp.full((8, LANES), jnp.sum(own * own), F32)
    slabs(lambda k, cut: low_ref[k, :, cut], send_ref)


def closing_kernel(
    entries, arrived_ref, begun_ref, all_ref, own_ref, diag_ref, before_ref,
    final_ref, send_ref, theta_ref,
):
    z, _, _ = place()
    first, second = scalars_of(arrived_ref)
    scale = lax.rsqrt(second / entries + 1e-6)
    squared = scale * scale
    theta = squared * first / (squared * second + 1e-6)
    lane = lax.broadcasted_iota(jnp.int32, (8, LANES), 1)
    theta_ref[...] = jnp.where(lane == 0, before_ref[...], theta)
    total = jnp.zeros(all_ref.shape[1:], F32)
    for k in range(all_ref.shape[0]):
        diag = begun_ref[k, 1].astype(F32) + begun_ref[k, 2].astype(F32)
        update = corrected(scale * all_ref[k], scale * sigma_of(arrived_ref, k), diag, theta)
        total = total + update * update
    sigma = sigma_of(arrived_ref, z)
    final_ref[...] = corrected(scale * own_ref[...], scale * sigma, diag_ref[0], theta)
    send_ref[...] = jnp.full(send_ref.shape, jnp.sum(total), F32)


def scaling_kernel(entries, arrived_ref, final_ref, vector_ref):
    total = arrived_ref[0]
    for peer in range(1, arrived_ref.shape[0]):
        total = total + arrived_ref[peer]
    vector_ref[0] = final_ref[...] * lax.rsqrt(total[0:1, 0:1] / entries + 1e-6)


def call(kernel, shapes, specs, name, scratch=(), limit=16):
    return pl.pallas_call(
        kernel,
        in_specs=specs,
        out_specs=[VMEM] * len(shapes),
        out_shape=[jax.ShapeDtypeStruct(s, t) for s, t in shapes],
        scratch_shapes=scratch,
        compiler_params=pltpu.CompilerParams(vmem_limit_bytes=limit << 20),
        name=name,
    )


def shards(wavefunction, diagonal, left_blocks, right_blocks, coupling, sector_sizes):
    _, share, block = wavefunction.shape
    sectors = lax.axis_size("sector")
    chips = lax.axis_size("op_0") * lax.axis_size("op_1")
    width = block // 2
    right_blocks = pltpu.with_memory_space_constraint(right_blocks, pltpu.HBM)
    entries = float(sectors * block * block)
    left_other = other_core(left_blocks)
    right_other = other_core(right_blocks)
    spread = ((chips, sectors + 2, share, width), BF)
    scalar = ((8, LANES), F32)

    begin, current, square = call(
        opening_kernel,
        [((sectors, 3, share, block), BF), ((share, block), F32), scalar],
        [SMEM, VMEM, VMEM],
        "opening",
        limit=60,
    )(sector_sizes, wavefunction, diagonal)
    begun = swap_all(begin, "sector")
    (outgoing,) = call(spreading_kernel, [spread], [VMEM], "spreading")(begun)

    def sigma_step(outgoing, square):
        mine = swap_all(outgoing, CHIP)
        send = products(
            coupling, mine, other_core(mine),
            left_blocks, right_blocks, left_other, right_other, square,
        )
        (send,) = call(
            joining_kernel,
            [((sectors * 2, block // 8 + 16, LANES), BF)],
            [SMEM, VMEM],
            "joining",
        )(sector_sizes, swap_all(send, CHIP))
        return swap_all(send, COLUMN)

    arrived = sigma_step(outgoing, square)
    outgoing, everyone, own, square, theta = call(
        middle_kernel,
        [spread, ((sectors, share, block), F32), ((share, block), F32), scalar, scalar],
        [VMEM] * 4,
        "middle",
        [pltpu.VMEM((sectors, share, block), BF)],
    )(arrived, begun, current, diagonal)

    arrived = sigma_step(outgoing, square)
    final, send, thetas = call(
        functools.partial(closing_kernel, entries),
        [((share, block), F32), ((chips * 2, 8, LANES), F32), scalar],
        [VMEM] * 6,
        "closing",
    )(arrived, begun, everyone, own, diagonal, theta)
    (vector,) = call(
        functools.partial(scaling_kernel, entries),
        [((1, share, block), F32)],
        [VMEM] * 2,
        "scaling",
    )(swap_all(send, OP), final)
    return vector, thetas[0, :2]


def solution(mesh):
    split = Mesh(
        mesh.devices.reshape(mesh.shape["sector"], 4, 4, 2), ("sector", "op_0", "op_1", "op_2")
    )
    in_specs = (
        P("sector", OP, None),
        P("sector", OP, None),
        P(OP, None, None),
        P(OP, None, None),
        P(),
        P(),
    )
    out_specs = (P("sector", OP, None), P())
    return jax.shard_map(
        shards, mesh=split, in_specs=in_specs, out_specs=out_specs, check_vma=False
    )
```

```python
import functools
import jax
import jax.numpy as jnp
from jax import lax
from jax.experimental import pallas as pl
from jax.experimental.pallas import tpu as pltpu
from jax.sharding import Mesh
from jax.sharding import PartitionSpec as P

OP = ("op_0", "op_1", "op_2")
CHIP = ("op_0", "op_1")
CORE = "op_2"
COLUMN = ("sector", "op_2")
BF = jnp.bfloat16
F32 = jnp.float32
VMEM = pl.BlockSpec(memory_space=pltpu.VMEM)
SMEM = pl.BlockSpec(memory_space=pltpu.SMEM)
HBM = pl.BlockSpec(memory_space=pltpu.HBM)
SHARE = 16
LANES = 128


def swap_all(x, axes):
    return lax.all_to_all(x, axes, split_axis=0, concat_axis=0, tiled=True)


def other_core(x):
    return lax.ppermute(x, CORE, [(0, 1), (1, 0)])


def three_way(first, second):
    row = lax.broadcasted_iota(jnp.int32, (16, 128), 0)
    value = jnp.where(row < 3, first, second)
    high = value.astype(BF).astype(F32)
    middle = (value - high).astype(BF).astype(F32)
    low = value - high - middle
    part = jnp.where(row < 3, row, row - 3)
    return jnp.where(part == 0, high, jnp.where(part == 1, middle, low)).astype(BF)


def two_sums(tile):
    first = tile[0:1] + tile[1:2] + tile[2:3]
    second = tile[3:4] + tile[4:5] + tile[5:6]
    return first[:, :1], second[:, :1]


def place():
    z = lax.axis_index("sector")
    chip = lax.axis_index("op_0") * lax.axis_size("op_1") + lax.axis_index("op_1")
    return z, chip, lax.axis_index(CORE)


def live(shape, first_row, size):
    row = lax.broadcasted_iota(jnp.int32, shape, 0) + first_row
    column = lax.broadcasted_iota(jnp.int32, shape, 1)
    return (row < size) & (column < size)


def stacked(ref, lead, tile):
    rows, block = tile.shape
    for j in range(block // LANES):
        ref[lead, j * rows : (j + 1) * rows, :] = tile[:, j * LANES : (j + 1) * LANES]


def unstacked(value, rows):
    parts = value.shape[0] // rows
    return jnp.concatenate([value[j * rows : (j + 1) * rows] for j in range(parts)], axis=1)


def opening_kernel(sizes_ref, wave_ref, diag_ref, send_ref, current_ref, square_ref):
    z, chip, core = place()
    wave = wave_ref[0]
    inside = live(wave.shape, (chip * 2 + core) * SHARE, sizes_ref[z])
    current = jnp.where(inside, wave, 0.0)
    current_ref[...] = current
    square_ref[...] = jnp.full((8, LANES), jnp.sum(current * current), F32)
    diag = diag_ref[0]
    high = diag.astype(BF)
    low = (diag - high.astype(F32)).astype(BF)
    current_low = current.astype(BF)
    for peer in range(send_ref.shape[0]):
        send_ref[peer, 0] = current_low
        send_ref[peer, 1] = high
        send_ref[peer, 2] = low


def halves_of(z, width):
    half = z % 2
    near = pl.ds(pl.multiple_of(half * width, width), width)
    far = pl.ds(pl.multiple_of((1 - half) * width, width), width)
    return near, far


def slabs(rows_at, send_ref):
    z, _, _ = place()
    chips, count, _, width = send_ref.shape
    near, far = halves_of(z, width)
    for k in range(count):
        if k < count - 2:
            slab = rows_at(k, near)
        else:
            slab = rows_at((z // 2) * 2 + k - (count - 2), far)
        for chip in range(chips):
            send_ref[chip, k] = slab


def spreading_kernel(begun_ref, send_ref):
    slabs(lambda k, cut: begun_ref[k, 0, :, cut], send_ref)


def product_kernel(
    coupling_ref, mine_ref, theirs_ref, left_a, left_b, right_a, right_b, square_ref,
    send_ref, total, rows, rights, halves, sems,
):
    z, chip, core = place()
    target = (z // 2) * 2 + core
    block, width = total.shape[0], rows.shape[-1]
    pairs = left_a.shape[0]
    near, far = halves_of(z, width)

    def fetch(pair):
        return pltpu.make_async_copy(right_a.at[pair, :, near], rights.at[pair], sems.at[pair])

    for pair in range(pairs):
        fetch(pair).start()
    for k in range(rows.shape[0]):
        for at in range(mine_ref.shape[0]):
            rows[k, 2 * at + core] = mine_ref[at, k]
            rows[k, 2 * at + 1 - core] = theirs_ref[at, k]
    total[...] = jnp.zeros_like(total)

    def first(pair):
        for j, (owner, left) in enumerate(((core, left_a), (1 - core, left_b))):
            source = coupling_ref[target, (chip * 2 + owner) * pairs + pair]
            vector = rows[source].reshape(block, width)
            half = jnp.dot(left[pair], vector, preferred_element_type=F32)
            halves[pair % 2, :, j * width : (j + 1) * width] = half.astype(BF)

    def second(pair):
        right = jnp.concatenate([rights[pair], right_b[pair, :, near]], axis=1)
        total[...] += lax.dot_general(
            halves[pair % 2], right, (((1,), (1,)), ((), ())), preferred_element_type=F32
        )

    def both(pair, _):
        fetch(pair - 1).wait()
        second(pair - 1)
        first(pair)
        return 0

    first(0)
    lax.fori_loop(1, pairs, both, 0)
    fetch(pairs - 1).wait()
    second(pairs - 1)

    here = rows[target].reshape(block, width).astype(F32)
    there = rows[rows.shape[0] - 2 + core].reshape(block, width).astype(F32)
    product = jnp.sum(here * total[:, near] + there * total[:, far])
    extra = three_way(product, square_ref[0, 0])
    for peer in range(send_ref.shape[0]):
        stacked(send_ref, peer, total[peer * 32 : (peer + 1) * 32, :].astype(BF))
        send_ref[peer, block // 4 :, :] = extra


def products(coupling, mine, theirs, left, right, left_other, right_other, square):
    pairs, block, _ = left.shape
    chips, count, share, width = mine.shape
    return pl.pallas_call(
        product_kernel,
        in_specs=[SMEM, VMEM, VMEM, VMEM, VMEM, HBM, VMEM, VMEM],
        out_specs=VMEM,
        scratch_shapes=[
            pltpu.VMEM((block, block), F32),
            pltpu.VMEM((count, 2 * chips, share, width), BF),
            pltpu.VMEM((pairs, block, width), BF),
            pltpu.VMEM((2, block, 2 * width), BF),
            pltpu.SemaphoreType.DMA((pairs,)),
        ],
        out_shape=jax.ShapeDtypeStruct((chips, block // 4 + 16, LANES), BF),
        compiler_params=pltpu.CompilerParams(vmem_limit_bytes=16 << 20),
        name="products",
    )(coupling, mine, theirs, left, left_other, right, right_other, square)


def joining_kernel(sizes_ref, arrived_ref, send_ref):
    z, chip, core = place()
    total = arrived_ref[0].astype(F32)
    for peer in range(1, arrived_ref.shape[0]):
        total = total + arrived_ref[peer].astype(F32)
    end = total.shape[0] - 16
    sigma = unstacked(total[:end], 32)
    inside = live(sigma.shape, chip * 32, sizes_ref[(z // 2) * 2 + core])
    low = jnp.where(inside, sigma, 0.0).astype(BF)
    extra = three_way(*two_sums(total[end:]))
    for peer in range(send_ref.shape[0]):
        at = (peer % 2) * SHARE
        stacked(send_ref, peer, low[at : at + SHARE])
        send_ref[peer, end // 2 :, :] = extra


def scalars_of(arrived_ref):
    at = arrived_ref.shape[1] - 16
    total = arrived_ref[0, at:].astype(F32)
    for peer in range(1, arrived_ref.shape[0]):
        total = total + arrived_ref[peer, at:].astype(F32)
    return two_sums(total)


def sigma_of(arrived_ref, target):
    end = arrived_ref.shape[1] - 16
    at = (target // 2) * 4 + target % 2
    both = arrived_ref[at, :end].astype(F32) + arrived_ref[at + 2, :end].astype(F32)
    return unstacked(both, SHARE)


def corrected(current, sigma, diag, theta):
    gap = diag - theta
    return current - (sigma - theta * current) * gap / (gap * gap + 1.0)


def middle_kernel(
    arrived_ref, begun_ref, current_ref, diag_ref,
    send_ref, all_ref, own_ref, square_ref, theta_ref, low_ref,
):
    z, _, _ = place()
    first, second = scalars_of(arrived_ref)
    theta = first / (second + 1e-6)
    theta_ref[...] = jnp.broadcast_to(theta, (8, LANES))
    for k in range(all_ref.shape[0]):
        diag = begun_ref[k, 1].astype(F32) + begun_ref[k, 2].astype(F32)
        update = corrected(begun_ref[k, 0].astype(F32), sigma_of(arrived_ref, k), diag, theta)
        all_ref[k] = update
        low_ref[k] = update.astype(BF)
    own = corrected(current_ref[...], sigma_of(arrived_ref, z), diag_ref[0], theta)
    own_ref[...] = own
    square_ref[...] = jnp.full((8, LANES), jnp.sum(own * own), F32)
    slabs(lambda k, cut: low_ref[k, :, cut], send_ref)


def closing_kernel(
    entries, arrived_ref, begun_ref, all_ref, own_ref, diag_ref, before_ref,
    final_ref, send_ref, theta_ref,
):
    z, _, _ = place()
    first, second = scalars_of(arrived_ref)
    scale = lax.rsqrt(second / entries + 1e-6)
    squared = scale * scale
    theta = squared * first / (squared * second + 1e-6)
    lane = lax.broadcasted_iota(jnp.int32, (8, LANES), 1)
    theta_ref[...] = jnp.where(lane == 0, before_ref[...], theta)
    total = jnp.zeros(all_ref.shape[1:], F32)
    for k in range(all_ref.shape[0]):
        diag = begun_ref[k, 1].astype(F32) + begun_ref[k, 2].astype(F32)
        update = corrected(scale * all_ref[k], scale * sigma_of(arrived_ref, k), diag, theta)
        total = total + update * update
    sigma = sigma_of(arrived_ref, z)
    final_ref[...] = corrected(scale * own_ref[...], scale * sigma, diag_ref[0], theta)
    send_ref[...] = jnp.full(send_ref.shape, jnp.sum(total), F32)


def scaling_kernel(entries, arrived_ref, final_ref, vector_ref):
    total = arrived_ref[0]
    for peer in range(1, arrived_ref.shape[0]):
        total = total + arrived_ref[peer]
    vector_ref[0] = final_ref[...] * lax.rsqrt(total[0:1, 0:1] / entries + 1e-6)


def call(kernel, shapes, specs, name, scratch=(), limit=16):
    return pl.pallas_call(
        kernel,
        in_specs=specs,
        out_specs=[VMEM] * len(shapes),
        out_shape=[jax.ShapeDtypeStruct(s, t) for s, t in shapes],
        scratch_shapes=scratch,
        compiler_params=pltpu.CompilerParams(vmem_limit_bytes=limit << 20),
        name=name,
    )


def shards(wavefunction, diagonal, left_blocks, right_blocks, coupling, sector_sizes):
    _, share, block = wavefunction.shape
    sectors = lax.axis_size("sector")
    chips = lax.axis_size("op_0") * lax.axis_size("op_1")
    width = block // 2
    left_other = other_core(left_blocks)
    right_other = other_core(right_blocks)
    wavefunction, diagonal, sector_sizes, right_blocks = (
        pltpu.with_memory_space_constraint(x, pltpu.HBM)
        for x in (wavefunction, diagonal, sector_sizes, right_blocks)
    )
    entries = float(sectors * block * block)
    spread = ((chips, sectors + 2, share, width), BF)
    scalar = ((8, LANES), F32)

    begin, current, square = call(
        opening_kernel,
        [((sectors, 3, share, block), BF), ((share, block), F32), scalar],
        [SMEM, VMEM, VMEM],
        "opening",
    )(sector_sizes, wavefunction, diagonal)
    begun = swap_all(begin, "sector")
    (outgoing,) = call(spreading_kernel, [spread], [VMEM], "spreading")(begun)

    def sigma_step(outgoing, square):
        mine = swap_all(outgoing, CHIP)
        send = products(
            coupling, mine, other_core(mine),
            left_blocks, right_blocks, left_other, right_other, square,
        )
        (send,) = call(
            joining_kernel,
            [((sectors * 2, block // 8 + 16, LANES), BF)],
            [SMEM, VMEM],
            "joining",
        )(sector_sizes, swap_all(send, CHIP))
        return swap_all(send, COLUMN)

    arrived = sigma_step(outgoing, square)
    outgoing, everyone, own, square, theta = call(
        middle_kernel,
        [spread, ((sectors, share, block), F32), ((share, block), F32), scalar, scalar],
        [VMEM] * 4,
        "middle",
        [pltpu.VMEM((sectors, share, block), BF)],
    )(arrived, begun, current, diagonal)

    arrived = sigma_step(outgoing, square)
    final, send, thetas = call(
        functools.partial(closing_kernel, entries),
        [((share, block), F32), ((chips * 2, 8, LANES), F32), scalar],
        [VMEM] * 6,
        "closing",
    )(arrived, begun, everyone, own, diagonal, theta)
    (vector,) = call(
        functools.partial(scaling_kernel, entries),
        [((1, share, block), F32)],
        [VMEM] * 2,
        "scaling",
    )(swap_all(send, OP), final)
    return vector, thetas[0, :2]


def solution(mesh):
    split = Mesh(
        mesh.devices.reshape(mesh.shape["sector"], 4, 4, 2), ("sector", "op_0", "op_1", "op_2")
    )
    in_specs = (
        P("sector", OP, None),
        P("sector", OP, None),
        P(OP, None, None),
        P(OP, None, None),
        P(),
        P(),
    )
    out_specs = (P("sector", OP, None), P())
    return jax.shard_map(
        shards, mesh=split, in_specs=in_specs, out_specs=out_specs, check_vma=False
    )
```

```python
import functools
import jax
import jax.numpy as jnp
from jax import lax
from jax.experimental import pallas as pl
from jax.experimental.pallas import tpu as pltpu
from jax.sharding import Mesh
from jax.sharding import PartitionSpec as P

OP = ("op_0", "op_1", "op_2")
CHIP = ("op_0", "op_1")
CORE = "op_2"
COLUMN = ("sector", "op_2")
BF = jnp.bfloat16
F32 = jnp.float32
VMEM = pl.BlockSpec(memory_space=pltpu.VMEM)
SMEM = pl.BlockSpec(memory_space=pltpu.SMEM)
HBM = pl.BlockSpec(memory_space=pltpu.HBM)
SHARE = 16
LANES = 128
TILE = 8


def swap_all(x, axes):
    return lax.all_to_all(x, axes, split_axis=0, concat_axis=0, tiled=True)


def other_core(x):
    return lax.ppermute(x, CORE, [(0, 1), (1, 0)])


def three_way(first, second):
    row = lax.broadcasted_iota(jnp.int32, (TILE, LANES), 0)
    value = jnp.where(row < 3, first, second)
    high = value.astype(BF).astype(F32)
    middle = (value - high).astype(BF).astype(F32)
    low = value - high - middle
    part = jnp.where(row < 3, row, row - 3)
    return jnp.where(part == 0, high, jnp.where(part == 1, middle, low)).astype(BF)


def two_sums(tile):
    first = tile[0:1] + tile[1:2] + tile[2:3]
    second = tile[3:4] + tile[4:5] + tile[5:6]
    return first[:, :1], second[:, :1]


def place():
    z = lax.axis_index("sector")
    chip = lax.axis_index("op_0") * lax.axis_size("op_1") + lax.axis_index("op_1")
    return z, chip, lax.axis_index(CORE)


def live(shape, first_row, size):
    row = lax.broadcasted_iota(jnp.int32, shape, 0) + first_row
    column = lax.broadcasted_iota(jnp.int32, shape, 1)
    return (row < size) & (column < size)


def stacked(ref, lead, tile):
    rows, block = tile.shape
    for j in range(block // LANES):
        ref[lead, j * rows : (j + 1) * rows, :] = tile[:, j * LANES : (j + 1) * LANES]


def unstacked(value, rows):
    parts = value.shape[0] // rows
    return jnp.concatenate([value[j * rows : (j + 1) * rows] for j in range(parts)], axis=1)


def opening_kernel(sizes_ref, wave_ref, diag_ref, send_ref, current_ref, square_ref):
    z, chip, core = place()
    wave = wave_ref[0]
    inside = live(wave.shape, (chip * 2 + core) * SHARE, sizes_ref[z])
    current = jnp.where(inside, wave, 0.0)
    current_ref[...] = current
    square_ref[...] = jnp.full((8, LANES), jnp.sum(current * current), F32)
    diag = diag_ref[0]
    high = diag.astype(BF)
    low = (diag - high.astype(F32)).astype(BF)
    current_low = current.astype(BF)
    for peer in range(send_ref.shape[0]):
        send_ref[peer, 0] = current_low
        send_ref[peer, 1] = high
        send_ref[peer, 2] = low


def halves_of(z, width):
    half = z % 2
    near = pl.ds(pl.multiple_of(half * width, width), width)
    far = pl.ds(pl.multiple_of((1 - half) * width, width), width)
    return near, far


def slabs(rows_at, send_ref):
    z, _, _ = place()
    chips, count, _, width = send_ref.shape
    near, far = halves_of(z, width)
    for k in range(count):
        if k < count - 2:
            slab = rows_at(k, near)
        else:
            slab = rows_at((z // 2) * 2 + k - (count - 2), far)
        for chip in range(chips):
            send_ref[chip, k] = slab


def spreading_kernel(begun_ref, send_ref):
    slabs(lambda k, cut: begun_ref[k, 0, :, cut], send_ref)


def product_kernel(
    coupling_ref, mine_ref, theirs_ref, left_a, left_b, right_a, right_b, square_ref,
    send_ref, total, rows, rights, halves, sems,
):
    z, chip, core = place()
    target = (z // 2) * 2 + core
    block, width = total.shape[0], rows.shape[-1]
    pairs = left_a.shape[0]
    near, far = halves_of(z, width)

    def fetch(pair):
        return pltpu.make_async_copy(right_a.at[pair, :, near], rights.at[pair], sems.at[pair])

    fetch(0).start()
    for k in range(rows.shape[0]):
        for at in range(mine_ref.shape[0]):
            rows[k, 2 * at + core] = mine_ref[at, k]
            rows[k, 2 * at + 1 - core] = theirs_ref[at, k]
    for pair in range(1, pairs):
        fetch(pair).start()
    total[...] = jnp.zeros_like(total)

    def first(pair):
        for j, (owner, left) in enumerate(((core, left_a), (1 - core, left_b))):
            source = coupling_ref[target, (chip * 2 + owner) * pairs + pair]
            vector = rows[source].reshape(block, width)
            half = jnp.dot(left[pair], vector, preferred_element_type=F32)
            halves[pair % 2, :, j * width : (j + 1) * width] = half.astype(BF)

    def second(pair):
        right = jnp.concatenate([rights[pair], right_b[pair, :, near]], axis=1)
        total[...] += lax.dot_general(
            halves[pair % 2], right, (((1,), (1,)), ((), ())), preferred_element_type=F32
        )

    def both(pair, _):
        fetch(pair - 1).wait()
        second(pair - 1)
        first(pair)
        return 0

    first(0)
    lax.fori_loop(1, pairs, both, 0)
    fetch(pairs - 1).wait()
    second(pairs - 1)

    here = rows[target].reshape(block, width).astype(F32)
    there = rows[rows.shape[0] - 2 + core].reshape(block, width).astype(F32)
    product = jnp.sum(here * total[:, near] + there * total[:, far])
    extra = three_way(product, square_ref[0, 0])
    for peer in range(send_ref.shape[0]):
        stacked(send_ref, peer, total[peer * 32 : (peer + 1) * 32, :].astype(BF))
        send_ref[peer, block // 4 :, :] = extra


def products(coupling, mine, theirs, left, right, left_other, right_other, square):
    pairs, block, _ = left.shape
    chips, count, share, width = mine.shape
    return pl.pallas_call(
        product_kernel,
        in_specs=[SMEM, VMEM, VMEM, VMEM, VMEM, HBM, VMEM, VMEM],
        out_specs=VMEM,
        scratch_shapes=[
            pltpu.VMEM((block, block), F32),
            pltpu.VMEM((count, 2 * chips, share, width), BF),
            pltpu.VMEM((pairs, block, width), BF),
            pltpu.VMEM((2, block, 2 * width), BF),
            pltpu.SemaphoreType.DMA((pairs,)),
        ],
        out_shape=jax.ShapeDtypeStruct((chips, block // 4 + TILE, LANES), BF),
        compiler_params=pltpu.CompilerParams(vmem_limit_bytes=16 << 20),
        name="products",
    )(coupling, mine, theirs, left, left_other, right, right_other, square)


def joining_kernel(sizes_ref, arrived_ref, send_ref):
    z, chip, core = place()
    total = arrived_ref[0].astype(F32)
    for peer in range(1, arrived_ref.shape[0]):
        total = total + arrived_ref[peer].astype(F32)
    end = total.shape[0] - TILE
    sigma = unstacked(total[:end], 32)
    inside = live(sigma.shape, chip * 32, sizes_ref[(z // 2) * 2 + core])
    low = jnp.where(inside, sigma, 0.0).astype(BF)
    extra = three_way(*two_sums(total[end:]))
    for peer in range(send_ref.shape[0]):
        at = (peer % 2) * SHARE
        stacked(send_ref, peer, low[at : at + SHARE])
        send_ref[peer, end // 2 :, :] = extra


def scalars_of(arrived_ref):
    at = arrived_ref.shape[1] - TILE
    total = arrived_ref[0, at:].astype(F32)
    for peer in range(1, arrived_ref.shape[0]):
        total = total + arrived_ref[peer, at:].astype(F32)
    return two_sums(total)


def sigma_of(arrived_ref, target):
    end = arrived_ref.shape[1] - TILE
    at = (target // 2) * 4 + target % 2
    both = arrived_ref[at, :end].astype(F32) + arrived_ref[at + 2, :end].astype(F32)
    return unstacked(both, SHARE)


def corrected(current, sigma, diag, theta):
    gap = diag - theta
    return current - (sigma - theta * current) * gap / (gap * gap + 1.0)


def middle_kernel(
    arrived_ref, begun_ref, current_ref, diag_ref,
    send_ref, all_ref, own_ref, square_ref, theta_ref, low_ref,
):
    z, _, _ = place()
    first, second = scalars_of(arrived_ref)
    theta = first / (second + 1e-6)
    theta_ref[0] = theta[0, 0]
    for k in range(all_ref.shape[0]):
        diag = begun_ref[k, 1].astype(F32) + begun_ref[k, 2].astype(F32)
        update = corrected(begun_ref[k, 0].astype(F32), sigma_of(arrived_ref, k), diag, theta)
        all_ref[k] = update
        low_ref[k] = update.astype(BF)
    own = corrected(current_ref[...], sigma_of(arrived_ref, z), diag_ref[0], theta)
    own_ref[...] = own
    square_ref[...] = jnp.full((8, LANES), jnp.sum(own * own), F32)
    slabs(lambda k, cut: low_ref[k, :, cut], send_ref)


def closing_kernel(
    entries, arrived_ref, begun_ref, all_ref, own_ref, diag_ref, before_ref,
    final_ref, send_ref, theta_ref,
):
    z, _, _ = place()
    first, second = scalars_of(arrived_ref)
    scale = lax.rsqrt(second / entries + 1e-6)
    squared = scale * scale
    theta = squared * first / (squared * second + 1e-6)
    theta_ref[0] = before_ref[0]
    theta_ref[1] = theta[0, 0]
    total = jnp.zeros(all_ref.shape[1:], F32)
    for k in range(all_ref.shape[0]):
        diag = begun_ref[k, 1].astype(F32) + begun_ref[k, 2].astype(F32)
        update = corrected(scale * all_ref[k], scale * sigma_of(arrived_ref, k), diag, theta)
        total = total + update * update
    sigma = sigma_of(arrived_ref, z)
    final_ref[...] = corrected(scale * own_ref[...], scale * sigma, diag_ref[0], theta)
    send_ref[...] = jnp.full(send_ref.shape, jnp.sum(total), F32)


def scaling_kernel(entries, arrived_ref, final_ref, vector_ref):
    total = arrived_ref[0]
    for peer in range(1, arrived_ref.shape[0]):
        total = total + arrived_ref[peer]
    vector_ref[0] = final_ref[...] * lax.rsqrt(total[0:1, 0:1] / entries + 1e-6)


def call(kernel, shapes, specs, name, scratch=(), outs=None):
    return pl.pallas_call(
        kernel,
        in_specs=specs,
        out_specs=outs or [VMEM] * len(shapes),
        out_shape=[jax.ShapeDtypeStruct(s, t) for s, t in shapes],
        scratch_shapes=scratch,
        compiler_params=pltpu.CompilerParams(vmem_limit_bytes=16 << 20),
        name=name,
    )


def shards(wavefunction, diagonal, left_blocks, right_blocks, coupling, sector_sizes):
    _, share, block = wavefunction.shape
    sectors = lax.axis_size("sector")
    chips = lax.axis_size("op_0") * lax.axis_size("op_1")
    width = block // 2
    left_other = other_core(left_blocks)
    right_other = other_core(right_blocks)
    opening_inputs = tuple(
        pltpu.with_memory_space_constraint(x, pltpu.HBM)
        for x in (sector_sizes, wavefunction, diagonal)
    )
    right_blocks = pltpu.with_memory_space_constraint(right_blocks, pltpu.HBM)
    entries = float(sectors * block * block)
    spread = ((chips, sectors + 2, share, width), BF)
    scalar = ((8, LANES), F32)

    begin, current, square = call(
        opening_kernel,
        [((sectors, 3, share, block), BF), ((share, block), F32), scalar],
        [SMEM, VMEM, VMEM],
        "opening",
    )(*opening_inputs)
    begun = swap_all(begin, "sector")
    (outgoing,) = call(spreading_kernel, [spread], [VMEM], "spreading")(begun)

    def sigma_step(outgoing, square):
        mine = swap_all(outgoing, CHIP)
        send = products(
            coupling, mine, other_core(mine),
            left_blocks, right_blocks, left_other, right_other, square,
        )
        (send,) = call(
            joining_kernel,
            [((sectors * 2, block // 8 + TILE, LANES), BF)],
            [SMEM, VMEM],
            "joining",
        )(sector_sizes, swap_all(send, CHIP))
        return swap_all(send, COLUMN)

    arrived = sigma_step(outgoing, square)
    outgoing, everyone, own, square, theta = call(
        middle_kernel,
        [spread, ((sectors, share, block), F32), ((share, block), F32), scalar, ((1,), F32)],
        [VMEM] * 4,
        "middle",
        [pltpu.VMEM((sectors, share, block), BF)],
        [VMEM, VMEM, VMEM, VMEM, SMEM],
    )(arrived, begun, current, diagonal)

    arrived = sigma_step(outgoing, square)
    final, send, thetas = call(
        functools.partial(closing_kernel, entries),
        [((share, block), F32), ((chips * 2, 8, LANES), F32), ((2,), F32)],
        [VMEM, VMEM, VMEM, VMEM, VMEM, SMEM],
        "closing",
        outs=[VMEM, VMEM, SMEM],
    )(arrived, begun, everyone, own, diagonal, theta)
    (vector,) = call(
        functools.partial(scaling_kernel, entries),
        [((1, share, block), F32)],
        [VMEM] * 2,
        "scaling",
    )(swap_all(send, OP), final)
    return vector, thetas


def solution(mesh):
    split = Mesh(
        mesh.devices.reshape(mesh.shape["sector"], 4, 4, 2), ("sector", "op_0", "op_1", "op_2")
    )
    in_specs = (
        P("sector", OP, None),
        P("sector", OP, None),
        P(OP, None, None),
        P(OP, None, None),
        P(),
        P(),
    )
    out_specs = (P("sector", OP, None), P())
    return jax.shard_map(
        shards, mesh=split, in_specs=in_specs, out_specs=out_specs, check_vma=False
    )
```

```python
import functools
import jax
import jax.numpy as jnp
from jax import lax
from jax.experimental import pallas as pl
from jax.experimental.pallas import tpu as pltpu
from jax.sharding import Mesh
from jax.sharding import PartitionSpec as P

OP = ("op_0", "op_1", "op_2")
CHIP = ("op_0", "op_1")
CORE = "op_2"
COLUMN = ("sector", "op_2")
BF = jnp.bfloat16
F32 = jnp.float32
VMEM = pl.BlockSpec(memory_space=pltpu.VMEM)
SMEM = pl.BlockSpec(memory_space=pltpu.SMEM)
HBM = pl.BlockSpec(memory_space=pltpu.HBM)
SHARE = 16
LANES = 128
TILE = 8
LAG = 2
LAG1 = LAG + 1


def swap_all(x, axes):
    return lax.all_to_all(x, axes, split_axis=0, concat_axis=0, tiled=True)


def other_core(x):
    return lax.ppermute(x, CORE, [(0, 1), (1, 0)])


def three_way(first, second):
    row = lax.broadcasted_iota(jnp.int32, (TILE, LANES), 0)
    value = jnp.where(row < 3, first, second)
    high = value.astype(BF).astype(F32)
    middle = (value - high).astype(BF).astype(F32)
    low = value - high - middle
    part = jnp.where(row < 3, row, row - 3)
    return jnp.where(part == 0, high, jnp.where(part == 1, middle, low)).astype(BF)


def two_sums(tile):
    first = tile[0:1] + tile[1:2] + tile[2:3]
    second = tile[3:4] + tile[4:5] + tile[5:6]
    return first[:, :1], second[:, :1]


def place():
    z = lax.axis_index("sector")
    chip = lax.axis_index("op_0") * lax.axis_size("op_1") + lax.axis_index("op_1")
    return z, chip, lax.axis_index(CORE)


def live(shape, first_row, size):
    row = lax.broadcasted_iota(jnp.int32, shape, 0) + first_row
    column = lax.broadcasted_iota(jnp.int32, shape, 1)
    return (row < size) & (column < size)


def stacked(ref, lead, tile):
    rows, block = tile.shape
    for j in range(block // LANES):
        ref[lead, j * rows : (j + 1) * rows, :] = tile[:, j * LANES : (j + 1) * LANES]


def unstacked(value, rows):
    parts = value.shape[0] // rows
    return jnp.concatenate([value[j * rows : (j + 1) * rows] for j in range(parts)], axis=1)


def opening_kernel(sizes_ref, wave_ref, diag_ref, send_ref, current_ref, square_ref):
    z, chip, core = place()
    wave = wave_ref[0]
    inside = live(wave.shape, (chip * 2 + core) * SHARE, sizes_ref[z])
    current = jnp.where(inside, wave, 0.0)
    current_ref[...] = current
    square_ref[...] = jnp.full((8, LANES), jnp.sum(current * current), F32)
    diag = diag_ref[0]
    high = diag.astype(BF)
    low = (diag - high.astype(F32)).astype(BF)
    current_low = current.astype(BF)
    for peer in range(send_ref.shape[0]):
        send_ref[peer, 0] = current_low
        send_ref[peer, 1] = high
        send_ref[peer, 2] = low


def halves_of(z, width):
    half = z % 2
    near = pl.ds(pl.multiple_of(half * width, width), width)
    far = pl.ds(pl.multiple_of((1 - half) * width, width), width)
    return near, far


def slabs(rows_at, send_ref):
    z, _, _ = place()
    chips, count, _, width = send_ref.shape
    near, far = halves_of(z, width)
    for k in range(count):
        if k < count - 2:
            slab = rows_at(k, near)
        else:
            slab = rows_at((z // 2) * 2 + k - (count - 2), far)
        for chip in range(chips):
            send_ref[chip, k] = slab


def spreading_kernel(begun_ref, send_ref):
    slabs(lambda k, cut: begun_ref[k, 0, :, cut], send_ref)


def product_kernel(
    coupling_ref, mine_ref, theirs_ref, left_a, left_b, right_a, right_b, square_ref,
    send_ref, total, rows, rights, halves, sems,
):
    z, chip, core = place()
    target = (z // 2) * 2 + core
    block, width = total.shape[0], rows.shape[-1]
    pairs = left_a.shape[0]
    near, far = halves_of(z, width)

    def fetch(pair):
        return pltpu.make_async_copy(
            right_a.at[pair, :, near], rights.at[pair, :, :width], sems.at[pair, 0]
        )

    def move(pair):
        return pltpu.make_async_copy(
            right_b.at[pair, :, near], rights.at[pair, :, width:], sems.at[pair, 1]
        )

    fetch(0).start()
    move(0).start()
    for k in range(rows.shape[0]):
        for at in range(mine_ref.shape[0]):
            rows[k, 2 * at + core] = mine_ref[at, k]
            rows[k, 2 * at + 1 - core] = theirs_ref[at, k]
    for pair in range(1, pairs):
        fetch(pair).start()
        move(pair).start()
    total[...] = jnp.zeros_like(total)

    def first(pair):
        for j, (owner, left) in enumerate(((core, left_a), (1 - core, left_b))):
            source = coupling_ref[target, (chip * 2 + owner) * pairs + pair]
            vector = rows[source].reshape(block, width)
            half = jnp.dot(left[pair], vector, preferred_element_type=F32)
            halves[pair % LAG1, :, j * width : (j + 1) * width] = half.astype(BF)

    def second(pair):
        total[...] += lax.dot_general(
            halves[pair % LAG1], rights[pair], (((1,), (1,)), ((), ())), preferred_element_type=F32
        )

    def both(pair, _):
        fetch(pair - LAG).wait()
        move(pair - LAG).wait()
        second(pair - LAG)
        first(pair)
        return 0

    for pair in range(LAG):
        first(pair)
    lax.fori_loop(LAG, pairs, both, 0)
    for pair in range(pairs - LAG, pairs):
        fetch(pair).wait()
        move(pair).wait()
    for pair in range(pairs - LAG, pairs):
        second(pair)

    here = rows[target].reshape(block, width).astype(F32)
    there = rows[rows.shape[0] - 2 + core].reshape(block, width).astype(F32)
    product = jnp.sum(here * total[:, near] + there * total[:, far])
    extra = three_way(product, square_ref[0, 0])
    for peer in range(send_ref.shape[0]):
        stacked(send_ref, peer, total[peer * 32 : (peer + 1) * 32, :].astype(BF))
        send_ref[peer, block // 4 :, :] = extra


def products(coupling, mine, theirs, left, right, left_other, right_other, square):
    pairs, block, _ = left.shape
    chips, count, share, width = mine.shape
    return pl.pallas_call(
        product_kernel,
        in_specs=[SMEM, VMEM, VMEM, VMEM, VMEM, HBM, VMEM, VMEM],
        out_specs=VMEM,
        scratch_shapes=[
            pltpu.VMEM((block, block), F32),
            pltpu.VMEM((count, 2 * chips, share, width), BF),
            pltpu.VMEM((pairs, block, 2 * width), BF),
            pltpu.VMEM((LAG1, block, 2 * width), BF),
            pltpu.SemaphoreType.DMA((pairs, 2)),
        ],
        out_shape=jax.ShapeDtypeStruct((chips, block // 4 + TILE, LANES), BF),
        compiler_params=pltpu.CompilerParams(vmem_limit_bytes=18 << 20),
        name="products",
    )(coupling, mine, theirs, left, left_other, right, right_other, square)


def joining_kernel(sizes_ref, arrived_ref, send_ref):
    z, chip, core = place()
    total = arrived_ref[0].astype(F32)
    for peer in range(1, arrived_ref.shape[0]):
        total = total + arrived_ref[peer].astype(F32)
    end = total.shape[0] - TILE
    sigma = unstacked(total[:end], 32)
    inside = live(sigma.shape, chip * 32, sizes_ref[(z // 2) * 2 + core])
    low = jnp.where(inside, sigma, 0.0).astype(BF)
    extra = three_way(*two_sums(total[end:]))
    for peer in range(send_ref.shape[0]):
        at = (peer % 2) * SHARE
        stacked(send_ref, peer, low[at : at + SHARE])
        send_ref[peer, end // 2 :, :] = extra


def scalars_of(arrived_ref):
    at = arrived_ref.shape[1] - TILE
    total = arrived_ref[0, at:].astype(F32)
    for peer in range(1, arrived_ref.shape[0]):
        total = total + arrived_ref[peer, at:].astype(F32)
    return two_sums(total)


def sigma_of(arrived_ref, target):
    end = arrived_ref.shape[1] - TILE
    at = (target // 2) * 4 + target % 2
    both = arrived_ref[at, :end].astype(F32) + arrived_ref[at + 2, :end].astype(F32)
    return unstacked(both, SHARE)


def corrected(current, sigma, diag, theta):
    gap = diag - theta
    return current - (sigma - theta * current) * gap / (gap * gap + 1.0)


def middle_kernel(
    arrived_ref, begun_ref, current_ref, diag_ref,
    send_ref, all_ref, own_ref, square_ref, theta_ref, low_ref,
):
    z, _, _ = place()
    first, second = scalars_of(arrived_ref)
    theta = first / (second + 1e-6)
    theta_ref[0] = theta[0, 0]
    for k in range(all_ref.shape[0]):
        diag = begun_ref[k, 1].astype(F32) + begun_ref[k, 2].astype(F32)
        update = corrected(begun_ref[k, 0].astype(F32), sigma_of(arrived_ref, k), diag, theta)
        all_ref[k] = update
        low_ref[k] = update.astype(BF)
    own = corrected(current_ref[...], sigma_of(arrived_ref, z), diag_ref[0], theta)
    own_ref[...] = own
    square_ref[...] = jnp.full((8, LANES), jnp.sum(own * own), F32)
    slabs(lambda k, cut: low_ref[k, :, cut], send_ref)


def closing_kernel(
    entries, arrived_ref, begun_ref, all_ref, own_ref, diag_ref, before_ref,
    final_ref, send_ref, theta_ref,
):
    z, _, _ = place()
    first, second = scalars_of(arrived_ref)
    scale = lax.rsqrt(second / entries + 1e-6)
    squared = scale * scale
    theta = squared * first / (squared * second + 1e-6)
    theta_ref[0] = before_ref[0]
    theta_ref[1] = theta[0, 0]
    total = jnp.zeros(all_ref.shape[1:], F32)
    for k in range(all_ref.shape[0]):
        diag = begun_ref[k, 1].astype(F32) + begun_ref[k, 2].astype(F32)
        update = corrected(scale * all_ref[k], scale * sigma_of(arrived_ref, k), diag, theta)
        total = total + update * update
    sigma = sigma_of(arrived_ref, z)
    final_ref[...] = corrected(scale * own_ref[...], scale * sigma, diag_ref[0], theta)
    send_ref[...] = jnp.full(send_ref.shape, jnp.sum(total), F32)


def scaling_kernel(entries, arrived_ref, final_ref, vector_ref):
    total = arrived_ref[0]
    for peer in range(1, arrived_ref.shape[0]):
        total = total + arrived_ref[peer]
    vector_ref[0] = final_ref[...] * lax.rsqrt(total[0:1, 0:1] / entries + 1e-6)


def call(kernel, shapes, specs, name, scratch=(), outs=None):
    return pl.pallas_call(
        kernel,
        in_specs=specs,
        out_specs=outs or [VMEM] * len(shapes),
        out_shape=[jax.ShapeDtypeStruct(s, t) for s, t in shapes],
        scratch_shapes=scratch,
        compiler_params=pltpu.CompilerParams(vmem_limit_bytes=16 << 20),
        name=name,
    )


def shards(wavefunction, diagonal, left_blocks, right_blocks, coupling, sector_sizes):
    _, share, block = wavefunction.shape
    sectors = lax.axis_size("sector")
    chips = lax.axis_size("op_0") * lax.axis_size("op_1")
    width = block // 2
    left_other = other_core(left_blocks)
    right_other = other_core(right_blocks)
    opening_inputs = tuple(
        pltpu.with_memory_space_constraint(x, pltpu.HBM)
        for x in (sector_sizes, wavefunction, diagonal)
    )
    right_blocks = pltpu.with_memory_space_constraint(right_blocks, pltpu.HBM)
    entries = float(sectors * block * block)
    spread = ((chips, sectors + 2, share, width), BF)
    scalar = ((8, LANES), F32)

    begin, current, square = call(
        opening_kernel,
        [((sectors, 3, share, block), BF), ((share, block), F32), scalar],
        [SMEM, VMEM, VMEM],
        "opening",
    )(*opening_inputs)
    begun = swap_all(begin, "sector")
    (outgoing,) = call(spreading_kernel, [spread], [VMEM], "spreading")(begun)

    def sigma_step(outgoing, square):
        mine = swap_all(outgoing, CHIP)
        send = products(
            coupling, mine, other_core(mine),
            left_blocks, right_blocks, left_other, right_other, square,
        )
        (send,) = call(
            joining_kernel,
            [((sectors * 2, block // 8 + TILE, LANES), BF)],
            [SMEM, VMEM],
            "joining",
        )(sector_sizes, swap_all(send, CHIP))
        return swap_all(send, COLUMN)

    arrived = sigma_step(outgoing, square)
    outgoing, everyone, own, square, theta = call(
        middle_kernel,
        [spread, ((sectors, share, block), F32), ((share, block), F32), scalar, ((1,), F32)],
        [VMEM] * 4,
        "middle",
        [pltpu.VMEM((sectors, share, block), BF)],
        [VMEM, VMEM, VMEM, VMEM, SMEM],
    )(arrived, begun, current, diagonal)

    arrived = sigma_step(outgoing, square)
    final, send, thetas = call(
        functools.partial(closing_kernel, entries),
        [((share, block), F32), ((chips * 2, 8, LANES), F32), ((2,), F32)],
        [VMEM, VMEM, VMEM, VMEM, VMEM, SMEM],
        "closing",
        outs=[VMEM, VMEM, SMEM],
    )(arrived, begun, everyone, own, diagonal, theta)
    (vector,) = call(
        functools.partial(scaling_kernel, entries),
        [((1, share, block), F32)],
        [VMEM] * 2,
        "scaling",
    )(swap_all(send, OP), final)
    return vector, thetas


def solution(mesh):
    split = Mesh(
        mesh.devices.reshape(mesh.shape["sector"], 4, 4, 2), ("sector", "op_0", "op_1", "op_2")
    )
    in_specs = (
        P("sector", OP, None),
        P("sector", OP, None),
        P(OP, None, None),
        P(OP, None, None),
        P(),
        P(),
    )
    out_specs = (P("sector", OP, None), P())
    return jax.shard_map(
        shards, mesh=split, in_specs=in_specs, out_specs=out_specs, check_vma=False
    )
```

```python
import functools
import jax
import jax.numpy as jnp
from jax import lax
from jax.experimental import pallas as pl
from jax.experimental.pallas import tpu as pltpu
from jax.sharding import Mesh
from jax.sharding import PartitionSpec as P

OP = ("op_0", "op_1", "op_2")
CHIP = ("op_0", "op_1")
CORE = "op_2"
BF = jnp.bfloat16
F32 = jnp.float32
VMEM = pl.BlockSpec(memory_space=pltpu.VMEM)
SMEM = pl.BlockSpec(memory_space=pltpu.SMEM)
HBM = pl.BlockSpec(memory_space=pltpu.HBM)
SHARE = 16
LANES = 128
TILE = 8
LAG = 3
LAG1 = LAG + 1


def swap_all(x, axes):
    return lax.all_to_all(x, axes, split_axis=0, concat_axis=0, tiled=True)


def other_core(x):
    return lax.ppermute(x, CORE, [(0, 1), (1, 0)])


def three_way(first, second):
    row = lax.broadcasted_iota(jnp.int32, (TILE, LANES), 0)
    value = jnp.where(row < 3, first, second)
    high = value.astype(BF).astype(F32)
    middle = (value - high).astype(BF).astype(F32)
    low = value - high - middle
    part = jnp.where(row < 3, row, row - 3)
    return jnp.where(part == 0, high, jnp.where(part == 1, middle, low)).astype(BF)


def two_sums(tile):
    first = tile[0:1] + tile[1:2] + tile[2:3]
    second = tile[3:4] + tile[4:5] + tile[5:6]
    return first[:, :1], second[:, :1]


def place():
    z = lax.axis_index("sector")
    chip = lax.axis_index("op_0") * lax.axis_size("op_1") + lax.axis_index("op_1")
    return z, chip, lax.axis_index(CORE)


def live(shape, first_row, size):
    row = lax.broadcasted_iota(jnp.int32, shape, 0) + first_row
    column = lax.broadcasted_iota(jnp.int32, shape, 1)
    return (row < size) & (column < size)


def stacked(ref, lead, tile):
    rows, block = tile.shape
    for j in range(block // LANES):
        ref[lead, j * rows : (j + 1) * rows, :] = tile[:, j * LANES : (j + 1) * LANES]


def unstacked(value, rows):
    parts = value.shape[0] // rows
    return jnp.concatenate([value[j * rows : (j + 1) * rows] for j in range(parts)], axis=1)


def opening_kernel(sizes_ref, wave_ref, diag_ref, send_ref, current_ref, square_ref):
    z, chip, core = place()
    wave = wave_ref[0]
    inside = live(wave.shape, (chip * 2 + core) * SHARE, sizes_ref[z])
    current = jnp.where(inside, wave, 0.0)
    current_ref[...] = current
    square_ref[...] = jnp.full((8, LANES), jnp.sum(current * current), F32)
    diag = diag_ref[0]
    high = diag.astype(BF)
    low = (diag - high.astype(F32)).astype(BF)
    current_low = current.astype(BF)
    for peer in range(send_ref.shape[0]):
        send_ref[peer, 0] = current_low
        send_ref[peer, 1] = high
        send_ref[peer, 2] = low


def halves_of(z, width):
    half = z % 2
    near = pl.ds(pl.multiple_of(half * width, width), width)
    far = pl.ds(pl.multiple_of((1 - half) * width, width), width)
    return near, far


def slabs(rows_at, send_ref):
    z, _, _ = place()
    chips, count, _, width = send_ref.shape
    near, far = halves_of(z, width)
    for k in range(count):
        if k < count - 2:
            slab = rows_at(k, near)
        else:
            slab = rows_at((z // 2) * 2 + k - (count - 2), far)
        for chip in range(chips):
            send_ref[chip, k] = slab


def spreading_kernel(begun_ref, send_ref):
    slabs(lambda k, cut: begun_ref[k, 0, :, cut], send_ref)


def product_kernel(
    coupling_ref, mine_ref, theirs_ref, left_a, left_b, right_a, right_b, square_ref,
    keep_ref, give_ref, total, rows, rights, halves, sems,
):
    z, chip, core = place()
    target = (z // 2) * 2 + core
    block, width = total.shape[0], rows.shape[-1]
    pairs = left_a.shape[0]
    near, far = halves_of(z, width)

    def fetch(pair):
        return pltpu.make_async_copy(
            right_a.at[pair, :, near], rights.at[pair, :, :width], sems.at[pair, 0]
        )

    def move(pair):
        return pltpu.make_async_copy(
            right_b.at[pair, :, near], rights.at[pair, :, width:], sems.at[pair, 1]
        )

    fetch(0).start()
    move(0).start()
    for k in range(rows.shape[0]):
        for at in range(mine_ref.shape[0]):
            rows[k, 2 * at + core] = mine_ref[at, k]
            rows[k, 2 * at + 1 - core] = theirs_ref[at, k]
    for pair in range(1, pairs):
        fetch(pair).start()
        move(pair).start()
    total[...] = jnp.zeros_like(total)

    def first(pair):
        for j, (owner, left) in enumerate(((core, left_a), (1 - core, left_b))):
            source = coupling_ref[target, (chip * 2 + owner) * pairs + pair]
            vector = rows[source].reshape(block, width)
            half = jnp.dot(left[pair], vector, preferred_element_type=F32)
            halves[pair % LAG1, :, j * width : (j + 1) * width] = half.astype(BF)

    def second(pair):
        total[...] += lax.dot_general(
            halves[pair % LAG1], rights[pair], (((1,), (1,)), ((), ())), preferred_element_type=F32
        )

    def both(pair, _):
        fetch(pair - LAG).wait()
        move(pair - LAG).wait()
        second(pair - LAG)
        first(pair)
        return 0

    for pair in range(LAG):
        first(pair)
    lax.fori_loop(LAG, pairs, both, 0)
    for pair in range(pairs - LAG, pairs):
        fetch(pair).wait()
        move(pair).wait()
    for pair in range(pairs - LAG, pairs):
        second(pair)

    here = rows[target].reshape(block, width).astype(F32)
    there = rows[rows.shape[0] - 2 + core].reshape(block, width).astype(F32)
    product = jnp.sum(here * total[:, near] + there * total[:, far])
    extra = three_way(product, square_ref[0, 0])
    for peer in range(keep_ref.shape[0]):
        for ref, side in ((keep_ref, core), (give_ref, 1 - core)):
            at = pl.multiple_of(peer * 2 * SHARE + side * SHARE, SHARE)
            stacked(ref, peer, total[pl.ds(at, SHARE), :].astype(BF))
        give_ref[peer, block // 8 :, :] = extra


def products(coupling, mine, theirs, left, right, left_other, right_other, square):
    pairs, block, _ = left.shape
    chips, count, share, width = mine.shape
    return pl.pallas_call(
        product_kernel,
        in_specs=[SMEM, VMEM, VMEM, VMEM, VMEM, HBM, VMEM, VMEM],
        out_specs=[VMEM, VMEM],
        scratch_shapes=[
            pltpu.VMEM((block, block), F32),
            pltpu.VMEM((count, 2 * chips, share, width), BF),
            pltpu.VMEM((pairs, block, 2 * width), BF),
            pltpu.VMEM((LAG1, block, 2 * width), BF),
            pltpu.SemaphoreType.DMA((pairs, 2)),
        ],
        out_shape=[
            jax.ShapeDtypeStruct((chips, block // 8, LANES), BF),
            jax.ShapeDtypeStruct((chips, block // 8 + TILE, LANES), BF),
        ],
        compiler_params=pltpu.CompilerParams(vmem_limit_bytes=18 << 20),
        name="products",
    )(coupling, mine, theirs, left, left_other, right, right_other, square)


def pairing_kernel(keep_ref, give_ref, got_ref, send_ref):
    _, _, core = place()
    half = keep_ref.shape[1]
    here = pl.ds(pl.multiple_of(core * half, half), half)
    there = pl.ds(pl.multiple_of((1 - core) * half, half), half)
    both = give_ref[0, half:].astype(F32) + got_ref[0, half:].astype(F32)
    extra = three_way(*two_sums(both))
    for peer in range(send_ref.shape[0]):
        send_ref[peer, here, :] = keep_ref[peer]
        send_ref[peer, there, :] = got_ref[peer, :half, :]
        send_ref[peer, 2 * half :, :] = extra


def joining_kernel(sizes_ref, arrived_ref, send_ref):
    z, chip, core = place()
    total = arrived_ref[0].astype(F32)
    for peer in range(1, arrived_ref.shape[0]):
        total = total + arrived_ref[peer].astype(F32)
    end = total.shape[0] - TILE
    half = end // 2
    extra = three_way(*two_sums(total[end:]))
    for j in range(2):
        sigma = unstacked(total[j * half : (j + 1) * half], SHARE)
        first_row = (chip * 2 + core) * SHARE
        inside = live(sigma.shape, first_row, sizes_ref[(z // 2) * 2 + j])
        low = jnp.where(inside, sigma, 0.0).astype(BF)
        for k in range(low.shape[1] // LANES):
            at = j * half + k * SHARE
            part = low[:, k * LANES : (k + 1) * LANES]
            for peer in range(send_ref.shape[0]):
                send_ref[peer, at : at + SHARE, :] = part
    for peer in range(send_ref.shape[0]):
        send_ref[peer, end:, :] = extra


def scalars_of(arrived_ref):
    at = arrived_ref.shape[1] - TILE
    total = arrived_ref[0, at:].astype(F32)
    for peer in range(1, arrived_ref.shape[0]):
        total = total + arrived_ref[peer, at:].astype(F32)
    return two_sums(total)


def sigma_of(arrived_ref, target):
    half = (arrived_ref.shape[1] - TILE) // 2
    at = (target // 2) * 2
    if isinstance(target, int):
        part = slice((target % 2) * half, (target % 2 + 1) * half)
    else:
        part = pl.ds(pl.multiple_of((target % 2) * half, half), half)
    both = arrived_ref[at, part, :].astype(F32) + arrived_ref[at + 1, part, :].astype(F32)
    return unstacked(both, SHARE)


def corrected(current, sigma, diag, theta):
    gap = diag - theta
    return current - (sigma - theta * current) * gap / (gap * gap + 1.0)


def middle_kernel(
    arrived_ref, begun_ref, current_ref, diag_ref,
    send_ref, all_ref, own_ref, square_ref, theta_ref, low_ref,
):
    z, _, _ = place()
    first, second = scalars_of(arrived_ref)
    theta = first / (second + 1e-6)
    theta_ref[0] = theta[0, 0]
    for k in range(all_ref.shape[0]):
        diag = begun_ref[k, 1].astype(F32) + begun_ref[k, 2].astype(F32)
        update = corrected(begun_ref[k, 0].astype(F32), sigma_of(arrived_ref, k), diag, theta)
        all_ref[k] = update
        low_ref[k] = update.astype(BF)
    own = corrected(current_ref[...], sigma_of(arrived_ref, z), diag_ref[0], theta)
    own_ref[...] = own
    square_ref[...] = jnp.full((8, LANES), jnp.sum(own * own), F32)
    slabs(lambda k, cut: low_ref[k, :, cut], send_ref)


def closing_kernel(
    entries, arrived_ref, begun_ref, all_ref, own_ref, diag_ref, before_ref,
    final_ref, send_ref, theta_ref,
):
    z, _, _ = place()
    first, second = scalars_of(arrived_ref)
    scale = lax.rsqrt(second / entries + 1e-6)
    squared = scale * scale
    theta = squared * first / (squared * second + 1e-6)
    theta_ref[0] = before_ref[0]
    theta_ref[1] = theta[0, 0]
    total = jnp.zeros(all_ref.shape[1:], F32)
    for k in range(all_ref.shape[0]):
        diag = begun_ref[k, 1].astype(F32) + begun_ref[k, 2].astype(F32)
        update = corrected(scale * all_ref[k], scale * sigma_of(arrived_ref, k), diag, theta)
        total = total + update * update
    sigma = sigma_of(arrived_ref, z)
    final_ref[...] = corrected(scale * own_ref[...], scale * sigma, diag_ref[0], theta)
    send_ref[...] = jnp.full(send_ref.shape, jnp.sum(total), F32)


def scaling_kernel(entries, arrived_ref, final_ref, vector_ref):
    total = arrived_ref[0]
    for peer in range(1, arrived_ref.shape[0]):
        total = total + arrived_ref[peer]
    vector_ref[0] = final_ref[...] * lax.rsqrt(total[0:1, 0:1] / entries + 1e-6)


def call(kernel, shapes, specs, name, scratch=(), outs=None):
    return pl.pallas_call(
        kernel,
        in_specs=specs,
        out_specs=outs or [VMEM] * len(shapes),
        out_shape=[jax.ShapeDtypeStruct(s, t) for s, t in shapes],
        scratch_shapes=scratch,
        compiler_params=pltpu.CompilerParams(vmem_limit_bytes=16 << 20),
        name=name,
    )


def shards(wavefunction, diagonal, left_blocks, right_blocks, coupling, sector_sizes):
    _, share, block = wavefunction.shape
    sectors = lax.axis_size("sector")
    chips = lax.axis_size("op_0") * lax.axis_size("op_1")
    width = block // 2
    left_other = other_core(left_blocks)
    right_other = other_core(right_blocks)
    opening_inputs = tuple(
        pltpu.with_memory_space_constraint(x, pltpu.HBM)
        for x in (sector_sizes, wavefunction, diagonal)
    )
    right_blocks = pltpu.with_memory_space_constraint(right_blocks, pltpu.HBM)
    entries = float(sectors * block * block)
    spread = ((chips, sectors + 2, share, width), BF)
    scalar = ((8, LANES), F32)

    begin, current, square = call(
        opening_kernel,
        [((sectors, 3, share, block), BF), ((share, block), F32), scalar],
        [SMEM, VMEM, VMEM],
        "opening",
    )(*opening_inputs)
    begun = swap_all(begin, "sector")
    (outgoing,) = call(spreading_kernel, [spread], [VMEM], "spreading")(begun)

    def sigma_step(outgoing, square):
        mine = swap_all(outgoing, CHIP)
        keep, give = products(
            coupling, mine, other_core(mine),
            left_blocks, right_blocks, left_other, right_other, square,
        )
        (send,) = call(
            pairing_kernel,
            [((chips, block // 4 + TILE, LANES), BF)],
            [VMEM] * 3,
            "pairing",
        )(keep, give, other_core(give))
        (send,) = call(
            joining_kernel,
            [((sectors, block // 4 + TILE, LANES), BF)],
            [SMEM, VMEM],
            "joining",
        )(sector_sizes, swap_all(send, CHIP))
        return swap_all(send, "sector")

    arrived = sigma_step(outgoing, square)
    outgoing, everyone, own, square, theta = call(
        middle_kernel,
        [spread, ((sectors, share, block), F32), ((share, block), F32), scalar, ((1,), F32)],
        [VMEM] * 4,
        "middle",
        [pltpu.VMEM((sectors, share, block), BF)],
        [VMEM, VMEM, VMEM, VMEM, SMEM],
    )(arrived, begun, current, diagonal)

    arrived = sigma_step(outgoing, square)
    final, send, thetas = call(
        functools.partial(closing_kernel, entries),
        [((share, block), F32), ((chips * 2, 8, LANES), F32), ((2,), F32)],
        [VMEM, VMEM, VMEM, VMEM, VMEM, SMEM],
        "closing",
        outs=[VMEM, VMEM, SMEM],
    )(arrived, begun, everyone, own, diagonal, theta)
    (vector,) = call(
        functools.partial(scaling_kernel, entries),
        [((1, share, block), F32)],
        [VMEM] * 2,
        "scaling",
    )(swap_all(send, OP), final)
    return vector, thetas


def solution(mesh):
    split = Mesh(
        mesh.devices.reshape(mesh.shape["sector"], 4, 4, 2), ("sector", "op_0", "op_1", "op_2")
    )
    in_specs = (
        P("sector", OP, None),
        P("sector", OP, None),
        P(OP, None, None),
        P(OP, None, None),
        P(),
        P(),
    )
    out_specs = (P("sector", OP, None), P())
    return jax.shard_map(
        shards, mesh=split, in_specs=in_specs, out_specs=out_specs, check_vma=False
    )
```

```python
import functools
import jax
import jax.numpy as jnp
from jax import lax
from jax.experimental import pallas as pl
from jax.experimental.pallas import tpu as pltpu
from jax.sharding import Mesh
from jax.sharding import PartitionSpec as P

OP = ("op_0", "op_1", "op_2")
CHIP = ("op_0", "op_1")
CORE = "op_2"
BF = jnp.bfloat16
F32 = jnp.float32
VMEM = pl.BlockSpec(memory_space=pltpu.VMEM)
SMEM = pl.BlockSpec(memory_space=pltpu.SMEM)
HBM = pl.BlockSpec(memory_space=pltpu.HBM)
SHARE = 16
LANES = 128
TILE = 8
LAG = 3
LAG1 = LAG + 1


def swap_all(x, axes):
    return lax.all_to_all(x, axes, split_axis=0, concat_axis=0, tiled=True)


def other_core(x):
    return lax.ppermute(x, CORE, [(0, 1), (1, 0)])


def three_way(first, second):
    row = lax.broadcasted_iota(jnp.int32, (TILE, LANES), 0)
    value = jnp.where(row < 3, first, second)
    high = value.astype(BF).astype(F32)
    middle = (value - high).astype(BF).astype(F32)
    low = value - high - middle
    part = jnp.where(row < 3, row, row - 3)
    return jnp.where(part == 0, high, jnp.where(part == 1, middle, low)).astype(BF)


def two_sums(tile):
    first = tile[0:1] + tile[1:2] + tile[2:3]
    second = tile[3:4] + tile[4:5] + tile[5:6]
    return first[:, :1], second[:, :1]


def place():
    z = lax.axis_index("sector")
    chip = lax.axis_index("op_0") * lax.axis_size("op_1") + lax.axis_index("op_1")
    return z, chip, lax.axis_index(CORE)


def live(shape, first_row, size):
    row = lax.broadcasted_iota(jnp.int32, shape, 0) + first_row
    column = lax.broadcasted_iota(jnp.int32, shape, 1)
    return (row < size) & (column < size)


def stacked(ref, lead, tile):
    rows, block = tile.shape
    for j in range(block // LANES):
        ref[lead, j * rows : (j + 1) * rows, :] = tile[:, j * LANES : (j + 1) * LANES]


def unstacked(value, rows):
    parts = value.shape[0] // rows
    return jnp.concatenate([value[j * rows : (j + 1) * rows] for j in range(parts)], axis=1)


def opening_kernel(sizes_ref, wave_ref, diag_ref, send_ref, current_ref, square_ref):
    z, chip, core = place()
    wave = wave_ref[0]
    inside = live(wave.shape, (chip * 2 + core) * SHARE, sizes_ref[z])
    current = jnp.where(inside, wave, 0.0)
    current_ref[...] = current
    square_ref[...] = jnp.full((8, LANES), jnp.sum(current * current), F32)
    diag = diag_ref[0]
    high = diag.astype(BF)
    low = (diag - high.astype(F32)).astype(BF)
    current_low = current.astype(BF)
    for peer in range(send_ref.shape[0]):
        send_ref[peer, 0] = current_low
        send_ref[peer, 1] = high
        send_ref[peer, 2] = low


def halves_of(z, width):
    half = z % 2
    near = pl.ds(pl.multiple_of(half * width, width), width)
    far = pl.ds(pl.multiple_of((1 - half) * width, width), width)
    return near, far


def slabs(rows_at, send_ref):
    z, _, _ = place()
    chips, count, _, width = send_ref.shape
    near, far = halves_of(z, width)
    for k in range(count):
        if k < count - 2:
            slab = rows_at(k, near)
        else:
            slab = rows_at((z // 2) * 2 + k - (count - 2), far)
        for chip in range(chips):
            send_ref[chip, k] = slab


def spreading_kernel(begun_ref, send_ref):
    slabs(lambda k, cut: begun_ref[k, 0, :, cut], send_ref)


def product_kernel(
    coupling_ref, mine_ref, theirs_ref, left_a, left_b, right_a, right_b, square_ref,
    send_ref, total, rows, rights, halves, sems,
):
    z, chip, core = place()
    target = (z // 2) * 2 + core
    block, width = total.shape[0], rows.shape[-1]
    pairs = left_a.shape[0]
    near, far = halves_of(z, width)

    def fetch(pair):
        return pltpu.make_async_copy(
            right_a.at[pair, :, near], rights.at[pair, :, :width], sems.at[pair, 0]
        )

    def move(pair):
        return pltpu.make_async_copy(
            right_b.at[pair, :, near], rights.at[pair, :, width:], sems.at[pair, 1]
        )

    fetch(0).start()
    move(0).start()
    for k in range(rows.shape[0]):
        for at in range(mine_ref.shape[0]):
            rows[k, 2 * at + core] = mine_ref[at, k]
            rows[k, 2 * at + 1 - core] = theirs_ref[at, k]
    for pair in range(1, pairs):
        fetch(pair).start()
        move(pair).start()
    total[...] = jnp.zeros_like(total)

    def first(pair):
        for j, (owner, left) in enumerate(((core, left_a), (1 - core, left_b))):
            source = coupling_ref[target, (chip * 2 + owner) * pairs + pair]
            vector = rows[source].reshape(block, width)
            half = jnp.dot(left[pair], vector, preferred_element_type=F32)
            halves[pair % LAG1, :, j * width : (j + 1) * width] = half.astype(BF)

    def second(pair):
        total[...] += lax.dot_general(
            halves[pair % LAG1], rights[pair], (((1,), (1,)), ((), ())), preferred_element_type=F32
        )

    def both(pair, _):
        fetch(pair - LAG).wait()
        move(pair - LAG).wait()
        second(pair - LAG)
        first(pair)
        return 0

    for pair in range(LAG):
        first(pair)
    lax.fori_loop(LAG, pairs, both, 0)
    for pair in range(pairs - LAG, pairs):
        fetch(pair).wait()
        move(pair).wait()
    for pair in range(pairs - LAG, pairs):
        second(pair)

    here = rows[target].reshape(block, width).astype(F32)
    there = rows[rows.shape[0] - 2 + core].reshape(block, width).astype(F32)
    product = jnp.sum(here * total[:, near] + there * total[:, far])
    extra = three_way(product, square_ref[0, 0])
    for peer in range(send_ref.shape[0]):
        stacked(send_ref, peer, total[peer * SHARE : (peer + 1) * SHARE, :].astype(BF))
        send_ref[peer, block // 8 :, :] = extra


def products(coupling, mine, theirs, left, right, left_other, right_other, square):
    pairs, block, _ = left.shape
    chips, count, share, width = mine.shape
    return pl.pallas_call(
        product_kernel,
        in_specs=[SMEM, VMEM, VMEM, VMEM, VMEM, HBM, VMEM, VMEM],
        out_specs=VMEM,
        scratch_shapes=[
            pltpu.VMEM((block, block), F32),
            pltpu.VMEM((count, 2 * chips, share, width), BF),
            pltpu.VMEM((pairs, block, 2 * width), BF),
            pltpu.VMEM((LAG1, block, 2 * width), BF),
            pltpu.SemaphoreType.DMA((pairs, 2)),
        ],
        out_shape=jax.ShapeDtypeStruct((2 * chips, block // 8 + TILE, LANES), BF),
        compiler_params=pltpu.CompilerParams(vmem_limit_bytes=18 << 20),
        name="products",
    )(coupling, mine, theirs, left, left_other, right, right_other, square)


def joining_kernel(sizes_ref, arrived_ref, send_ref):
    z, chip, core = place()
    totals = []
    for j in range(2):
        total = arrived_ref[j].astype(F32)
        for peer in range(2 + j, arrived_ref.shape[0], 2):
            total = total + arrived_ref[peer].astype(F32)
        totals.append(total)
    half = totals[0].shape[0] - TILE
    extra = three_way(*two_sums(totals[0][half:] + totals[1][half:]))
    for j, total in enumerate(totals):
        sigma = unstacked(total[:half], SHARE)
        first_row = (chip * 2 + core) * SHARE
        inside = live(sigma.shape, first_row, sizes_ref[(z // 2) * 2 + j])
        low = jnp.where(inside, sigma, 0.0).astype(BF)
        for k in range(low.shape[1] // LANES):
            at = j * half + k * SHARE
            part = low[:, k * LANES : (k + 1) * LANES]
            for peer in range(send_ref.shape[0]):
                send_ref[peer, at : at + SHARE, :] = part
    for peer in range(send_ref.shape[0]):
        send_ref[peer, 2 * half :, :] = extra


def scalars_of(arrived_ref):
    at = arrived_ref.shape[1] - TILE
    total = arrived_ref[0, at:].astype(F32)
    for peer in range(1, arrived_ref.shape[0]):
        total = total + arrived_ref[peer, at:].astype(F32)
    return two_sums(total)


def sigma_of(arrived_ref, target):
    half = (arrived_ref.shape[1] - TILE) // 2
    at = (target // 2) * 2
    if isinstance(target, int):
        part = slice((target % 2) * half, (target % 2 + 1) * half)
    else:
        part = pl.ds(pl.multiple_of((target % 2) * half, half), half)
    both = arrived_ref[at, part, :].astype(F32) + arrived_ref[at + 1, part, :].astype(F32)
    return unstacked(both, SHARE)


def corrected(current, sigma, diag, theta):
    gap = diag - theta
    return current - (sigma - theta * current) * gap / (gap * gap + 1.0)


def middle_kernel(
    arrived_ref, begun_ref, current_ref, diag_ref,
    send_ref, all_ref, own_ref, square_ref, theta_ref, low_ref,
):
    z, _, _ = place()
    first, second = scalars_of(arrived_ref)
    theta = first / (second + 1e-6)
    theta_ref[0] = theta[0, 0]
    for k in range(all_ref.shape[0]):
        diag = begun_ref[k, 1].astype(F32) + begun_ref[k, 2].astype(F32)
        update = corrected(begun_ref[k, 0].astype(F32), sigma_of(arrived_ref, k), diag, theta)
        all_ref[k] = update
        low_ref[k] = update.astype(BF)
    own = corrected(current_ref[...], sigma_of(arrived_ref, z), diag_ref[0], theta)
    own_ref[...] = own
    square_ref[...] = jnp.full((8, LANES), jnp.sum(own * own), F32)
    slabs(lambda k, cut: low_ref[k, :, cut], send_ref)


def closing_kernel(
    entries, arrived_ref, begun_ref, all_ref, own_ref, diag_ref, before_ref,
    final_ref, send_ref, theta_ref,
):
    z, _, _ = place()
    first, second = scalars_of(arrived_ref)
    scale = lax.rsqrt(second / entries + 1e-6)
    squared = scale * scale
    theta = squared * first / (squared * second + 1e-6)
    theta_ref[0] = before_ref[0]
    theta_ref[1] = theta[0, 0]
    total = jnp.zeros(all_ref.shape[1:], F32)
    for k in range(all_ref.shape[0]):
        diag = begun_ref[k, 1].astype(F32) + begun_ref[k, 2].astype(F32)
        update = corrected(scale * all_ref[k], scale * sigma_of(arrived_ref, k), diag, theta)
        total = total + update * update
    sigma = sigma_of(arrived_ref, z)
    final_ref[...] = corrected(scale * own_ref[...], scale * sigma, diag_ref[0], theta)
    send_ref[...] = jnp.full(send_ref.shape, jnp.sum(total), F32)


def scaling_kernel(entries, arrived_ref, final_ref, vector_ref):
    total = arrived_ref[0]
    for peer in range(1, arrived_ref.shape[0]):
        total = total + arrived_ref[peer]
    vector_ref[0] = final_ref[...] * lax.rsqrt(total[0:1, 0:1] / entries + 1e-6)


def call(kernel, shapes, specs, name, scratch=(), outs=None):
    return pl.pallas_call(
        kernel,
        in_specs=specs,
        out_specs=outs or [VMEM] * len(shapes),
        out_shape=[jax.ShapeDtypeStruct(s, t) for s, t in shapes],
        scratch_shapes=scratch,
        compiler_params=pltpu.CompilerParams(vmem_limit_bytes=16 << 20),
        name=name,
    )


def shards(wavefunction, diagonal, left_blocks, right_blocks, coupling, sector_sizes):
    _, share, block = wavefunction.shape
    sectors = lax.axis_size("sector")
    chips = lax.axis_size("op_0") * lax.axis_size("op_1")
    width = block // 2
    left_other = other_core(left_blocks)
    right_other = other_core(right_blocks)
    opening_inputs = tuple(
        pltpu.with_memory_space_constraint(x, pltpu.HBM)
        for x in (sector_sizes, wavefunction, diagonal)
    )
    right_blocks = pltpu.with_memory_space_constraint(right_blocks, pltpu.HBM)
    entries = float(sectors * block * block)
    spread = ((chips, sectors + 2, share, width), BF)
    scalar = ((8, LANES), F32)

    begin, current, square = call(
        opening_kernel,
        [((sectors, 3, share, block), BF), ((share, block), F32), scalar],
        [SMEM, VMEM, VMEM],
        "opening",
    )(*opening_inputs)
    begun = swap_all(begin, "sector")
    (outgoing,) = call(spreading_kernel, [spread], [VMEM], "spreading")(begun)

    def sigma_step(outgoing, square):
        mine = swap_all(outgoing, CHIP)
        send = products(
            coupling, mine, other_core(mine),
            left_blocks, right_blocks, left_other, right_other, square,
        )
        (send,) = call(
            joining_kernel,
            [((sectors, block // 4 + TILE, LANES), BF)],
            [SMEM, VMEM],
            "joining",
        )(sector_sizes, swap_all(send, OP))
        return swap_all(send, "sector")

    arrived = sigma_step(outgoing, square)
    outgoing, everyone, own, square, theta = call(
        middle_kernel,
        [spread, ((sectors, share, block), F32), ((share, block), F32), scalar, ((1,), F32)],
        [VMEM] * 4,
        "middle",
        [pltpu.VMEM((sectors, share, block), BF)],
        [VMEM, VMEM, VMEM, VMEM, SMEM],
    )(arrived, begun, current, diagonal)

    arrived = sigma_step(outgoing, square)
    final, send, thetas = call(
        functools.partial(closing_kernel, entries),
        [((share, block), F32), ((chips * 2, 8, LANES), F32), ((2,), F32)],
        [VMEM, VMEM, VMEM, VMEM, VMEM, SMEM],
        "closing",
        outs=[VMEM, VMEM, SMEM],
    )(arrived, begun, everyone, own, diagonal, theta)
    (vector,) = call(
        functools.partial(scaling_kernel, entries),
        [((1, share, block), F32)],
        [VMEM] * 2,
        "scaling",
    )(swap_all(send, OP), final)
    return vector, thetas


def solution(mesh):
    split = Mesh(
        mesh.devices.reshape(mesh.shape["sector"], 4, 4, 2), ("sector", "op_0", "op_1", "op_2")
    )
    in_specs = (
        P("sector", OP, None),
        P("sector", OP, None),
        P(OP, None, None),
        P(OP, None, None),
        P(),
        P(),
    )
    out_specs = (P("sector", OP, None), P())
    return jax.shard_map(
        shards, mesh=split, in_specs=in_specs, out_specs=out_specs, check_vma=False
    )
```

```python
import functools
import jax
import jax.numpy as jnp
from jax import lax
from jax.experimental import pallas as pl
from jax.experimental.pallas import tpu as pltpu
from jax.sharding import Mesh
from jax.sharding import PartitionSpec as P

OP = ("op_0", "op_1", "op_2")
CHIP = ("op_1", "op_0")
CORE = "op_2"
BF = jnp.bfloat16
F32 = jnp.float32
VMEM = pl.BlockSpec(memory_space=pltpu.VMEM)
SMEM = pl.BlockSpec(memory_space=pltpu.SMEM)
HBM = pl.BlockSpec(memory_space=pltpu.HBM)
SHARE = 16
LANES = 128
TILE = 8
LAG = 3
LAG1 = LAG + 1


def swap_all(x, axes):
    return lax.all_to_all(x, axes, split_axis=0, concat_axis=0, tiled=True)


def other_core(x):
    return lax.ppermute(x, CORE, [(0, 1), (1, 0)])


def three_way(first, second):
    row = lax.broadcasted_iota(jnp.int32, (TILE, LANES), 0)
    value = jnp.where(row < 3, first, second)
    high = value.astype(BF).astype(F32)
    middle = (value - high).astype(BF).astype(F32)
    low = value - high - middle
    part = jnp.where(row < 3, row, row - 3)
    return jnp.where(part == 0, high, jnp.where(part == 1, middle, low)).astype(BF)


def two_sums(tile):
    first = tile[0:1] + tile[1:2] + tile[2:3]
    second = tile[3:4] + tile[4:5] + tile[5:6]
    return first[:, :1], second[:, :1]


def place():
    z = lax.axis_index("sector")
    chip = lax.axis_index("op_0") * lax.axis_size("op_1") + lax.axis_index("op_1")
    return z, chip, lax.axis_index(CORE)


def live(shape, first_row, size):
    row = lax.broadcasted_iota(jnp.int32, shape, 0) + first_row
    column = lax.broadcasted_iota(jnp.int32, shape, 1)
    return (row < size) & (column < size)


def stacked(ref, lead, tile):
    rows, block = tile.shape
    for j in range(block // LANES):
        ref[lead, j * rows : (j + 1) * rows, :] = tile[:, j * LANES : (j + 1) * LANES]


def unstacked(value, rows):
    parts = value.shape[0] // rows
    return jnp.concatenate([value[j * rows : (j + 1) * rows] for j in range(parts)], axis=1)


def opening_kernel(sizes_ref, wave_ref, diag_ref, send_ref, current_ref, square_ref):
    z, chip, core = place()
    wave = wave_ref[0]
    inside = live(wave.shape, (chip * 2 + core) * SHARE, sizes_ref[z])
    current = jnp.where(inside, wave, 0.0)
    current_ref[...] = current
    square_ref[...] = jnp.full((8, LANES), jnp.sum(current * current), F32)
    diag = diag_ref[0]
    high = diag.astype(BF)
    low = (diag - high.astype(F32)).astype(BF)
    current_low = current.astype(BF)
    for peer in range(send_ref.shape[0]):
        send_ref[peer, 0] = current_low
        send_ref[peer, 1] = high
        send_ref[peer, 2] = low


def halves_of(z, width):
    half = z % 2
    near = pl.ds(pl.multiple_of(half * width, width), width)
    far = pl.ds(pl.multiple_of((1 - half) * width, width), width)
    return near, far


def slabs(rows_at, send_ref):
    z, _, _ = place()
    chips, count, _, width = send_ref.shape
    near, far = halves_of(z, width)
    for k in range(count):
        if k < count - 2:
            slab = rows_at(k, near)
        else:
            slab = rows_at((z // 2) * 2 + k - (count - 2), far)
        for chip in range(chips):
            send_ref[chip, k] = slab


def spreading_kernel(begun_ref, send_ref):
    slabs(lambda k, cut: begun_ref[k, 0, :, cut], send_ref)


def product_kernel(
    coupling_ref, mine_ref, theirs_ref, left_a, left_b, right_a, right_b, square_ref,
    keep_ref, give_ref, total, rows, rights, halves, sems,
):
    z, chip, core = place()
    target = (z // 2) * 2 + core
    block, width = total.shape[0], rows.shape[-1]
    pairs = left_a.shape[0]
    near, far = halves_of(z, width)

    def fetch(pair):
        return pltpu.make_async_copy(
            right_a.at[pair, :, near], rights.at[pair, :, :width], sems.at[pair, 0]
        )

    def move(pair):
        return pltpu.make_async_copy(
            right_b.at[pair, :, near], rights.at[pair, :, width:], sems.at[pair, 1]
        )

    fetch(0).start()
    move(0).start()
    for k in range(rows.shape[0]):
        for at in range(mine_ref.shape[0]):
            turned = (at % 4) * 4 + at // 4
            rows[k, 2 * turned + core] = mine_ref[at, k]
            rows[k, 2 * turned + 1 - core] = theirs_ref[at, k]
    for pair in range(1, pairs):
        fetch(pair).start()
        move(pair).start()
    total[...] = jnp.zeros_like(total)

    def first(pair):
        for j, (owner, left) in enumerate(((core, left_a), (1 - core, left_b))):
            source = coupling_ref[target, (chip * 2 + owner) * pairs + pair]
            vector = rows[source].reshape(block, width)
            half = jnp.dot(left[pair], vector, preferred_element_type=F32)
            halves[pair % LAG1, :, j * width : (j + 1) * width] = half.astype(BF)

    def second(pair):
        total[...] += lax.dot_general(
            halves[pair % LAG1], rights[pair], (((1,), (1,)), ((), ())), preferred_element_type=F32
        )

    def both(pair, _):
        fetch(pair - LAG).wait()
        move(pair - LAG).wait()
        second(pair - LAG)
        first(pair)
        return 0

    for pair in range(LAG):
        first(pair)
    lax.fori_loop(LAG, pairs, both, 0)
    for pair in range(pairs - LAG, pairs):
        fetch(pair).wait()
        move(pair).wait()
    for pair in range(pairs - LAG, pairs):
        second(pair)

    here = rows[target].reshape(block, width).astype(F32)
    there = rows[rows.shape[0] - 2 + core].reshape(block, width).astype(F32)
    product = jnp.sum(here * total[:, near] + there * total[:, far])
    extra = three_way(product, square_ref[0, 0])
    for peer in range(keep_ref.shape[0]):
        for ref, side in ((keep_ref, core), (give_ref, 1 - core)):
            at = pl.multiple_of(peer * 2 * SHARE + side * SHARE, SHARE)
            stacked(ref, peer, total[pl.ds(at, SHARE), :].astype(BF))
        give_ref[peer, block // 8 :, :] = extra


def products(coupling, mine, theirs, left, right, left_other, right_other, square):
    pairs, block, _ = left.shape
    chips, count, share, width = mine.shape
    return pl.pallas_call(
        product_kernel,
        in_specs=[SMEM, VMEM, VMEM, VMEM, VMEM, HBM, VMEM, VMEM],
        out_specs=[VMEM, VMEM],
        scratch_shapes=[
            pltpu.VMEM((block, block), F32),
            pltpu.VMEM((count, 2 * chips, share, width), BF),
            pltpu.VMEM((pairs, block, 2 * width), BF),
            pltpu.VMEM((LAG1, block, 2 * width), BF),
            pltpu.SemaphoreType.DMA((pairs, 2)),
        ],
        out_shape=[
            jax.ShapeDtypeStruct((chips, block // 8, LANES), BF),
            jax.ShapeDtypeStruct((chips, block // 8 + TILE, LANES), BF),
        ],
        compiler_params=pltpu.CompilerParams(vmem_limit_bytes=18 << 20),
        name="products",
    )(coupling, mine, theirs, left, left_other, right, right_other, square)


def pairing_kernel(keep_ref, give_ref, got_ref, send_ref):
    _, _, core = place()
    half = keep_ref.shape[1]
    here = pl.ds(pl.multiple_of(core * half, half), half)
    there = pl.ds(pl.multiple_of((1 - core) * half, half), half)
    both = give_ref[0, half:].astype(F32) + got_ref[0, half:].astype(F32)
    extra = three_way(*two_sums(both))
    for peer in range(send_ref.shape[0]):
        turned = (peer % 4) * 4 + peer // 4
        send_ref[peer, here, :] = keep_ref[turned]
        send_ref[peer, there, :] = got_ref[turned, :half, :]
        send_ref[peer, 2 * half :, :] = extra


def joining_kernel(sizes_ref, arrived_ref, send_ref):
    z, chip, core = place()
    total = arrived_ref[0].astype(F32)
    for peer in range(1, arrived_ref.shape[0]):
        total = total + arrived_ref[peer].astype(F32)
    end = total.shape[0] - TILE
    half = end // 2
    extra = three_way(*two_sums(total[end:]))
    for j in range(2):
        sigma = unstacked(total[j * half : (j + 1) * half], SHARE)
        first_row = (chip * 2 + core) * SHARE
        inside = live(sigma.shape, first_row, sizes_ref[(z // 2) * 2 + j])
        low = jnp.where(inside, sigma, 0.0).astype(BF)
        for k in range(low.shape[1] // LANES):
            at = j * half + k * SHARE
            part = low[:, k * LANES : (k + 1) * LANES]
            for peer in range(send_ref.shape[0]):
                send_ref[peer, at : at + SHARE, :] = part
    for peer in range(send_ref.shape[0]):
        send_ref[peer, end:, :] = extra


def scalars_of(arrived_ref):
    at = arrived_ref.shape[1] - TILE
    total = arrived_ref[0, at:].astype(F32)
    for peer in range(1, arrived_ref.shape[0]):
        total = total + arrived_ref[peer, at:].astype(F32)
    return two_sums(total)


def sigma_of(arrived_ref, target):
    half = (arrived_ref.shape[1] - TILE) // 2
    at = (target // 2) * 2
    if isinstance(target, int):
        part = slice((target % 2) * half, (target % 2 + 1) * half)
    else:
        part = pl.ds(pl.multiple_of((target % 2) * half, half), half)
    both = arrived_ref[at, part, :].astype(F32) + arrived_ref[at + 1, part, :].astype(F32)
    return unstacked(both, SHARE)


def corrected(current, sigma, diag, theta):
    gap = diag - theta
    return current - (sigma - theta * current) * gap / (gap * gap + 1.0)


def middle_kernel(
    arrived_ref, begun_ref, current_ref, diag_ref,
    send_ref, all_ref, own_ref, square_ref, theta_ref, low_ref,
):
    z, _, _ = place()
    first, second = scalars_of(arrived_ref)
    theta = first / (second + 1e-6)
    theta_ref[0] = theta[0, 0]
    for k in range(all_ref.shape[0]):
        diag = begun_ref[k, 1].astype(F32) + begun_ref[k, 2].astype(F32)
        update = corrected(begun_ref[k, 0].astype(F32), sigma_of(arrived_ref, k), diag, theta)
        all_ref[k] = update
        low_ref[k] = update.astype(BF)
    own = corrected(current_ref[...], sigma_of(arrived_ref, z), diag_ref[0], theta)
    own_ref[...] = own
    square_ref[...] = jnp.full((8, LANES), jnp.sum(own * own), F32)
    slabs(lambda k, cut: low_ref[k, :, cut], send_ref)


def closing_kernel(
    entries, arrived_ref, begun_ref, all_ref, own_ref, diag_ref, before_ref,
    final_ref, send_ref, theta_ref,
):
    z, _, _ = place()
    first, second = scalars_of(arrived_ref)
    scale = lax.rsqrt(second / entries + 1e-6)
    squared = scale * scale
    theta = squared * first / (squared * second + 1e-6)
    theta_ref[0] = before_ref[0]
    theta_ref[1] = theta[0, 0]
    total = jnp.zeros(all_ref.shape[1:], F32)
    for k in range(all_ref.shape[0]):
        diag = begun_ref[k, 1].astype(F32) + begun_ref[k, 2].astype(F32)
        update = corrected(scale * all_ref[k], scale * sigma_of(arrived_ref, k), diag, theta)
        total = total + update * update
    sigma = sigma_of(arrived_ref, z)
    final_ref[...] = corrected(scale * own_ref[...], scale * sigma, diag_ref[0], theta)
    send_ref[...] = jnp.full(send_ref.shape, jnp.sum(total), F32)


def scaling_kernel(entries, arrived_ref, final_ref, vector_ref):
    total = arrived_ref[0]
    for peer in range(1, arrived_ref.shape[0]):
        total = total + arrived_ref[peer]
    vector_ref[0] = final_ref[...] * lax.rsqrt(total[0:1, 0:1] / entries + 1e-6)


def call(kernel, shapes, specs, name, scratch=(), outs=None):
    return pl.pallas_call(
        kernel,
        in_specs=specs,
        out_specs=outs or [VMEM] * len(shapes),
        out_shape=[jax.ShapeDtypeStruct(s, t) for s, t in shapes],
        scratch_shapes=scratch,
        compiler_params=pltpu.CompilerParams(vmem_limit_bytes=16 << 20),
        name=name,
    )


def shards(wavefunction, diagonal, left_blocks, right_blocks, coupling, sector_sizes):
    _, share, block = wavefunction.shape
    sectors = lax.axis_size("sector")
    chips = lax.axis_size("op_0") * lax.axis_size("op_1")
    width = block // 2
    left_other = other_core(left_blocks)
    right_other = other_core(right_blocks)
    opening_inputs = tuple(
        pltpu.with_memory_space_constraint(x, pltpu.HBM)
        for x in (sector_sizes, wavefunction, diagonal)
    )
    right_blocks = pltpu.with_memory_space_constraint(right_blocks, pltpu.HBM)
    entries = float(sectors * block * block)
    spread = ((chips, sectors + 2, share, width), BF)
    scalar = ((8, LANES), F32)

    begin, current, square = call(
        opening_kernel,
        [((sectors, 3, share, block), BF), ((share, block), F32), scalar],
        [SMEM, VMEM, VMEM],
        "opening",
    )(*opening_inputs)
    begun = swap_all(begin, "sector")
    (outgoing,) = call(spreading_kernel, [spread], [VMEM], "spreading")(begun)

    def sigma_step(outgoing, square):
        mine = swap_all(outgoing, CHIP)
        keep, give = products(
            coupling, mine, other_core(mine),
            left_blocks, right_blocks, left_other, right_other, square,
        )
        (send,) = call(
            pairing_kernel,
            [((chips, block // 4 + TILE, LANES), BF)],
            [VMEM] * 3,
            "pairing",
        )(keep, give, other_core(give))
        (send,) = call(
            joining_kernel,
            [((sectors, block // 4 + TILE, LANES), BF)],
            [SMEM, VMEM],
            "joining",
        )(sector_sizes, swap_all(send, CHIP))
        return swap_all(send, "sector")

    arrived = sigma_step(outgoing, square)
    outgoing, everyone, own, square, theta = call(
        middle_kernel,
        [spread, ((sectors, share, block), F32), ((share, block), F32), scalar, ((1,), F32)],
        [VMEM] * 4,
        "middle",
        [pltpu.VMEM((sectors, share, block), BF)],
        [VMEM, VMEM, VMEM, VMEM, SMEM],
    )(arrived, begun, current, diagonal)

    arrived = sigma_step(outgoing, square)
    final, send, thetas = call(
        functools.partial(closing_kernel, entries),
        [((share, block), F32), ((chips * 2, 8, LANES), F32), ((2,), F32)],
        [VMEM, VMEM, VMEM, VMEM, VMEM, SMEM],
        "closing",
        outs=[VMEM, VMEM, SMEM],
    )(arrived, begun, everyone, own, diagonal, theta)
    (vector,) = call(
        functools.partial(scaling_kernel, entries),
        [((1, share, block), F32)],
        [VMEM] * 2,
        "scaling",
    )(swap_all(send, OP), final)
    return vector, thetas


def solution(mesh):
    split = Mesh(
        mesh.devices.reshape(mesh.shape["sector"], 4, 4, 2), ("sector", "op_0", "op_1", "op_2")
    )
    in_specs = (
        P("sector", OP, None),
        P("sector", OP, None),
        P(OP, None, None),
        P(OP, None, None),
        P(),
        P(),
    )
    out_specs = (P("sector", OP, None), P())
    return jax.shard_map(
        shards, mesh=split, in_specs=in_specs, out_specs=out_specs, check_vma=False
    )
```

```python
import functools
import jax
import jax.numpy as jnp
from jax import lax
from jax.experimental import pallas as pl
from jax.experimental.pallas import tpu as pltpu
from jax.sharding import Mesh
from jax.sharding import PartitionSpec as P

OP = ("op_0", "op_1", "op_2")
CHIP = ("op_1", "op_0")
CORE = "op_2"
BF = jnp.bfloat16
F32 = jnp.float32
VMEM = pl.BlockSpec(memory_space=pltpu.VMEM)
SMEM = pl.BlockSpec(memory_space=pltpu.SMEM)
HBM = pl.BlockSpec(memory_space=pltpu.HBM)
SHARE = 16
LANES = 128
TILE = 8
LAG = 3
LAG1 = LAG + 1


def swap_all(x, axes):
    return lax.all_to_all(x, axes, split_axis=0, concat_axis=0, tiled=True)


def other_core(x):
    return lax.ppermute(x, CORE, [(0, 1), (1, 0)])


def three_way(first, second):
    row = lax.broadcasted_iota(jnp.int32, (TILE, LANES), 0)
    value = jnp.where(row < 3, first, second)
    high = value.astype(BF).astype(F32)
    middle = (value - high).astype(BF).astype(F32)
    low = value - high - middle
    part = jnp.where(row < 3, row, row - 3)
    return jnp.where(part == 0, high, jnp.where(part == 1, middle, low)).astype(BF)


def two_sums(tile):
    first = tile[0:1] + tile[1:2] + tile[2:3]
    second = tile[3:4] + tile[4:5] + tile[5:6]
    return first[:, :1], second[:, :1]


def place():
    z = lax.axis_index("sector")
    chip = lax.axis_index("op_0") * lax.axis_size("op_1") + lax.axis_index("op_1")
    return z, chip, lax.axis_index(CORE)


def live(shape, first_row, size):
    row = lax.broadcasted_iota(jnp.int32, shape, 0) + first_row
    column = lax.broadcasted_iota(jnp.int32, shape, 1)
    return (row < size) & (column < size)


def stacked(ref, lead, tile):
    rows, block = tile.shape
    for j in range(block // LANES):
        ref[lead, j * rows : (j + 1) * rows, :] = tile[:, j * LANES : (j + 1) * LANES]


def unstacked(value, rows):
    parts = value.shape[0] // rows
    return jnp.concatenate([value[j * rows : (j + 1) * rows] for j in range(parts)], axis=1)


def opening_kernel(sizes_ref, wave_ref, diag_ref, send_ref, current_ref, square_ref):
    z, chip, core = place()
    wave = wave_ref[0]
    inside = live(wave.shape, (chip * 2 + core) * SHARE, sizes_ref[z])
    current = jnp.where(inside, wave, 0.0)
    current_ref[...] = current
    square_ref[...] = jnp.full((8, LANES), jnp.sum(current * current), F32)
    diag = diag_ref[0]
    high = diag.astype(BF)
    low = (diag - high.astype(F32)).astype(BF)
    current_low = current.astype(BF)
    for peer in range(send_ref.shape[0]):
        send_ref[peer, 0] = current_low
        send_ref[peer, 1] = high
        send_ref[peer, 2] = low


def halves_of(z, width):
    half = z % 2
    near = pl.ds(pl.multiple_of(half * width, width), width)
    far = pl.ds(pl.multiple_of((1 - half) * width, width), width)
    return near, far


def slabs(rows_at, send_ref):
    z, _, _ = place()
    chips, count, _, width = send_ref.shape
    near, far = halves_of(z, width)
    for k in range(count):
        if k < count - 2:
            slab = rows_at(k, near)
        else:
            slab = rows_at((z // 2) * 2 + k - (count - 2), far)
        for chip in range(chips):
            send_ref[chip, k] = slab


def spreading_kernel(begun_ref, send_ref):
    slabs(lambda k, cut: begun_ref[k, 0, :, cut], send_ref)


def product_kernel(
    coupling_ref, mine_ref, theirs_ref, left_a, left_b, right_a, right_b, square_ref,
    keep_ref, give_ref, total, rows, rights, halves, sems,
):
    z, chip, core = place()
    target = (z // 2) * 2 + core
    block, width = total.shape[0], rows.shape[-1]
    pairs = left_a.shape[0]
    near, far = halves_of(z, width)

    def fetch(pair):
        return pltpu.make_async_copy(
            right_a.at[pair, :, near], rights.at[pair, :, :width], sems.at[pair, 0]
        )

    def move(pair):
        return pltpu.make_async_copy(
            right_b.at[pair, :, near], rights.at[pair, :, width:], sems.at[pair, 1]
        )

    fetch(0).start()
    move(0).start()
    for k in range(rows.shape[0]):
        for at in range(mine_ref.shape[0]):
            turned = (at % 4) * 4 + at // 4
            rows[k, 2 * turned + core] = mine_ref[at, k]
            rows[k, 2 * turned + 1 - core] = theirs_ref[at, k]
    for pair in range(1, pairs):
        fetch(pair).start()
        move(pair).start()
    total[...] = jnp.zeros_like(total)

    def first(pair):
        for j, (owner, left) in enumerate(((core, left_a), (1 - core, left_b))):
            source = coupling_ref[target, (chip * 2 + owner) * pairs + pair]
            vector = rows[source].reshape(block, width)
            half = jnp.dot(left[pair], vector, preferred_element_type=F32)
            halves[pair % LAG1, :, j * width : (j + 1) * width] = half.astype(BF)

    def second(pair):
        total[...] += lax.dot_general(
            halves[pair % LAG1], rights[pair], (((1,), (1,)), ((), ())), preferred_element_type=F32
        )

    def both(pair, _):
        fetch(pair - LAG).wait()
        move(pair - LAG).wait()
        second(pair - LAG)
        first(pair)
        return 0

    for pair in range(LAG):
        first(pair)
    lax.fori_loop(LAG, pairs, both, 0)
    for pair in range(pairs - LAG, pairs):
        fetch(pair).wait()
        move(pair).wait()
    for pair in range(pairs - LAG, pairs):
        second(pair)

    here = rows[target].reshape(block, width).astype(F32)
    there = rows[rows.shape[0] - 2 + core].reshape(block, width).astype(F32)
    product = jnp.sum(here * total[:, near] + there * total[:, far])
    extra = three_way(product, square_ref[0, 0])
    for peer in range(keep_ref.shape[0]):
        for ref, side in ((keep_ref, core), (give_ref, 1 - core)):
            at = pl.multiple_of(peer * 2 * SHARE + side * SHARE, SHARE)
            stacked(ref, peer, total[pl.ds(at, SHARE), :].astype(BF))
        give_ref[peer, block // 8 :, :] = extra


def products(coupling, mine, theirs, left, right, left_other, right_other, square):
    pairs, block, _ = left.shape
    chips, count, share, width = mine.shape
    return pl.pallas_call(
        product_kernel,
        in_specs=[SMEM, VMEM, VMEM, VMEM, VMEM, HBM, VMEM, VMEM],
        out_specs=[VMEM, VMEM],
        scratch_shapes=[
            pltpu.VMEM((block, block), F32),
            pltpu.VMEM((count, 2 * chips, share, width), BF),
            pltpu.VMEM((pairs, block, 2 * width), BF),
            pltpu.VMEM((LAG1, block, 2 * width), BF),
            pltpu.SemaphoreType.DMA((pairs, 2)),
        ],
        out_shape=[
            jax.ShapeDtypeStruct((chips, block // 8, LANES), BF),
            jax.ShapeDtypeStruct((chips, block // 8 + TILE, LANES), BF),
        ],
        compiler_params=pltpu.CompilerParams(vmem_limit_bytes=18 << 20),
        name="products",
    )(coupling, mine, theirs, left, left_other, right, right_other, square)


def pairing_kernel(keep_ref, give_ref, got_ref, send_ref):
    _, _, core = place()
    half = keep_ref.shape[1]
    here = pl.ds(pl.multiple_of(core * half, half), half)
    there = pl.ds(pl.multiple_of((1 - core) * half, half), half)
    both = give_ref[0, half:].astype(F32) + got_ref[0, half:].astype(F32)
    extra = three_way(*two_sums(both))
    for peer in range(send_ref.shape[0]):
        turned = (peer % 4) * 4 + peer // 4
        send_ref[peer, here, :] = keep_ref[turned]
        send_ref[peer, there, :] = got_ref[turned, :half, :]
        send_ref[peer, 2 * half :, :] = extra


def joining_kernel(sizes_ref, arrived_ref, send_ref):
    z, chip, core = place()
    total = arrived_ref[0].astype(F32)
    for peer in range(1, arrived_ref.shape[0]):
        total = total + arrived_ref[peer].astype(F32)
    end = total.shape[0] - TILE
    half = end // 2
    extra = three_way(*two_sums(total[end:]))
    for j in range(2):
        sigma = unstacked(total[j * half : (j + 1) * half], SHARE)
        first_row = (chip * 2 + core) * SHARE
        inside = live(sigma.shape, first_row, sizes_ref[(z // 2) * 2 + j])
        low = jnp.where(inside, sigma, 0.0).astype(BF)
        for k in range(low.shape[1] // LANES):
            at = j * half + k * SHARE
            part = low[:, k * LANES : (k + 1) * LANES]
            for peer in range(send_ref.shape[0]):
                send_ref[peer, at : at + SHARE, :] = part
    for peer in range(send_ref.shape[0]):
        send_ref[peer, end:, :] = extra


def scalars_of(arrived_ref):
    at = arrived_ref.shape[1] - TILE
    total = arrived_ref[0, at:].astype(F32)
    for peer in range(1, arrived_ref.shape[0]):
        total = total + arrived_ref[peer, at:].astype(F32)
    return two_sums(total)


def sigma_of(arrived_ref, target):
    half = (arrived_ref.shape[1] - TILE) // 2
    at = (target // 2) * 2
    if isinstance(target, int):
        part = slice((target % 2) * half, (target % 2 + 1) * half)
    else:
        part = pl.ds(pl.multiple_of((target % 2) * half, half), half)
    both = arrived_ref[at, part, :].astype(F32) + arrived_ref[at + 1, part, :].astype(F32)
    return unstacked(both, SHARE)


def corrected(current, sigma, diag, theta):
    gap = diag - theta
    return current - (sigma - theta * current) * gap / (gap * gap + 1.0)


def middle_kernel(
    arrived_ref, begun_ref, current_ref, diag_ref,
    send_ref, all_ref, own_ref, square_ref, theta_ref, low_ref,
):
    z, _, _ = place()
    first, second = scalars_of(arrived_ref)
    theta = first / (second + 1e-6)
    theta_ref[...] = jnp.broadcast_to(theta, (8, LANES))
    for k in range(all_ref.shape[0]):
        diag = begun_ref[k, 1].astype(F32) + begun_ref[k, 2].astype(F32)
        update = corrected(begun_ref[k, 0].astype(F32), sigma_of(arrived_ref, k), diag, theta)
        all_ref[k] = update
        low_ref[k] = update.astype(BF)
    own = corrected(current_ref[...], sigma_of(arrived_ref, z), diag_ref[0], theta)
    own_ref[...] = own
    square_ref[...] = jnp.full((8, LANES), jnp.sum(own * own), F32)
    slabs(lambda k, cut: low_ref[k, :, cut], send_ref)


def closing_kernel(
    entries, arrived_ref, begun_ref, all_ref, own_ref, diag_ref, before_ref,
    final_ref, send_ref, theta_ref,
):
    z, _, _ = place()
    first, second = scalars_of(arrived_ref)
    scale = lax.rsqrt(second / entries + 1e-6)
    squared = scale * scale
    theta = squared * first / (squared * second + 1e-6)
    lane = lax.broadcasted_iota(jnp.int32, (8, LANES), 1)
    theta_ref[...] = jnp.where(lane == 0, before_ref[...], theta)
    total = jnp.zeros(all_ref.shape[1:], F32)
    for k in range(all_ref.shape[0]):
        diag = begun_ref[k, 1].astype(F32) + begun_ref[k, 2].astype(F32)
        update = corrected(scale * all_ref[k], scale * sigma_of(arrived_ref, k), diag, theta)
        total = total + update * update
    sigma = sigma_of(arrived_ref, z)
    final_ref[...] = corrected(scale * own_ref[...], scale * sigma, diag_ref[0], theta)
    send_ref[...] = jnp.full(send_ref.shape, jnp.sum(total), F32)


def scaling_kernel(entries, arrived_ref, final_ref, theta_ref, vector_ref, energies_ref):
    energies_ref[0] = theta_ref[0, 0]
    energies_ref[1] = theta_ref[0, 1]
    total = arrived_ref[0]
    for peer in range(1, arrived_ref.shape[0]):
        total = total + arrived_ref[peer]
    vector_ref[0] = final_ref[...] * lax.rsqrt(total[0:1, 0:1] / entries + 1e-6)


def call(kernel, shapes, specs, name, scratch=(), outs=None):
    return pl.pallas_call(
        kernel,
        in_specs=specs,
        out_specs=outs or [VMEM] * len(shapes),
        out_shape=[jax.ShapeDtypeStruct(s, t) for s, t in shapes],
        scratch_shapes=scratch,
        compiler_params=pltpu.CompilerParams(vmem_limit_bytes=16 << 20),
        name=name,
    )


def shards(wavefunction, diagonal, left_blocks, right_blocks, coupling, sector_sizes):
    _, share, block = wavefunction.shape
    sectors = lax.axis_size("sector")
    chips = lax.axis_size("op_0") * lax.axis_size("op_1")
    width = block // 2
    left_other = other_core(left_blocks)
    right_other = other_core(right_blocks)
    opening_inputs = tuple(
        pltpu.with_memory_space_constraint(x, pltpu.HBM)
        for x in (sector_sizes, wavefunction, diagonal)
    )
    right_blocks = pltpu.with_memory_space_constraint(right_blocks, pltpu.HBM)
    entries = float(sectors * block * block)
    spread = ((chips, sectors + 2, share, width), BF)
    scalar = ((8, LANES), F32)

    begin, current, square = call(
        opening_kernel,
        [((sectors, 3, share, block), BF), ((share, block), F32), scalar],
        [SMEM, VMEM, VMEM],
        "opening",
    )(*opening_inputs)
    begun = swap_all(begin, "sector")
    (outgoing,) = call(spreading_kernel, [spread], [VMEM], "spreading")(begun)

    def sigma_step(outgoing, square):
        mine = swap_all(outgoing, CHIP)
        keep, give = products(
            coupling, mine, other_core(mine),
            left_blocks, right_blocks, left_other, right_other, square,
        )
        (send,) = call(
            pairing_kernel,
            [((chips, block // 4 + TILE, LANES), BF)],
            [VMEM] * 3,
            "pairing",
        )(keep, give, other_core(give))
        (send,) = call(
            joining_kernel,
            [((sectors, block // 4 + TILE, LANES), BF)],
            [SMEM, VMEM],
            "joining",
        )(sector_sizes, swap_all(send, CHIP))
        return swap_all(send, "sector")

    arrived = sigma_step(outgoing, square)
    outgoing, everyone, own, square, theta = call(
        middle_kernel,
        [spread, ((sectors, share, block), F32), ((share, block), F32), scalar, scalar],
        [VMEM] * 4,
        "middle",
        [pltpu.VMEM((sectors, share, block), BF)],
    )(arrived, begun, current, diagonal)

    arrived = sigma_step(outgoing, square)
    final, send, thetas = call(
        functools.partial(closing_kernel, entries),
        [((share, block), F32), ((chips * 2, 8, LANES), F32), scalar],
        [VMEM] * 6,
        "closing",
    )(arrived, begun, everyone, own, diagonal, theta)
    vector, energies = call(
        functools.partial(scaling_kernel, entries),
        [((1, share, block), F32), ((2,), F32)],
        [VMEM] * 3,
        "scaling",
        outs=[VMEM, SMEM],
    )(swap_all(send, OP), final, thetas)
    return vector, energies


def solution(mesh):
    split = Mesh(
        mesh.devices.reshape(mesh.shape["sector"], 4, 4, 2), ("sector", "op_0", "op_1", "op_2")
    )
    in_specs = (
        P("sector", OP, None),
        P("sector", OP, None),
        P(OP, None, None),
        P(OP, None, None),
        P(),
        P(),
    )
    out_specs = (P("sector", OP, None), P())
    return jax.shard_map(
        shards, mesh=split, in_specs=in_specs, out_specs=out_specs, check_vma=False
    )
```

```python
import functools
import jax
import jax.numpy as jnp
from jax import lax
from jax.experimental import pallas as pl
from jax.experimental.pallas import tpu as pltpu
from jax.sharding import Mesh
from jax.sharding import PartitionSpec as P

OP = ("op_0", "op_1", "op_2")
CHIP = ("op_1", "op_0")
CORE = "op_2"
BF = jnp.bfloat16
F32 = jnp.float32
VMEM = pl.BlockSpec(memory_space=pltpu.VMEM)
SMEM = pl.BlockSpec(memory_space=pltpu.SMEM)
HBM = pl.BlockSpec(memory_space=pltpu.HBM)
SHARE = 16
LANES = 128
TILE = 8
LAG = 3
LAG1 = LAG + 1


def swap_all(x, axes):
    return lax.all_to_all(x, axes, split_axis=0, concat_axis=0, tiled=True)


def other_core(x):
    return lax.ppermute(x, CORE, [(0, 1), (1, 0)])


def three_way(first, second):
    row = lax.broadcasted_iota(jnp.int32, (TILE, LANES), 0)
    value = jnp.where(row < 3, first, second)
    high = value.astype(BF).astype(F32)
    middle = (value - high).astype(BF).astype(F32)
    low = value - high - middle
    part = jnp.where(row < 3, row, row - 3)
    return jnp.where(part == 0, high, jnp.where(part == 1, middle, low)).astype(BF)


def two_sums(tile):
    first = tile[0:1] + tile[1:2] + tile[2:3]
    second = tile[3:4] + tile[4:5] + tile[5:6]
    return first[:, :1], second[:, :1]


def place():
    z = lax.axis_index("sector")
    chip = lax.axis_index("op_0") * lax.axis_size("op_1") + lax.axis_index("op_1")
    return z, chip, lax.axis_index(CORE)


def live(shape, first_row, size):
    row = lax.broadcasted_iota(jnp.int32, shape, 0) + first_row
    column = lax.broadcasted_iota(jnp.int32, shape, 1)
    return (row < size) & (column < size)


def stacked(ref, lead, tile):
    rows, block = tile.shape
    for j in range(block // LANES):
        ref[lead, j * rows : (j + 1) * rows, :] = tile[:, j * LANES : (j + 1) * LANES]


def unstacked(value, rows):
    parts = value.shape[0] // rows
    return jnp.concatenate([value[j * rows : (j + 1) * rows] for j in range(parts)], axis=1)


def opening_kernel(
    sizes_ref, wave_ref, diag_ref, send_ref, current_ref, square_ref, extent_ref
):
    z, chip, core = place()
    row = lax.broadcasted_iota(jnp.int32, (8, LANES), 0)
    extent = jnp.full((8, LANES), sizes_ref[0], jnp.int32)
    for k in range(1, 8):
        extent = jnp.where(row == k, sizes_ref[k], extent)
    extent_ref[...] = extent
    wave = wave_ref[0]
    inside = live(wave.shape, (chip * 2 + core) * SHARE, sizes_ref[z])
    current = jnp.where(inside, wave, 0.0)
    current_ref[...] = current
    square_ref[...] = jnp.full((8, LANES), jnp.sum(current * current), F32)
    diag = diag_ref[0]
    high = diag.astype(BF)
    low = (diag - high.astype(F32)).astype(BF)
    current_low = current.astype(BF)
    for peer in range(send_ref.shape[0]):
        send_ref[peer, 0] = current_low
        send_ref[peer, 1] = high
        send_ref[peer, 2] = low


def halves_of(z, width):
    half = z % 2
    near = pl.ds(pl.multiple_of(half * width, width), width)
    far = pl.ds(pl.multiple_of((1 - half) * width, width), width)
    return near, far


def slabs(rows_at, send_ref):
    z, _, _ = place()
    chips, count, _, width = send_ref.shape
    near, far = halves_of(z, width)
    for k in range(count):
        if k < count - 2:
            slab = rows_at(k, near)
        else:
            slab = rows_at((z // 2) * 2 + k - (count - 2), far)
        for chip in range(chips):
            send_ref[chip, k] = slab


def spreading_kernel(begun_ref, send_ref):
    slabs(lambda k, cut: begun_ref[k, 0, :, cut], send_ref)


def product_kernel(
    coupling_ref, mine_ref, theirs_ref, left_a, left_b, right_a, right_b, square_ref,
    keep_ref, give_ref, total, rows, rights, halves, sems,
):
    z, chip, core = place()
    target = (z // 2) * 2 + core
    block, width = total.shape[0], rows.shape[-1]
    pairs = left_a.shape[0]
    near, far = halves_of(z, width)

    def fetch(pair):
        return pltpu.make_async_copy(
            right_a.at[pair, :, near], rights.at[pair, :, :width], sems.at[pair, 0]
        )

    def move(pair):
        return pltpu.make_async_copy(
            right_b.at[pair, :, near], rights.at[pair, :, width:], sems.at[pair, 1]
        )

    fetch(0).start()
    move(0).start()
    for k in range(rows.shape[0]):
        for at in range(mine_ref.shape[0]):
            turned = (at % 4) * 4 + at // 4
            rows[k, 2 * turned + core] = mine_ref[at, k]
            rows[k, 2 * turned + 1 - core] = theirs_ref[at, k]
    for pair in range(1, pairs):
        fetch(pair).start()
        move(pair).start()
    total[...] = jnp.zeros_like(total)

    def first(pair):
        for j, (owner, left) in enumerate(((core, left_a), (1 - core, left_b))):
            source = coupling_ref[target, (chip * 2 + owner) * pairs + pair]
            vector = rows[source].reshape(block, width)
            half = jnp.dot(left[pair], vector, preferred_element_type=F32)
            halves[pair % LAG1, :, j * width : (j + 1) * width] = half.astype(BF)

    def second(pair):
        total[...] += lax.dot_general(
            halves[pair % LAG1], rights[pair], (((1,), (1,)), ((), ())), preferred_element_type=F32
        )

    def both(pair, _):
        fetch(pair - LAG).wait()
        move(pair - LAG).wait()
        second(pair - LAG)
        first(pair)
        return 0

    for pair in range(LAG):
        first(pair)
    lax.fori_loop(LAG, pairs, both, 0)
    for pair in range(pairs - LAG, pairs):
        fetch(pair).wait()
        move(pair).wait()
    for pair in range(pairs - LAG, pairs):
        second(pair)

    here = rows[target].reshape(block, width).astype(F32)
    there = rows[rows.shape[0] - 2 + core].reshape(block, width).astype(F32)
    product = jnp.sum(here * total[:, near] + there * total[:, far])
    extra = three_way(product, square_ref[0, 0])
    for peer in range(keep_ref.shape[0]):
        for ref, side in ((keep_ref, core), (give_ref, 1 - core)):
            at = pl.multiple_of(peer * 2 * SHARE + side * SHARE, SHARE)
            stacked(ref, peer, total[pl.ds(at, SHARE), :].astype(BF))
        give_ref[peer, block // 8 :, :] = extra


def products(coupling, mine, theirs, left, right, left_other, right_other, square):
    pairs, block, _ = left.shape
    chips, count, share, width = mine.shape
    return pl.pallas_call(
        product_kernel,
        in_specs=[SMEM, VMEM, VMEM, VMEM, VMEM, HBM, VMEM, VMEM],
        out_specs=[VMEM, VMEM],
        scratch_shapes=[
            pltpu.VMEM((block, block), F32),
            pltpu.VMEM((count, 2 * chips, share, width), BF),
            pltpu.VMEM((pairs, block, 2 * width), BF),
            pltpu.VMEM((LAG1, block, 2 * width), BF),
            pltpu.SemaphoreType.DMA((pairs, 2)),
        ],
        out_shape=[
            jax.ShapeDtypeStruct((chips, block // 8, LANES), BF),
            jax.ShapeDtypeStruct((chips, block // 8 + TILE, LANES), BF),
        ],
        compiler_params=pltpu.CompilerParams(vmem_limit_bytes=18 << 20),
        name="products",
    )(coupling, mine, theirs, left, left_other, right, right_other, square)


def pairing_kernel(keep_ref, give_ref, got_ref, send_ref):
    _, _, core = place()
    half = keep_ref.shape[1]
    here = pl.ds(pl.multiple_of(core * half, half), half)
    there = pl.ds(pl.multiple_of((1 - core) * half, half), half)
    both = give_ref[0, half:].astype(F32) + got_ref[0, half:].astype(F32)
    extra = three_way(*two_sums(both))
    for peer in range(send_ref.shape[0]):
        turned = (peer % 4) * 4 + peer // 4
        send_ref[peer, here, :] = keep_ref[turned]
        send_ref[peer, there, :] = got_ref[turned, :half, :]
        send_ref[peer, 2 * half :, :] = extra


def joining_kernel(extent_ref, arrived_ref, send_ref):
    z, chip, core = place()
    total = arrived_ref[0].astype(F32)
    for peer in range(1, arrived_ref.shape[0]):
        total = total + arrived_ref[peer].astype(F32)
    end = total.shape[0] - TILE
    half = end // 2
    extra = three_way(*two_sums(total[end:]))
    for j in range(2):
        sigma = unstacked(total[j * half : (j + 1) * half], SHARE)
        first_row = (chip * 2 + core) * SHARE
        size = extent_ref[pl.ds((z // 2) * 2 + j, 1), :][:, :1]
        inside = live(sigma.shape, first_row, size)
        low = jnp.where(inside, sigma, 0.0).astype(BF)
        for k in range(low.shape[1] // LANES):
            at = j * half + k * SHARE
            part = low[:, k * LANES : (k + 1) * LANES]
            for peer in range(send_ref.shape[0]):
                send_ref[peer, at : at + SHARE, :] = part
    for peer in range(send_ref.shape[0]):
        send_ref[peer, end:, :] = extra


def scalars_of(arrived_ref):
    at = arrived_ref.shape[1] - TILE
    total = arrived_ref[0, at:].astype(F32)
    for peer in range(1, arrived_ref.shape[0]):
        total = total + arrived_ref[peer, at:].astype(F32)
    return two_sums(total)


def sigma_of(arrived_ref, target):
    half = (arrived_ref.shape[1] - TILE) // 2
    at = (target // 2) * 2
    if isinstance(target, int):
        part = slice((target % 2) * half, (target % 2 + 1) * half)
    else:
        part = pl.ds(pl.multiple_of((target % 2) * half, half), half)
    both = arrived_ref[at, part, :].astype(F32) + arrived_ref[at + 1, part, :].astype(F32)
    return unstacked(both, SHARE)


def corrected(current, sigma, diag, theta):
    gap = diag - theta
    return current - (sigma - theta * current) * gap / (gap * gap + 1.0)


def middle_kernel(
    arrived_ref, begun_ref, current_ref, diag_ref,
    send_ref, all_ref, own_ref, square_ref, theta_ref, low_ref,
):
    z, _, _ = place()
    first, second = scalars_of(arrived_ref)
    theta = first / (second + 1e-6)
    theta_ref[...] = jnp.broadcast_to(theta, (8, LANES))
    for k in range(all_ref.shape[0]):
        diag = begun_ref[k, 1].astype(F32) + begun_ref[k, 2].astype(F32)
        update = corrected(begun_ref[k, 0].astype(F32), sigma_of(arrived_ref, k), diag, theta)
        all_ref[k] = update
        low_ref[k] = update.astype(BF)
    own = corrected(current_ref[...], sigma_of(arrived_ref, z), diag_ref[0], theta)
    own_ref[...] = own
    square_ref[...] = jnp.full((8, LANES), jnp.sum(own * own), F32)
    slabs(lambda k, cut: low_ref[k, :, cut], send_ref)


def closing_kernel(
    entries, arrived_ref, begun_ref, all_ref, own_ref, diag_ref, before_ref,
    final_ref, send_ref, theta_ref,
):
    z, _, _ = place()
    first, second = scalars_of(arrived_ref)
    scale = lax.rsqrt(second / entries + 1e-6)
    squared = scale * scale
    theta = squared * first / (squared * second + 1e-6)
    lane = lax.broadcasted_iota(jnp.int32, (8, LANES), 1)
    theta_ref[...] = jnp.where(lane == 0, before_ref[...], theta)
    total = jnp.zeros(all_ref.shape[1:], F32)
    for k in range(all_ref.shape[0]):
        diag = begun_ref[k, 1].astype(F32) + begun_ref[k, 2].astype(F32)
        update = corrected(scale * all_ref[k], scale * sigma_of(arrived_ref, k), diag, theta)
        total = total + update * update
    sigma = sigma_of(arrived_ref, z)
    final_ref[...] = corrected(scale * own_ref[...], scale * sigma, diag_ref[0], theta)
    send_ref[...] = jnp.full(send_ref.shape, jnp.sum(total), F32)


def scaling_kernel(entries, arrived_ref, final_ref, theta_ref, vector_ref, energies_ref):
    energies_ref[0] = theta_ref[0, 0]
    energies_ref[1] = theta_ref[0, 1]
    total = arrived_ref[0]
    for peer in range(1, arrived_ref.shape[0]):
        total = total + arrived_ref[peer]
    vector_ref[0] = final_ref[...] * lax.rsqrt(total[0:1, 0:1] / entries + 1e-6)


def call(kernel, shapes, specs, name, scratch=(), outs=None):
    return pl.pallas_call(
        kernel,
        in_specs=specs,
        out_specs=outs or [VMEM] * len(shapes),
        out_shape=[jax.ShapeDtypeStruct(s, t) for s, t in shapes],
        scratch_shapes=scratch,
        compiler_params=pltpu.CompilerParams(vmem_limit_bytes=16 << 20),
        name=name,
    )


def shards(wavefunction, diagonal, left_blocks, right_blocks, coupling, sector_sizes):
    _, share, block = wavefunction.shape
    sectors = lax.axis_size("sector")
    chips = lax.axis_size("op_0") * lax.axis_size("op_1")
    width = block // 2
    left_other = other_core(left_blocks)
    right_other = other_core(right_blocks)
    opening_inputs = tuple(
        pltpu.with_memory_space_constraint(x, pltpu.HBM)
        for x in (sector_sizes, wavefunction, diagonal)
    )
    right_blocks = pltpu.with_memory_space_constraint(right_blocks, pltpu.HBM)
    entries = float(sectors * block * block)
    spread = ((chips, sectors + 2, share, width), BF)
    scalar = ((8, LANES), F32)

    begin, current, square, extent = call(
        opening_kernel,
        [
            ((sectors, 3, share, block), BF),
            ((share, block), F32),
            scalar,
            ((8, LANES), jnp.int32),
        ],
        [SMEM, VMEM, VMEM],
        "opening",
    )(*opening_inputs)
    begun = swap_all(begin, "sector")
    (outgoing,) = call(spreading_kernel, [spread], [VMEM], "spreading")(begun)

    def sigma_step(outgoing, square):
        mine = swap_all(outgoing, CHIP)
        keep, give = products(
            coupling, mine, other_core(mine),
            left_blocks, right_blocks, left_other, right_other, square,
        )
        (send,) = call(
            pairing_kernel,
            [((chips, block // 4 + TILE, LANES), BF)],
            [VMEM] * 3,
            "pairing",
        )(keep, give, other_core(give))
        (send,) = call(
            joining_kernel,
            [((sectors, block // 4 + TILE, LANES), BF)],
            [VMEM] * 2,
            "joining",
        )(extent, swap_all(send, CHIP))
        return swap_all(send, "sector")

    arrived = sigma_step(outgoing, square)
    outgoing, everyone, own, square, theta = call(
        middle_kernel,
        [spread, ((sectors, share, block), F32), ((share, block), F32), scalar, scalar],
        [VMEM] * 4,
        "middle",
        [pltpu.VMEM((sectors, share, block), BF)],
    )(arrived, begun, current, diagonal)

    arrived = sigma_step(outgoing, square)
    final, send, thetas = call(
        functools.partial(closing_kernel, entries),
        [((share, block), F32), ((chips * 2, 8, LANES), F32), scalar],
        [VMEM] * 6,
        "closing",
    )(arrived, begun, everyone, own, diagonal, theta)
    vector, energies = call(
        functools.partial(scaling_kernel, entries),
        [((1, share, block), F32), ((2,), F32)],
        [VMEM] * 3,
        "scaling",
        outs=[VMEM, SMEM],
    )(swap_all(send, OP), final, thetas)
    return vector, energies


def solution(mesh):
    split = Mesh(
        mesh.devices.reshape(mesh.shape["sector"], 4, 4, 2), ("sector", "op_0", "op_1", "op_2")
    )
    in_specs = (
        P("sector", OP, None),
        P("sector", OP, None),
        P(OP, None, None),
        P(OP, None, None),
        P(),
        P(),
    )
    out_specs = (P("sector", OP, None), P())
    return jax.shard_map(
        shards, mesh=split, in_specs=in_specs, out_specs=out_specs, check_vma=False
    )
```

```python
import functools
import jax
import jax.numpy as jnp
from jax import lax
from jax.experimental import pallas as pl
from jax.experimental.pallas import tpu as pltpu
from jax.sharding import Mesh
from jax.sharding import PartitionSpec as P

OP = ("op_0", "op_1", "op_2")
CHIP = ("op_1", "op_0")
CORE = "op_2"
BF = jnp.bfloat16
F32 = jnp.float32
VMEM = pl.BlockSpec(memory_space=pltpu.VMEM)
SMEM = pl.BlockSpec(memory_space=pltpu.SMEM)
HBM = pl.BlockSpec(memory_space=pltpu.HBM)
SHARE = 16
LANES = 128
TILE = 8
LAG = 3
LAG1 = LAG + 1


def swap_all(x, axes):
    return lax.all_to_all(x, axes, split_axis=0, concat_axis=0, tiled=True)


def other_core(x):
    return lax.ppermute(x, CORE, [(0, 1), (1, 0)])


def three_way(first, second):
    row = lax.broadcasted_iota(jnp.int32, (TILE, LANES), 0)
    value = jnp.where(row < 3, first, second)
    high = value.astype(BF).astype(F32)
    middle = (value - high).astype(BF).astype(F32)
    low = value - high - middle
    part = jnp.where(row < 3, row, row - 3)
    return jnp.where(part == 0, high, jnp.where(part == 1, middle, low)).astype(BF)


def two_sums(tile):
    first = tile[0:1] + tile[1:2] + tile[2:3]
    second = tile[3:4] + tile[4:5] + tile[5:6]
    return first[:, :1], second[:, :1]


def place():
    z = lax.axis_index("sector")
    chip = lax.axis_index("op_0") * lax.axis_size("op_1") + lax.axis_index("op_1")
    return z, chip, lax.axis_index(CORE)


def live(shape, first_row, size):
    row = lax.broadcasted_iota(jnp.int32, shape, 0) + first_row
    column = lax.broadcasted_iota(jnp.int32, shape, 1)
    return (row < size) & (column < size)


def stacked(ref, lead, tile):
    rows, block = tile.shape
    for j in range(block // LANES):
        ref[lead, j * rows : (j + 1) * rows, :] = tile[:, j * LANES : (j + 1) * LANES]


def unstacked(value, rows):
    parts = value.shape[0] // rows
    return jnp.concatenate([value[j * rows : (j + 1) * rows] for j in range(parts)], axis=1)


def opening_kernel(
    sizes_ref, wave_ref, diag_ref, send_ref, current_ref, square_ref, extent_ref
):
    z, chip, core = place()
    row = lax.broadcasted_iota(jnp.int32, (8, LANES), 0)
    extent = jnp.full((8, LANES), sizes_ref[0], jnp.int32)
    for k in range(1, 8):
        extent = jnp.where(row == k, sizes_ref[k], extent)
    extent_ref[...] = extent
    wave = wave_ref[0]
    inside = live(wave.shape, (chip * 2 + core) * SHARE, sizes_ref[z])
    current = jnp.where(inside, wave, 0.0)
    current_ref[...] = current
    square_ref[...] = jnp.full((8, LANES), jnp.sum(current * current), F32)
    diag = diag_ref[0]
    high = diag.astype(BF)
    low = (diag - high.astype(F32)).astype(BF)
    current_low = current.astype(BF)
    for peer in range(send_ref.shape[0]):
        send_ref[peer, 0] = current_low
        send_ref[peer, 1] = high
        send_ref[peer, 2] = low


def halves_of(z, width):
    half = z % 2
    near = pl.ds(pl.multiple_of(half * width, width), width)
    far = pl.ds(pl.multiple_of((1 - half) * width, width), width)
    return near, far


def slabs(rows_at, send_ref):
    z, _, _ = place()
    chips, count, _, width = send_ref.shape
    near, far = halves_of(z, width)
    for k in range(count):
        if k < count - 2:
            slab = rows_at(k, near)
        else:
            slab = rows_at((z // 2) * 2 + k - (count - 2), far)
        for chip in range(chips):
            send_ref[chip, k] = slab


def spreading_kernel(begun_ref, send_ref):
    slabs(lambda k, cut: begun_ref[k, 0, :, cut], send_ref)


def product_kernel(
    coupling_ref, mine_ref, theirs_ref, left_a, left_b, right_a, right_b, square_ref,
    keep_ref, give_ref, total, rows, rights, halves, sems,
):
    z, chip, core = place()
    target = (z // 2) * 2 + core
    block, width = total.shape[0], rows.shape[-1]
    pairs = left_a.shape[0]
    near, far = halves_of(z, width)

    def fetch(pair):
        return pltpu.make_async_copy(
            right_a.at[pair, :, near], rights.at[pair, :, :width], sems.at[pair, 0]
        )

    def move(pair):
        return pltpu.make_async_copy(
            right_b.at[pair, :, near], rights.at[pair, :, width:], sems.at[pair, 1]
        )

    fetch(0).start()
    move(0).start()
    for k in range(rows.shape[0]):
        for at in range(mine_ref.shape[0]):
            turned = (at % 4) * 4 + at // 4
            rows[k, 2 * turned + core] = mine_ref[at, k]
            rows[k, 2 * turned + 1 - core] = theirs_ref[at, k]
    for pair in range(1, pairs):
        fetch(pair).start()
        move(pair).start()

    def first(pair):
        for j, (owner, left) in enumerate(((core, left_a), (1 - core, left_b))):
            source = coupling_ref[target, (chip * 2 + owner) * pairs + pair]
            vector = rows[source].reshape(block, width)
            half = jnp.dot(left[pair], vector, preferred_element_type=F32)
            halves[pair % LAG1, :, j * width : (j + 1) * width] = half.astype(BF)

    def second(pair, opening=False):
        term = lax.dot_general(
            halves[pair % LAG1], rights[pair], (((1,), (1,)), ((), ())), preferred_element_type=F32
        )
        total[...] = term if opening else total[...] + term

    def both(pair, _):
        fetch(pair - LAG).wait()
        move(pair - LAG).wait()
        second(pair - LAG)
        first(pair)
        return 0

    for pair in range(LAG):
        first(pair)
    fetch(0).wait()
    move(0).wait()
    second(0, True)
    first(LAG)
    lax.fori_loop(LAG + 1, pairs, both, 0)
    for pair in range(pairs - LAG, pairs):
        fetch(pair).wait()
        move(pair).wait()
    for pair in range(pairs - LAG, pairs):
        second(pair)

    here = rows[target].reshape(block, width).astype(F32)
    there = rows[rows.shape[0] - 2 + core].reshape(block, width).astype(F32)
    product = jnp.sum(here * total[:, near] + there * total[:, far])
    extra = three_way(product, square_ref[0, 0])
    for peer in range(keep_ref.shape[0]):
        for ref, side in ((keep_ref, core), (give_ref, 1 - core)):
            at = pl.multiple_of(peer * 2 * SHARE + side * SHARE, SHARE)
            stacked(ref, peer, total[pl.ds(at, SHARE), :].astype(BF))
        give_ref[peer, block // 8 :, :] = extra


def products(coupling, mine, theirs, left, right, left_other, right_other, square):
    pairs, block, _ = left.shape
    chips, count, share, width = mine.shape
    return pl.pallas_call(
        product_kernel,
        in_specs=[SMEM, VMEM, VMEM, VMEM, VMEM, HBM, VMEM, VMEM],
        out_specs=[VMEM, VMEM],
        scratch_shapes=[
            pltpu.VMEM((block, block), F32),
            pltpu.VMEM((count, 2 * chips, share, width), BF),
            pltpu.VMEM((pairs, block, 2 * width), BF),
            pltpu.VMEM((LAG1, block, 2 * width), BF),
            pltpu.SemaphoreType.DMA((pairs, 2)),
        ],
        out_shape=[
            jax.ShapeDtypeStruct((chips, block // 8, LANES), BF),
            jax.ShapeDtypeStruct((chips, block // 8 + TILE, LANES), BF),
        ],
        compiler_params=pltpu.CompilerParams(vmem_limit_bytes=18 << 20),
        name="products",
    )(coupling, mine, theirs, left, left_other, right, right_other, square)


def pairing_kernel(keep_ref, give_ref, got_ref, send_ref):
    _, _, core = place()
    half = keep_ref.shape[1]
    here = pl.ds(pl.multiple_of(core * half, half), half)
    there = pl.ds(pl.multiple_of((1 - core) * half, half), half)
    both = give_ref[0, half:].astype(F32) + got_ref[0, half:].astype(F32)
    extra = three_way(*two_sums(both))
    for peer in range(send_ref.shape[0]):
        turned = (peer % 4) * 4 + peer // 4
        send_ref[peer, here, :] = keep_ref[turned]
        send_ref[peer, there, :] = got_ref[turned, :half, :]
        send_ref[peer, 2 * half :, :] = extra


def joining_kernel(extent_ref, arrived_ref, send_ref):
    z, chip, core = place()
    total = arrived_ref[0].astype(F32)
    for peer in range(1, arrived_ref.shape[0]):
        total = total + arrived_ref[peer].astype(F32)
    end = total.shape[0] - TILE
    half = end // 2
    extra = three_way(*two_sums(total[end:]))
    for j in range(2):
        sigma = unstacked(total[j * half : (j + 1) * half], SHARE)
        first_row = (chip * 2 + core) * SHARE
        size = extent_ref[pl.ds((z // 2) * 2 + j, 1), :][:, :1]
        inside = live(sigma.shape, first_row, size)
        low = jnp.where(inside, sigma, 0.0).astype(BF)
        for k in range(low.shape[1] // LANES):
            at = j * half + k * SHARE
            part = low[:, k * LANES : (k + 1) * LANES]
            for peer in range(send_ref.shape[0]):
                send_ref[peer, at : at + SHARE, :] = part
    for peer in range(send_ref.shape[0]):
        send_ref[peer, end:, :] = extra


def scalars_of(arrived_ref):
    at = arrived_ref.shape[1] - TILE
    total = arrived_ref[0, at:].astype(F32)
    for peer in range(1, arrived_ref.shape[0]):
        total = total + arrived_ref[peer, at:].astype(F32)
    return two_sums(total)


def sigma_of(arrived_ref, target):
    half = (arrived_ref.shape[1] - TILE) // 2
    at = (target // 2) * 2
    if isinstance(target, int):
        part = slice((target % 2) * half, (target % 2 + 1) * half)
    else:
        part = pl.ds(pl.multiple_of((target % 2) * half, half), half)
    both = arrived_ref[at, part, :].astype(F32) + arrived_ref[at + 1, part, :].astype(F32)
    return unstacked(both, SHARE)


def corrected(current, sigma, diag, theta):
    gap = diag - theta
    return current - (sigma - theta * current) * gap / (gap * gap + 1.0)


def middle_kernel(
    arrived_ref, begun_ref, current_ref, diag_ref,
    send_ref, all_ref, own_ref, square_ref, theta_ref, low_ref,
):
    z, _, _ = place()
    first, second = scalars_of(arrived_ref)
    theta = first / (second + 1e-6)
    theta_ref[...] = jnp.broadcast_to(theta, (8, LANES))
    for k in range(all_ref.shape[0]):
        diag = begun_ref[k, 1].astype(F32) + begun_ref[k, 2].astype(F32)
        update = corrected(begun_ref[k, 0].astype(F32), sigma_of(arrived_ref, k), diag, theta)
        all_ref[k] = update
        low_ref[k] = update.astype(BF)
    own = corrected(current_ref[...], sigma_of(arrived_ref, z), diag_ref[0], theta)
    own_ref[...] = own
    square_ref[...] = jnp.full((8, LANES), jnp.sum(own * own), F32)
    slabs(lambda k, cut: low_ref[k, :, cut], send_ref)


def closing_kernel(
    entries, arrived_ref, begun_ref, all_ref, own_ref, diag_ref, before_ref,
    final_ref, send_ref, theta_ref,
):
    z, _, _ = place()
    first, second = scalars_of(arrived_ref)
    scale = lax.rsqrt(second / entries + 1e-6)
    squared = scale * scale
    theta = squared * first / (squared * second + 1e-6)
    lane = lax.broadcasted_iota(jnp.int32, (8, LANES), 1)
    theta_ref[...] = jnp.where(lane == 0, before_ref[...], theta)
    total = jnp.zeros(all_ref.shape[1:], F32)
    for k in range(all_ref.shape[0]):
        diag = begun_ref[k, 1].astype(F32) + begun_ref[k, 2].astype(F32)
        update = corrected(scale * all_ref[k], scale * sigma_of(arrived_ref, k), diag, theta)
        total = total + update * update
    sigma = sigma_of(arrived_ref, z)
    final_ref[...] = corrected(scale * own_ref[...], scale * sigma, diag_ref[0], theta)
    send_ref[...] = jnp.full(send_ref.shape, jnp.sum(total), F32)


def scaling_kernel(entries, arrived_ref, final_ref, theta_ref, vector_ref, energies_ref):
    energies_ref[0] = theta_ref[0, 0]
    energies_ref[1] = theta_ref[0, 1]
    total = arrived_ref[0]
    for peer in range(1, arrived_ref.shape[0]):
        total = total + arrived_ref[peer]
    vector_ref[0] = final_ref[...] * lax.rsqrt(total[0:1, 0:1] / entries + 1e-6)


def call(kernel, shapes, specs, name, scratch=(), outs=None):
    return pl.pallas_call(
        kernel,
        in_specs=specs,
        out_specs=outs or [VMEM] * len(shapes),
        out_shape=[jax.ShapeDtypeStruct(s, t) for s, t in shapes],
        scratch_shapes=scratch,
        compiler_params=pltpu.CompilerParams(vmem_limit_bytes=16 << 20),
        name=name,
    )


def shards(wavefunction, diagonal, left_blocks, right_blocks, coupling, sector_sizes):
    _, share, block = wavefunction.shape
    sectors = lax.axis_size("sector")
    chips = lax.axis_size("op_0") * lax.axis_size("op_1")
    width = block // 2
    left_other = other_core(left_blocks)
    right_other = other_core(right_blocks)
    opening_inputs = tuple(
        pltpu.with_memory_space_constraint(x, pltpu.HBM)
        for x in (sector_sizes, wavefunction, diagonal)
    )
    right_blocks = pltpu.with_memory_space_constraint(right_blocks, pltpu.HBM)
    entries = float(sectors * block * block)
    spread = ((chips, sectors + 2, share, width), BF)
    scalar = ((8, LANES), F32)

    begin, current, square, extent = call(
        opening_kernel,
        [
            ((sectors, 3, share, block), BF),
            ((share, block), F32),
            scalar,
            ((8, LANES), jnp.int32),
        ],
        [SMEM, VMEM, VMEM],
        "opening",
    )(*opening_inputs)
    begun = swap_all(begin, "sector")
    (outgoing,) = call(spreading_kernel, [spread], [VMEM], "spreading")(begun)

    def sigma_step(outgoing, square):
        mine = swap_all(outgoing, CHIP)
        keep, give = products(
            coupling, mine, other_core(mine),
            left_blocks, right_blocks, left_other, right_other, square,
        )
        (send,) = call(
            pairing_kernel,
            [((chips, block // 4 + TILE, LANES), BF)],
            [VMEM] * 3,
            "pairing",
        )(keep, give, other_core(give))
        (send,) = call(
            joining_kernel,
            [((sectors, block // 4 + TILE, LANES), BF)],
            [VMEM] * 2,
            "joining",
        )(extent, swap_all(send, CHIP))
        return swap_all(send, "sector")

    arrived = sigma_step(outgoing, square)
    outgoing, everyone, own, square, theta = call(
        middle_kernel,
        [spread, ((sectors, share, block), F32), ((share, block), F32), scalar, scalar],
        [VMEM] * 4,
        "middle",
        [pltpu.VMEM((sectors, share, block), BF)],
    )(arrived, begun, current, diagonal)

    arrived = sigma_step(outgoing, square)
    final, send, thetas = call(
        functools.partial(closing_kernel, entries),
        [((share, block), F32), ((chips * 2, 8, LANES), F32), scalar],
        [VMEM] * 6,
        "closing",
    )(arrived, begun, everyone, own, diagonal, theta)
    vector, energies = call(
        functools.partial(scaling_kernel, entries),
        [((1, share, block), F32), ((2,), F32)],
        [VMEM] * 3,
        "scaling",
        outs=[VMEM, SMEM],
    )(swap_all(send, OP), final, thetas)
    return vector, energies


def solution(mesh):
    split = Mesh(
        mesh.devices.reshape(mesh.shape["sector"], 4, 4, 2), ("sector", "op_0", "op_1", "op_2")
    )
    in_specs = (
        P("sector", OP, None),
        P("sector", OP, None),
        P(OP, None, None),
        P(OP, None, None),
        P(),
        P(),
    )
    out_specs = (P("sector", OP, None), P())
    return jax.shard_map(
        shards, mesh=split, in_specs=in_specs, out_specs=out_specs, check_vma=False
    )
```
